512 devices in a mesh: group: 16 (over y, core), slab: 32 (over z, x).
Axes of the slice: x: 4, y: 8, z: 8, core: 2. Of those that a mesh axis runs over, the one named last changes fastest.
Arguments:
- state: float32 [32, 256, 32, 256], P('group', 'slab'), may hold values from -3 to 3
- theta: float32 [32, 128, 16, 128], P('group', 'slab'), may hold values from -2.5 to 2.5
- forcing: float32 [256, 32, 256], P('slab'), may hold values from -6 to 6
- boxes: int32 [6, 16384], replicated, may hold values from 0 to 256, as said below
- observed: float32 [16384], P('slab'), may hold values from -6 to 6
- noise_var: float32 [16384], P('slab'), may hold values from 0.05 to 0.5
- perturb: float32 [32, 16384], P('group', 'slab'), may hold values from -6 to 6
Outputs:
- final_state: float32 [32, 256, 32, 256], P('group', 'slab')
- theta_new: float32 [32, 128, 16, 128], P('group', 'slab')
The draws below stay inside these ranges and needn't reach their ends.
Inputs may be any that keep to these rules, and one draw needn't show every extreme that they name: `boxes`: for every observation z0 < z1 <= 256, y0 < y1 <= 8, x0 < x1 <= 64; a box spans at most 16 planes, 4 tiles along the second dimension and 8 along the third (fewer where the grid is narrower), and these most are reached.
All inputs are finite; a program needn't handle non-finite values.
Results may differ from the reference program's by a relative error of at most 0.00019.
Values sent between devices are 32-bit elements; how exact they have to be, the bound alone decides.
No kernel may reach another device: no remote copies, remote signals or barrier semaphores. Data moves between devices by JAX's collectives and lax.ppermute only.
A program may use at most 64 MiB of HBM per device.

```python
import math
import jax
import jax.numpy as jnp
from jax import lax

CZ = 8
NY = 32
NX = 256
MEMBERS = 32
NZ = 256
OBS = 16384


def draw_boxes(key, part):
    keys = jax.random.split(key, 6)
    tiles_y = NY // 4
    tiles_x = NX // 4
    length_z = jax.random.randint(keys[0], (OBS,), 1, 2 * CZ + 1)
    start_z = jax.random.randint(keys[1], (OBS,), 0, NZ - length_z + 1)
    length_y = jax.random.randint(keys[2], (OBS,), 1, min(4, tiles_y) + 1)
    start_y = jax.random.randint(keys[3], (OBS,), 0, tiles_y - length_y + 1)
    length_x = jax.random.randint(keys[4], (OBS,), 1, min(8, tiles_x) + 1)
    start_x = jax.random.randint(keys[5], (OBS,), 0, tiles_x - length_x + 1)
    stacked = jnp.stack([start_z, start_z + length_z, start_y, start_y + length_y, start_x, start_x + length_x])
    return stacked.astype(jnp.int32)


def block_scale(own_key, shape, shards, low, high):
    level, own = 1.0, jax.random.fold_in(own_key, 6)
    for position, parts in shards:
        heights = jnp.exp(jax.random.uniform(jax.random.fold_in(own, position), (parts,), jnp.float32, low / len(shards), high / len(shards)))
        level = level * jnp.repeat(heights, shape[position] // parts).reshape([-1 if axis == position else 1 for axis in range(len(shape))])
    return level


def bell_draw(own_key, extent, spread, reach, shards=(), held_as=jnp.bfloat16):
    loudness = block_scale(own_key, extent, shards, -0.22, 0.18) if shards else 1.0
    array = jax.random.normal(own_key, extent, jnp.float32) * spread * loudness
    return jnp.minimum(jnp.maximum(array, -reach), reach).astype(held_as)


def setup_inputs(seed: int = 0) -> dict:
    streams_of = jax.random.split(jax.random.key(seed), 8)
    state = bell_draw(streams_of[0], (MEMBERS, NZ, NY, NX), 0.5, 3.0, ((0, 16), (1, 32)), jnp.float32)
    theta = bell_draw(streams_of[1], (MEMBERS, NZ // 2, NY // 2, NX // 2), 0.4, 2.5, ((0, 16), (1, 32)), jnp.float32)
    forcing = bell_draw(streams_of[2], (NZ, NY, NX), 1.0, 6.0, ((0, 32),), jnp.float32)
    boxes = draw_boxes(jax.random.fold_in(streams_of[7], 71), 0)
    observed = bell_draw(streams_of[4], (OBS,), 1.0, 6.0, ((0, 32),), jnp.float32)
    noise_var = jnp.clip(jnp.exp(math.log(0.5) - 2.3025851 * jax.random.uniform(streams_of[5], (OBS,), jnp.float32) ** block_scale(streams_of[5], (OBS,), ((0, 32),), -0.2, 0.2)), 0.05, 0.5)
    perturb = bell_draw(streams_of[6], (MEMBERS, OBS), 1.0, 6.0, ((0, 16), (1, 32)), jnp.float32)
    return {"state": state, "theta": theta, "forcing": forcing, "boxes": boxes, "observed": observed, "noise_var": noise_var, "perturb": perturb}


STEP_SIZE = 0.1

def advance(padded, diffusivity, forcing):
    center = padded[:, 1:-1]
    side_pad = jnp.pad(center, ((0, 0), (0, 0), (1, 1), (1, 1)))
    beside_all = padded[:, 2:] + padded[:, :-2]
    beside_all = beside_all + side_pad[:, :, 2:, 1:-1] + side_pad[:, :, :-2, 1:-1]
    beside_all = beside_all + side_pad[:, :, 1:-1, 2:] + side_pad[:, :, 1:-1, :-2]
    change = diffusivity * (beside_all - 6.0 * center) + 0.5 * center * (1.0 - center * center) + forcing
    return center + STEP_SIZE * change

def upsample(params):
    return jnp.repeat(jnp.repeat(jnp.repeat(params, 2, axis=1), 2, axis=2), 2, axis=3)

def reference(state, theta, forcing, boxes, observed, noise_var, perturb):
    diffusivity = 0.5 * jnp.exp(upsample(theta))
    current = state
    for sweep in range(2):
        padded = jnp.pad(current, ((0, 0), (1, 1), (0, 0), (0, 0)))
        current = advance(padded, diffusivity, forcing[None])
    members = current.shape[0]
    tiles = current.reshape(members, NZ, NY // 4, 4, NX // 4, 4).sum(axis=(3, 5))
    table = jnp.cumsum(jnp.cumsum(jnp.cumsum(tiles, axis=1), axis=2), axis=3)
    table = jnp.pad(table, ((0, 0), (1, 0), (1, 0), (1, 0)))
    lower_z, upper_z = (boxes[0], boxes[1])
    lower_y, upper_y = (boxes[2], boxes[3])
    lower_x, upper_x = (boxes[4], boxes[5])
    total = table[:, upper_z, upper_y, upper_x] - table[:, lower_z, upper_y, upper_x]
    total = total - table[:, upper_z, lower_y, upper_x] - table[:, upper_z, upper_y, lower_x]
    total = total + table[:, lower_z, lower_y, upper_x] + table[:, lower_z, upper_y, lower_x]
    total = total + table[:, upper_z, lower_y, lower_x] - table[:, lower_z, lower_y, lower_x]
    count = ((upper_z - lower_z) * (upper_y - lower_y) * (upper_x - lower_x) * 16).astype(jnp.float32)
    predicted = total / count[None]
    scale = jnp.sqrt(jnp.float32(members - 1))
    anomaly = (predicted - lax.optimization_barrier(jnp.mean(predicted, axis=0, keepdims=True))) / scale
    misfit = observed[None] + jnp.sqrt(noise_var)[None] * perturb - predicted
    weighted = anomaly / noise_var[None]
    inner = jnp.dot(weighted, anomaly.T, precision=lax.Precision.HIGHEST)
    cross = jnp.dot(weighted, misfit.T, precision=lax.Precision.HIGHEST)
    identity = jnp.eye(members, dtype=jnp.float32)
    factor = jnp.linalg.cholesky(identity + inner)
    gain = jax.scipy.linalg.cho_solve((factor, True), cross)
    mixing = identity + (gain - lax.optimization_barrier(jnp.mean(gain, axis=0, keepdims=True))) / scale
    flat_theta = theta.reshape(members, -1)
    updated = jnp.dot(mixing.T, flat_theta, precision=lax.Precision.HIGHEST)
    return (current, updated.reshape(theta.shape))
```

```python
import functools

import jax
import jax.numpy as jnp
from jax import lax
from jax.experimental import pallas as pl
from jax.experimental.pallas import tpu as pltpu
from jax.sharding import PartitionSpec as P

STEP_SIZE = 0.1
F32 = jnp.float32
BF16 = jnp.bfloat16

LOCAL = 2
PLANES = 8
ROWS = 32
COLS = 256
COARSE = 4
SLABS = 32
GROUPS = 16
MEMBERS = 32
BLOCK = 512
HALO_ROWS = 176


def split3(value):
    a = value.astype(BF16)
    rest = value - a.astype(F32)
    b = rest.astype(BF16)
    c = (rest - b.astype(F32)).astype(BF16)
    return a, b, c


def pack_kernel(state, theta, forcing, first, last, sems):
    copies = []

    def copy(src, dst):
        copies.append(pltpu.make_async_copy(src, dst, sems.at[len(copies)]))

    for out, plane, coarse, force in ((first, 0, 0, 0), (last, PLANES - 2, COARSE - 1, PLANES - 1)):
        for m in range(LOCAL):
            for p in range(2):
                at = (m * 2 + p) * ROWS
                copy(state.at[m, plane + p], out.at[pl.ds(at, ROWS), :])
            copy(theta.at[m, coarse], out.at[pl.ds(160, 16), pl.ds(m * 128, 128)])
        copy(forcing.at[force], out.at[pl.ds(128, ROWS), :])
    for c in copies:
        c.start()
    for c in copies:
        c.wait()


def pack(state, theta, forcing):
    shape = jax.ShapeDtypeStruct((HALO_ROWS, COLS), F32)
    anywhere = pl.BlockSpec(memory_space=pl.ANY)
    return pl.pallas_call(
        pack_kernel,
        out_shape=(shape, shape),
        in_specs=[anywhere] * 3,
        out_specs=(anywhere, anywhere),
        scratch_shapes=[pltpu.SemaphoreType.DMA((14,))],
        name="pack",
    )(state, theta, forcing)


def window_kernel(slab, state, theta, forcing, low, high, boxes, final, part, count, diff, mid, done):
    s = slab[0]
    keep_low = jnp.where(s > 0, 0.5, 0.0).astype(F32)
    keep_high = jnp.where(s < SLABS - 1, 0.5, 0.0).astype(F32)
    pieces = []
    for m in range(LOCAL):
        pieces.append(keep_low * jnp.exp(low[160:176, m * 128 : (m + 1) * 128]))
        for c in range(COARSE):
            pieces.append(0.5 * jnp.exp(theta[m, c]))
        pieces.append(keep_high * jnp.exp(high[160:176, m * 128 : (m + 1) * 128]))
    coarse = jnp.concatenate(pieces, axis=0)
    up = (
        lax.broadcasted_iota(jnp.int32, (128, COLS), 1) // 2
        == lax.broadcasted_iota(jnp.int32, (128, COLS), 0)
    ).astype(F32).astype(BF16)
    wide = sum(jnp.dot(part_, up, preferred_element_type=F32) for part_ in split3(coarse))
    rows = LOCAL * (COARSE + 2) * 16
    for h in range(2):
        diff[h, pl.ds(0, rows, stride=2), :] = wide[:, h * 128 : (h + 1) * 128]
        diff[h, pl.ds(1, rows, stride=2), :] = wide[:, h * 128 : (h + 1) * 128]

    row = lax.broadcasted_iota(jnp.int32, (ROWS, COLS), 0)
    col = lax.broadcasted_iota(jnp.int32, (ROWS, COLS), 1)

    def step(below, center, above, d, f):
        beside = above + below
        beside = beside + jnp.where(row == ROWS - 1, 0.0, pltpu.roll(center, ROWS - 1, 0))
        beside = beside + jnp.where(row == 0, 0.0, pltpu.roll(center, 1, 0))
        beside = beside + jnp.where(col == COLS - 1, 0.0, pltpu.roll(center, COLS - 1, 1))
        beside = beside + jnp.where(col == 0, 0.0, pltpu.roll(center, 1, 1))
        change = d * (beside - 6.0 * center) + 0.5 * center * (1.0 - center * center) + f
        return center + STEP_SIZE * change

    def plane(m, p):
        if p < 0:
            at = (m * 2 + p + 2) * ROWS
            return low[at : at + ROWS, :]
        if p >= PLANES:
            at = (m * 2 + p - PLANES) * ROWS
            return high[at : at + ROWS, :]
        return state[m, p]

    def force(p):
        if p < 0:
            return low[128:160, :]
        if p >= PLANES:
            return high[128:160, :]
        return forcing[p]

    def diffusivity(m, p):
        at = (m * (COARSE + 2) + (p + 2) // 2) * ROWS
        return jnp.concatenate([diff[h, at : at + ROWS, :] for h in range(2)], axis=1)

    for m in range(LOCAL):
        for p in range(-1, PLANES + 1):
            mid[m * (PLANES + 2) + p + 1] = step(
                plane(m, p - 1), plane(m, p), plane(m, p + 1), diffusivity(m, p), force(p)
            )
        for p in range(PLANES):
            at = m * (PLANES + 2) + p
            new = step(mid[at], mid[at + 1], mid[at + 2], diffusivity(m, p), forcing[p])
            final[m, p] = new
            to = (m * PLANES + p) * ROWS
            for h in range(2):
                done[h, to : to + ROWS, :] = new[:, h * 128 : (h + 1) * 128]

    tall = LOCAL * PLANES * 8
    sums = jnp.concatenate(
        [sum(done[h, pl.ds(q, tall, stride=4), :] for q in range(4)) for h in range(2)], axis=1
    )
    fold = (
        lax.broadcasted_iota(jnp.int32, (COLS, 128), 0) // 4
        == lax.broadcasted_iota(jnp.int32, (COLS, 128), 1) % 64
    ).astype(F32).astype(BF16)
    tiles = sum(jnp.dot(part_, fold, preferred_element_type=F32) for part_ in split3(sums))
    top = tiles.astype(BF16).astype(F32)
    lane = lax.broadcasted_iota(jnp.int32, (tall, 128), 1)
    left = jnp.where(lane < 64, top, tiles - top).astype(BF16)

    iota_x = lax.broadcasted_iota(jnp.int32, (64, BLOCK), 0)
    iota_y = lax.broadcasted_iota(jnp.int32, (8, BLOCK), 0)

    def observe(d, carry):
        here = pl.ds(pl.multiple_of(d * BLOCK, BLOCK), BLOCK)
        b = boxes[:, here]
        in_x = ((iota_x >= b[4:5]) & (iota_x < b[5:6])).astype(F32).astype(BF16)
        along = jnp.dot(left, jnp.concatenate([in_x, in_x], axis=0), preferred_element_type=F32)
        z0 = jnp.broadcast_to(b[0:1], (8, BLOCK)) - s * PLANES
        z1 = jnp.broadcast_to(b[1:2], (8, BLOCK)) - s * PLANES
        in_y = (iota_y >= b[2:3]) & (iota_y < b[3:4])
        sums = [jnp.zeros((8, BLOCK), F32) for m in range(LOCAL)]
        for z in range(PLANES):
            in_z = (z0 <= z) & (z1 > z)
            for m in range(LOCAL):
                at = (m * PLANES + z) * 8
                sums[m] = sums[m] + jnp.where(in_z, along[at : at + 8], 0.0)
        for m in range(LOCAL):
            total = jnp.sum(jnp.where(in_y, sums[m], 0.0), axis=0, keepdims=True)
            for q in range(4):
                part[d, m * 4 + q : m * 4 + q + 1, :] = total[:, q * 128 : (q + 1) * 128]
        return carry

    lax.fori_loop(0, SLABS, observe, 0)

    b = boxes[:, pl.ds(pl.multiple_of(s * BLOCK, BLOCK), BLOCK)]
    cells = ((b[1:2] - b[0:1]) * (b[3:4] - b[2:3]) * (b[5:6] - b[4:5]) * 16).astype(F32)
    for m in range(LOCAL):
        for q in range(4):
            count[m * 4 + q : m * 4 + q + 1, :] = cells[:, q * 128 : (q + 1) * 128]


def window(slab, state, theta, forcing, low, high, boxes):
    vmem = pl.BlockSpec(memory_space=pltpu.VMEM)
    return pl.pallas_call(
        window_kernel,
        out_shape=(
            jax.ShapeDtypeStruct(state.shape, F32),
            jax.ShapeDtypeStruct((SLABS, 8, 128), F32),
            jax.ShapeDtypeStruct((8, 128), F32),
        ),
        in_specs=[pl.BlockSpec(memory_space=pltpu.SMEM)] + [vmem] * 6,
        out_specs=(vmem, vmem, vmem),
        scratch_shapes=[
            pltpu.VMEM((2, LOCAL * (COARSE + 2) * ROWS, 128), F32),
            pltpu.VMEM((LOCAL * (PLANES + 2), ROWS, COLS), F32),
            pltpu.VMEM((2, LOCAL * PLANES * ROWS, 128), F32),
        ],
        name="window",
    )(slab, state, theta, forcing, low, high, boxes)


def gather_kernel(arrived, count, copies, own):
    pred = jnp.sum(arrived[...], axis=0) / count[...]
    own[...] = pred
    for g in range(GROUPS):
        copies[g] = pred


def own_predictions(arrived, count):
    return pl.pallas_call(
        gather_kernel,
        out_shape=(
            jax.ShapeDtypeStruct((GROUPS, 8, 128), F32),
            jax.ShapeDtypeStruct((8, 128), F32),
        ),
        name="own_predictions",
    )(arrived, count)


def moments_kernel(preds, own, observed, noise, perturb, out):
    scale = 1.0 / (float(MEMBERS - 1) ** 0.5)
    everyone = jnp.concatenate(
        [preds[pl.ds(q, MEMBERS, stride=4), :] for q in range(4)], axis=1
    )
    mine = jnp.concatenate([own[pl.ds(q, LOCAL, stride=4), :] for q in range(4)], axis=1)
    anomaly = (everyone - jnp.mean(everyone, axis=0, keepdims=True)) * scale
    var = noise[...]
    misfit = observed[...] + jnp.sqrt(var) * perturb[...] - mine
    weighted = anomaly / var
    left = jnp.concatenate([anomaly, misfit, jnp.zeros((6, BLOCK), F32)], axis=0)
    right = jnp.concatenate(
        [
            weighted,
            weighted[8:],
            weighted[16:],
            weighted[24:],
            weighted,
            jnp.zeros((16, BLOCK), F32),
        ],
        axis=0,
    )
    product = lax.dot_general(
        left, right, (((1,), (1,)), ((), ())), precision=lax.Precision.HIGHEST,
        preferred_element_type=F32,
    )
    lane = lax.broadcasted_iota(jnp.int32, (8, 128), 1)
    packed = product[0:8]
    for start, at in ((32, 8), (56, 16), (72, 24), (80, 32)):
        packed = jnp.where(lane >= start, product[at : at + 8], packed)
    for d in range(SLABS):
        out[d] = packed


def moments(preds, own, observed, noise, perturb):
    return pl.pallas_call(
        moments_kernel,
        out_shape=jax.ShapeDtypeStruct((SLABS, 8, 128), F32),
        name="moments",
    )(preds, own, observed, noise, perturb)


def update_kernel(group, arrived, theta, out):
    packed = jnp.sum(arrived[...], axis=0)
    lane8 = lax.broadcasted_iota(jnp.int32, (8, 128), 1)
    blocks = []
    for c, start in enumerate((0, 32, 56, 72)):
        moved = pltpu.roll(packed, (8 * c - start) % 128, 1)
        blocks.append(jnp.where((lane8 >= 8 * c) & (lane8 < 32), moved, 0.0))
    upper = jnp.concatenate(blocks + [jnp.zeros((96, 128), F32)], axis=0)
    mirrored = upper.T[0:MEMBERS]
    upper = upper[0:MEMBERS]
    row = lax.broadcasted_iota(jnp.int32, (MEMBERS, 128), 0)
    lane = lax.broadcasted_iota(jnp.int32, (MEMBERS, 128), 1)
    matrix = jnp.where(lane // 8 >= row // 8, upper, mirrored)
    matrix = jnp.where(row == lane, matrix + 1.0, matrix)
    cross_rows = jnp.where(lane8 < MEMBERS, pltpu.roll(packed, 128 - 80, 1), 0.0)
    cross = jnp.concatenate([cross_rows, jnp.zeros((120, 128), F32)], axis=0).T[0:MEMBERS]
    cross = pltpu.roll(cross, MEMBERS, 1)
    work = jnp.where((lane >= MEMBERS) & (lane < MEMBERS + LOCAL), cross, matrix)
    for k in range(MEMBERS):
        column = jnp.broadcast_to(work[:, k : k + 1], (MEMBERS, 128))
        pivot = column[k : k + 1, :]
        line = work[k : k + 1, :] / pivot
        work = jnp.where(row == k, line, work - column * line)
    gain = work
    mixing = (gain - jnp.mean(gain, axis=0, keepdims=True)) * (1.0 / float(MEMBERS - 1) ** 0.5)
    first = group[0] * LOCAL
    mixing = jnp.where(row - first == lane - MEMBERS, mixing + 1.0, mixing)
    columns = [
        jnp.broadcast_to(mixing[:, MEMBERS + j : MEMBERS + j + 1], (MEMBERS, 128))
        for j in range(LOCAL)
    ]
    totals = [jnp.zeros((64, 128), F32) for j in range(LOCAL)]
    for k in range(MEMBERS):
        field = theta[k]
        for j in range(LOCAL):
            totals[j] = totals[j] + columns[j][k : k + 1, :] * field
    for j in range(LOCAL):
        out[j] = totals[j]


def update(group, arrived, theta):
    vmem = pl.BlockSpec(memory_space=pltpu.VMEM)
    return pl.pallas_call(
        update_kernel,
        out_shape=jax.ShapeDtypeStruct((LOCAL, 64, 128), F32),
        in_specs=[pl.BlockSpec(memory_space=pltpu.SMEM), vmem, vmem],
        out_specs=vmem,
        name="update",
    )(group, arrived, theta)


def local(state, theta, forcing, boxes, observed, noise_var, perturb):
    slab = lax.axis_index("slab").astype(jnp.int32).reshape(1)
    group = lax.axis_index("group").astype(jnp.int32).reshape(1)
    first, last = pack(state, theta, forcing)
    low = lax.ppermute(last, "slab", [(i, i + 1) for i in range(SLABS - 1)])
    high = lax.ppermute(first, "slab", [(i + 1, i) for i in range(SLABS - 1)])
    field = theta.reshape(1, LOCAL, 64, 128)
    fields = lax.all_to_all(
        jnp.broadcast_to(field, (GROUPS, LOCAL, 64, 128)), "group", 0, 0, tiled=True
    ).reshape(MEMBERS, 64, 128)
    final, part, count = window(slab, state, theta, forcing, low, high, boxes)
    arrived = lax.all_to_all(part, "slab", 0, 0, tiled=True)
    copies, own = own_predictions(arrived, count)
    preds = lax.all_to_all(copies, "group", 0, 0, tiled=True).reshape(GROUPS * 8, 128)
    sums = moments(preds, own, observed.reshape(1, BLOCK), noise_var.reshape(1, BLOCK), perturb)
    sums = lax.all_to_all(sums, "slab", 0, 0, tiled=True)
    updated = update(group, sums, fields)
    return final, updated.reshape(theta.shape)


def solution(mesh):
    return jax.shard_map(
        local,
        mesh=mesh,
        in_specs=(
            P("group", "slab", None, None),
            P("group", "slab", None, None),
            P("slab", None, None),
            P(),
            P("slab"),
            P("slab"),
            P("group", "slab"),
        ),
        out_specs=(P("group", "slab", None, None), P("group", "slab", None, None)),
        check_vma=False,
    )
```

```python
import jax
import jax.numpy as jnp
from jax import lax
from jax.experimental import pallas as pl
from jax.experimental.pallas import tpu as pltpu
from jax.sharding import PartitionSpec as P


STEP_SIZE = 0.1
F32 = jnp.float32
BF16 = jnp.bfloat16

LOCAL = 2
PLANES = 8
ROWS = 32
COLS = 256
COARSE = 4
SLABS = 32
GROUPS = 16
MEMBERS = 32
BLOCK = 512
MIB = 1 << 20
HALO_ROWS = 176


def split3(value):
    a = value.astype(BF16)
    rest = value - a.astype(F32)
    b = rest.astype(BF16)
    c = (rest - b.astype(F32)).astype(BF16)
    return a, b, c


def pack_kernel(state, theta, forcing, first, last, sems):
    copies = []

    def copy(src, dst):
        copies.append(pltpu.make_async_copy(src, dst, sems.at[len(copies)]))

    for out, plane, coarse, force in ((first, 0, 0, 0), (last, PLANES - 2, COARSE - 1, PLANES - 1)):
        for m in range(LOCAL):
            for p in range(2):
                at = (m * 2 + p) * ROWS
                copy(state.at[m, plane + p], out.at[pl.ds(at, ROWS), :])
            copy(theta.at[m, coarse], out.at[pl.ds(160, 16), pl.ds(m * 128, 128)])
        copy(forcing.at[force], out.at[pl.ds(128, ROWS), :])
    for c in copies:
        c.start()
    for c in copies:
        c.wait()


def pack(state, theta, forcing):
    shape = jax.ShapeDtypeStruct((HALO_ROWS, COLS), F32)
    vmem = pl.BlockSpec(memory_space=pltpu.VMEM)
    return pl.pallas_call(
        pack_kernel,
        out_shape=(shape, shape),
        in_specs=[pl.BlockSpec(memory_space=pltpu.HBM)] * 3,
        out_specs=(vmem, vmem),
        compiler_params=pltpu.CompilerParams(vmem_limit_bytes=2 * MIB),
        scratch_shapes=[pltpu.SemaphoreType.DMA((14,))],
        name="pack",
    )(*(pltpu.with_memory_space_constraint(a, pltpu.HBM) for a in (state, theta, forcing)))


def window_kernel(slab, state, theta, forcing, low, high, boxes, final, part, count, diff, mid, fresh, done, sem):
    s = slab[0]
    keep_low = jnp.where(s > 0, 0.5, 0.0).astype(F32)
    keep_high = jnp.where(s < SLABS - 1, 0.5, 0.0).astype(F32)
    pieces = []
    for m in range(LOCAL):
        pieces.append(keep_low * jnp.exp(low[160:176, m * 128 : (m + 1) * 128]))
        for c in range(COARSE):
            pieces.append(0.5 * jnp.exp(theta[m, c]))
        pieces.append(keep_high * jnp.exp(high[160:176, m * 128 : (m + 1) * 128]))
    coarse = jnp.concatenate(pieces, axis=0)
    up = (
        lax.broadcasted_iota(jnp.int32, (128, COLS), 1) // 2
        == lax.broadcasted_iota(jnp.int32, (128, COLS), 0)
    ).astype(F32).astype(BF16)
    wide = sum(jnp.dot(part_, up, preferred_element_type=F32) for part_ in split3(coarse))
    rows = LOCAL * (COARSE + 2) * 16
    for h in range(2):
        diff[h, pl.ds(0, rows, stride=2), :] = wide[:, h * 128 : (h + 1) * 128]
        diff[h, pl.ds(1, rows, stride=2), :] = wide[:, h * 128 : (h + 1) * 128]

    row = lax.broadcasted_iota(jnp.int32, (ROWS, COLS), 0)
    col = lax.broadcasted_iota(jnp.int32, (ROWS, COLS), 1)

    def step(below, center, above, d, f):
        beside = above + below
        beside = beside + jnp.where(row == ROWS - 1, 0.0, pltpu.roll(center, ROWS - 1, 0))
        beside = beside + jnp.where(row == 0, 0.0, pltpu.roll(center, 1, 0))
        beside = beside + jnp.where(col == COLS - 1, 0.0, pltpu.roll(center, COLS - 1, 1))
        beside = beside + jnp.where(col == 0, 0.0, pltpu.roll(center, 1, 1))
        change = d * (beside - 6.0 * center) + 0.5 * center * (1.0 - center * center) + f
        return center + STEP_SIZE * change

    def plane(m, p):
        if p < 0:
            at = (m * 2 + p + 2) * ROWS
            return low[at : at + ROWS, :]
        if p >= PLANES:
            at = (m * 2 + p - PLANES) * ROWS
            return high[at : at + ROWS, :]
        return state[m, p]

    def force(p):
        if p < 0:
            return low[128:160, :]
        if p >= PLANES:
            return high[128:160, :]
        return forcing[p]

    def diffusivity(m, p):
        at = (m * (COARSE + 2) + (p + 2) // 2) * ROWS
        return jnp.concatenate([diff[h, at : at + ROWS, :] for h in range(2)], axis=1)

    for m in range(LOCAL):
        for p in range(-1, PLANES + 1):
            mid[m * (PLANES + 2) + p + 1] = step(
                plane(m, p - 1), plane(m, p), plane(m, p + 1), diffusivity(m, p), force(p)
            )
        for p in range(PLANES):
            at = m * (PLANES + 2) + p
            new = step(mid[at], mid[at + 1], mid[at + 2], diffusivity(m, p), forcing[p])
            fresh[m, p] = new
            to = (m * PLANES + p) * ROWS
            for h in range(2):
                done[h, to : to + ROWS, :] = new[:, h * 128 : (h + 1) * 128]

    leave = pltpu.make_async_copy(fresh, final, sem)
    leave.start()

    tall = LOCAL * PLANES * 8
    sums = jnp.concatenate(
        [sum(done[h, pl.ds(q, tall, stride=4), :] for q in range(4)) for h in range(2)], axis=1
    )
    fold = (
        lax.broadcasted_iota(jnp.int32, (COLS, 128), 0) // 4
        == lax.broadcasted_iota(jnp.int32, (COLS, 128), 1) % 64
    ).astype(F32).astype(BF16)
    tiles = sum(jnp.dot(part_, fold, preferred_element_type=F32) for part_ in split3(sums))
    top = tiles.astype(BF16).astype(F32)
    lane = lax.broadcasted_iota(jnp.int32, (tall, 128), 1)
    left = jnp.where(lane < 64, top, tiles - top).astype(BF16)

    iota_x = lax.broadcasted_iota(jnp.int32, (64, BLOCK), 0)
    iota_y = lax.broadcasted_iota(jnp.int32, (8, BLOCK), 0)

    def observe(d, carry):
        here = pl.ds(pl.multiple_of(d * BLOCK, BLOCK), BLOCK)
        b = boxes[:, here]
        in_x = ((iota_x >= b[4:5]) & (iota_x < b[5:6])).astype(F32).astype(BF16)
        along = jnp.dot(left, jnp.concatenate([in_x, in_x], axis=0), preferred_element_type=F32)
        z0 = jnp.broadcast_to(b[0:1], (8, BLOCK)) - s * PLANES
        z1 = jnp.broadcast_to(b[1:2], (8, BLOCK)) - s * PLANES
        in_y = (iota_y >= b[2:3]) & (iota_y < b[3:4])
        sums = [jnp.zeros((8, BLOCK), F32) for _ in range(LOCAL)]
        for z in range(PLANES):
            in_z = (z0 <= z) & (z1 > z)
            for m in range(LOCAL):
                at = (m * PLANES + z) * 8
                sums[m] = sums[m] + jnp.where(in_z, along[at : at + 8], 0.0)
        for m in range(LOCAL):
            total = jnp.sum(jnp.where(in_y, sums[m], 0.0), axis=0, keepdims=True)
            for q in range(4):
                part[d, m * 4 + q : m * 4 + q + 1, :] = total[:, q * 128 : (q + 1) * 128]
        return carry

    lax.fori_loop(0, SLABS, observe, 0)

    b = boxes[:, pl.ds(pl.multiple_of(s * BLOCK, BLOCK), BLOCK)]
    cells = ((b[1:2] - b[0:1]) * (b[3:4] - b[2:3]) * (b[5:6] - b[4:5]) * 16).astype(F32)
    for m in range(LOCAL):
        for q in range(4):
            count[m * 4 + q : m * 4 + q + 1, :] = cells[:, q * 128 : (q + 1) * 128]
    leave.wait()


def window(slab, state, theta, forcing, low, high, boxes):
    vmem = pl.BlockSpec(memory_space=pltpu.VMEM)
    return pl.pallas_call(
        window_kernel,
        out_shape=(
            jax.ShapeDtypeStruct(state.shape, F32),
            jax.ShapeDtypeStruct((SLABS, 8, 128), F32),
            jax.ShapeDtypeStruct((8, 128), F32),
        ),
        in_specs=[pl.BlockSpec(memory_space=pltpu.SMEM)] + [vmem] * 6,
        out_specs=(pl.BlockSpec(memory_space=pltpu.HBM), vmem, vmem),
        compiler_params=pltpu.CompilerParams(vmem_limit_bytes=12 * MIB),
        scratch_shapes=[
            pltpu.VMEM((2, LOCAL * (COARSE + 2) * ROWS, 128), F32),
            pltpu.VMEM((LOCAL * (PLANES + 2), ROWS, COLS), F32),
            pltpu.VMEM((LOCAL, PLANES, ROWS, COLS), F32),
            pltpu.VMEM((2, LOCAL * PLANES * ROWS, 128), F32),
            pltpu.SemaphoreType.DMA,
        ],
        name="window",
    )(slab, state, theta, forcing, low, high, boxes)


def gather_kernel(arrived, count, copies, own):
    pred = jnp.sum(arrived[...], axis=0) / count[...]
    own[...] = pred
    for g in range(GROUPS):
        copies[g] = pred


def own_predictions(arrived, count):
    return pl.pallas_call(
        gather_kernel,
        out_shape=(
            jax.ShapeDtypeStruct((GROUPS, 8, 128), F32),
            jax.ShapeDtypeStruct((8, 128), F32),
        ),
        compiler_params=pltpu.CompilerParams(vmem_limit_bytes=4 * MIB),
        name="own_predictions",
    )(arrived, count)


def moments_kernel(preds, own, observed, noise, perturb, out):
    scale = 1.0 / (float(MEMBERS - 1) ** 0.5)
    everyone = jnp.concatenate(
        [preds[pl.ds(q, MEMBERS, stride=4), :] for q in range(4)], axis=1
    )
    mine = jnp.concatenate([own[pl.ds(q, LOCAL, stride=4), :] for q in range(4)], axis=1)
    anomaly = (everyone - jnp.mean(everyone, axis=0, keepdims=True)) * scale
    var = noise[...]
    misfit = observed[...] + jnp.sqrt(var) * perturb[...] - mine
    weighted = anomaly / var
    left = jnp.concatenate([anomaly, misfit, jnp.zeros((6, BLOCK), F32)], axis=0)
    right = jnp.concatenate(
        [
            weighted,
            weighted[8:],
            weighted[16:],
            weighted[24:],
            weighted,
            jnp.zeros((16, BLOCK), F32),
        ],
        axis=0,
    )
    product = lax.dot_general(
        left, right, (((1,), (1,)), ((), ())), precision=lax.Precision.HIGHEST,
        preferred_element_type=F32,
    )
    lane = lax.broadcasted_iota(jnp.int32, (8, 128), 1)
    packed = product[0:8]
    for start, at in ((32, 8), (56, 16), (72, 24), (80, 32)):
        packed = jnp.where(lane >= start, product[at : at + 8], packed)
    for d in range(SLABS):
        out[d] = packed


def moments(preds, own, observed, noise, perturb):
    return pl.pallas_call(
        moments_kernel,
        out_shape=jax.ShapeDtypeStruct((SLABS, 8, 128), F32),
        compiler_params=pltpu.CompilerParams(vmem_limit_bytes=4 * MIB),
        name="moments",
    )(preds, own, observed, noise, perturb)


def update_kernel(group, arrived, theta, others, out):
    packed = jnp.sum(arrived[...], axis=0)
    lane8 = lax.broadcasted_iota(jnp.int32, (8, 128), 1)
    blocks = []
    for c, start in enumerate((0, 32, 56, 72)):
        moved = pltpu.roll(packed, (8 * c - start) % 128, 1)
        blocks.append(jnp.where((lane8 >= 8 * c) & (lane8 < 32), moved, 0.0))
    upper = jnp.concatenate(blocks + [jnp.zeros((96, 128), F32)], axis=0)
    mirrored = upper.T[0:MEMBERS]
    upper = upper[0:MEMBERS]
    row = lax.broadcasted_iota(jnp.int32, (MEMBERS, 128), 0)
    lane = lax.broadcasted_iota(jnp.int32, (MEMBERS, 128), 1)
    matrix = jnp.where(lane // 8 >= row // 8, upper, mirrored)
    matrix = jnp.where(row == lane, matrix + 1.0, matrix)
    cross_rows = jnp.where(lane8 < MEMBERS, pltpu.roll(packed, 128 - 80, 1), 0.0)
    cross = jnp.concatenate([cross_rows, jnp.zeros((120, 128), F32)], axis=0).T[0:MEMBERS]
    cross = pltpu.roll(cross, MEMBERS, 1)
    work = jnp.where((lane >= MEMBERS) & (lane < MEMBERS + LOCAL), cross, matrix)
    for k in range(MEMBERS):
        column = jnp.broadcast_to(work[:, k : k + 1], (MEMBERS, 128))
        pivot = column[k : k + 1, :]
        line = work[k : k + 1, :] / pivot
        work = jnp.where(row == k, line, work - column * line)
    gain = work
    mixing = (gain - jnp.mean(gain, axis=0, keepdims=True)) * (1.0 / float(MEMBERS - 1) ** 0.5)
    first = group[0] * LOCAL
    mixing = jnp.where(row - first == lane - MEMBERS, mixing + 1.0, mixing)
    south = group[0] % 2 == 0
    totals = [jnp.zeros((64, 128), F32) for _ in range(LOCAL)]
    for j in range(LOCAL):
        column = jnp.broadcast_to(mixing[:, MEMBERS + j : MEMBERS + j + 1], (MEMBERS, 128))
        later = pltpu.roll(column, MEMBERS - 2, 0)
        here = jnp.where(south, column, later)
        there = jnp.where(south, later, column)
        for y in range(GROUPS // 2):
            for m in range(LOCAL):
                at = 4 * y + m
                totals[j] = totals[j] + here[at : at + 1, :] * theta[2 * y + m]
                totals[j] = totals[j] + there[at : at + 1, :] * others[2 * y + m]
    for j in range(LOCAL):
        out[j] = totals[j]


def update(group, arrived, theta, others):
    vmem = pl.BlockSpec(memory_space=pltpu.VMEM)
    return pl.pallas_call(
        update_kernel,
        out_shape=jax.ShapeDtypeStruct((LOCAL, 64, 128), F32),
        in_specs=[pl.BlockSpec(memory_space=pltpu.SMEM)] + [vmem] * 3,
        out_specs=vmem,
        compiler_params=pltpu.CompilerParams(vmem_limit_bytes=4 * MIB),
        name="update",
    )(group, arrived, theta, others)


def local(state, theta, forcing, boxes, observed, noise_var, perturb):
    slab = lax.axis_index("slab").astype(jnp.int32).reshape(1)
    group = lax.axis_index("group").astype(jnp.int32).reshape(1)
    first, last = pack(state, theta, forcing)
    low = lax.ppermute(last, "slab", [(i, i + 1) for i in range(SLABS - 1)])
    high = lax.ppermute(first, "slab", [(i + 1, i) for i in range(SLABS - 1)])
    field = theta.reshape(1, LOCAL, 64, 128)
    copies = jnp.broadcast_to(field, (GROUPS // 2, LOCAL, 64, 128))
    sides = [list(range(core, GROUPS, 2)) for core in range(2)]
    fields = lax.all_to_all(copies, "group", 0, 0, axis_index_groups=sides, tiled=True)
    fields = fields.reshape(GROUPS, 64, 128)
    others = lax.ppermute(fields, "group", [(i, i ^ 1) for i in range(GROUPS)])
    final, part, count = window(slab, state, theta, forcing, low, high, boxes)
    arrived = lax.all_to_all(part, "slab", 0, 0, tiled=True)
    copies, own = own_predictions(arrived, count)
    preds = lax.all_to_all(copies, "group", 0, 0, tiled=True).reshape(GROUPS * 8, 128)
    sums = moments(preds, own, observed.reshape(1, BLOCK), noise_var.reshape(1, BLOCK), perturb)
    sums = lax.all_to_all(sums, "slab", 0, 0, tiled=True)
    updated = update(group, sums, fields, others)
    return final, updated.reshape(theta.shape)


def solution(mesh):
    return jax.shard_map(
        local,
        mesh=mesh,
        in_specs=(
            P("group", "slab", None, None),
            P("group", "slab", None, None),
            P("slab", None, None),
            P(),
            P("slab"),
            P("slab"),
            P("group", "slab"),
        ),
        out_specs=(P("group", "slab", None, None), P("group", "slab", None, None)),
        check_vma=False,
    )
```

```python
import jax
import jax.numpy as jnp
from jax import lax
from jax.experimental import pallas as pl
from jax.experimental.pallas import tpu as pltpu
from jax.sharding import PartitionSpec as P


STEP_SIZE = 0.1
F32 = jnp.float32
BF16 = jnp.bfloat16

LOCAL = 2
PLANES = 8
ROWS = 32
COLS = 256
COARSE = 4
SLABS = 32
GROUPS = 16
MEMBERS = 32
BLOCK = 512
MIB = 1 << 20
EVEN = (0, -2, 2, 4)
ODD = (-1, -3, 1, 3)
HALO_ROWS = 176


def split3(value):
    a = value.astype(BF16)
    rest = value - a.astype(F32)
    b = rest.astype(BF16)
    c = (rest - b.astype(F32)).astype(BF16)
    return a, b, c


def pack_kernel(state, theta, forcing, first, last, sems):
    copies = []

    def copy(src, dst):
        copies.append(pltpu.make_async_copy(src, dst, sems.at[len(copies)]))

    for out, plane, coarse, force in ((first, 0, 0, 0), (last, PLANES - 2, COARSE - 1, PLANES - 1)):
        for m in range(LOCAL):
            for p in range(2):
                at = (m * 2 + p) * ROWS
                copy(state.at[m, plane + p], out.at[pl.ds(at, ROWS), :])
            copy(theta.at[m, coarse], out.at[pl.ds(160, 16), pl.ds(m * 128, 128)])
        copy(forcing.at[force], out.at[pl.ds(128, ROWS), :])
    for c in copies:
        c.start()
    for c in copies:
        c.wait()


def pack(state, theta, forcing):
    shape = jax.ShapeDtypeStruct((HALO_ROWS, COLS), F32)
    vmem = pl.BlockSpec(memory_space=pltpu.VMEM)
    return pl.pallas_call(
        pack_kernel,
        out_shape=(shape, shape),
        in_specs=[pl.BlockSpec(memory_space=pltpu.HBM)] * 3,
        out_specs=(vmem, vmem),
        compiler_params=pltpu.CompilerParams(vmem_limit_bytes=2 * MIB),
        scratch_shapes=[pltpu.SemaphoreType.DMA((14,))],
        name="pack",
    )(*(pltpu.with_memory_space_constraint(a, pltpu.HBM) for a in (state, theta, forcing)))


def window_kernel(
    slab, state, theta, forcing, low, high, observed, noise, perturb, footprints,
    final, part, count, given, diff, mid, fresh, done, boxes, sems,
):
    enter = pltpu.make_async_copy(footprints, boxes, sems.at[0])
    enter.start()
    s = slab[0]
    keep_low = jnp.where(s > 0, 0.5, 0.0).astype(F32)
    keep_high = jnp.where(s < SLABS - 1, 0.5, 0.0).astype(F32)
    pieces = []
    for m in range(LOCAL):
        pieces.append(keep_low * jnp.exp(low[160:176, m * 128 : (m + 1) * 128]))
        for c in range(COARSE):
            pieces.append(0.5 * jnp.exp(theta[m, c]))
        pieces.append(keep_high * jnp.exp(high[160:176, m * 128 : (m + 1) * 128]))
    coarse = jnp.concatenate(pieces, axis=0)
    up = (
        lax.broadcasted_iota(jnp.int32, (128, COLS), 1) // 2
        == lax.broadcasted_iota(jnp.int32, (128, COLS), 0)
    ).astype(F32).astype(BF16)
    wide = sum(jnp.dot(part_, up, preferred_element_type=F32) for part_ in split3(coarse))
    rows = LOCAL * (COARSE + 2) * 16
    for h in range(2):
        diff[h, pl.ds(0, rows, stride=2), :] = wide[:, h * 128 : (h + 1) * 128]
        diff[h, pl.ds(1, rows, stride=2), :] = wide[:, h * 128 : (h + 1) * 128]

    row = lax.broadcasted_iota(jnp.int32, (ROWS, COLS), 0)
    col = lax.broadcasted_iota(jnp.int32, (ROWS, COLS), 1)

    def step(below, center, above, d, f):
        beside = above + below
        beside = beside + jnp.where(row == ROWS - 1, 0.0, pltpu.roll(center, ROWS - 1, 0))
        beside = beside + jnp.where(row == 0, 0.0, pltpu.roll(center, 1, 0))
        beside = beside + jnp.where(col == COLS - 1, 0.0, pltpu.roll(center, COLS - 1, 1))
        beside = beside + jnp.where(col == 0, 0.0, pltpu.roll(center, 1, 1))
        change = d * (beside - 6.0 * center) + 0.5 * center * (1.0 - center * center) + f
        return center + STEP_SIZE * change

    def plane(m, p):
        if p < 0:
            at = (m * 2 + p + 2) * ROWS
            return low[at : at + ROWS, :]
        if p >= PLANES:
            at = (m * 2 + p - PLANES) * ROWS
            return high[at : at + ROWS, :]
        return state[m, p]

    def force(p):
        if p < 0:
            return low[128:160, :]
        if p >= PLANES:
            return high[128:160, :]
        return forcing[p]

    def diffusivity(m, p):
        at = (m * (COARSE + 2) + (p + 2) // 2) * ROWS
        return jnp.concatenate([diff[h, at : at + ROWS, :] for h in range(2)], axis=1)

    for m in range(LOCAL):
        for p in range(-1, PLANES + 1):
            mid[m * (PLANES + 2) + p + 1] = step(
                plane(m, p - 1), plane(m, p), plane(m, p + 1), diffusivity(m, p), force(p)
            )
        for p in range(PLANES):
            at = m * (PLANES + 2) + p
            new = step(mid[at], mid[at + 1], mid[at + 2], diffusivity(m, p), forcing[p])
            fresh[m, p] = new
            to = (m * PLANES + p) * ROWS
            for h in range(2):
                done[h, to : to + ROWS, :] = new[:, h * 128 : (h + 1) * 128]

    leave = pltpu.make_async_copy(fresh, final, sems.at[1])
    leave.start()

    tall = LOCAL * PLANES * 8
    sums = jnp.concatenate(
        [sum(done[h, pl.ds(q, tall, stride=4), :] for q in range(4)) for h in range(2)], axis=1
    )
    fold = (
        lax.broadcasted_iota(jnp.int32, (COLS, 128), 0) // 4
        == lax.broadcasted_iota(jnp.int32, (COLS, 128), 1) % 64
    ).astype(F32).astype(BF16)
    tiles = sum(jnp.dot(part_, fold, preferred_element_type=F32) for part_ in split3(sums))
    top = tiles.astype(BF16).astype(F32)
    lane = lax.broadcasted_iota(jnp.int32, (tall, 128), 1)
    left = jnp.where(lane < 64, top, tiles - top).astype(BF16)

    enter.wait()
    iota_x = lax.broadcasted_iota(jnp.int32, (64, BLOCK), 0)
    iota_y = lax.broadcasted_iota(jnp.int32, (8, BLOCK), 0)

    def observe(d, carry):
        here = pl.ds(pl.multiple_of(d * BLOCK, BLOCK), BLOCK)
        b = boxes[:, here]
        in_x = ((iota_x >= b[4:5]) & (iota_x < b[5:6])).astype(F32).astype(BF16)
        along = jnp.dot(left, jnp.concatenate([in_x, in_x], axis=0), preferred_element_type=F32)
        z0 = jnp.broadcast_to(b[0:1], (8, BLOCK)) - s * PLANES
        z1 = jnp.broadcast_to(b[1:2], (8, BLOCK)) - s * PLANES
        in_y = (iota_y >= b[2:3]) & (iota_y < b[3:4])
        sums = [jnp.zeros((8, BLOCK), F32) for _ in range(LOCAL)]
        for z in range(PLANES):
            in_z = (z0 <= z) & (z1 > z)
            for m in range(LOCAL):
                at = (m * PLANES + z) * 8
                sums[m] = sums[m] + jnp.where(in_z, along[at : at + 8], 0.0)
        for m in range(LOCAL):
            total = jnp.sum(jnp.where(in_y, sums[m], 0.0), axis=0, keepdims=True)
            for q in range(4):
                part[d, m * 4 + q : m * 4 + q + 1, :] = total[:, q * 128 : (q + 1) * 128]
        return carry

    lax.fori_loop(0, SLABS, observe, 0, unroll=4)

    b = boxes[:, pl.ds(pl.multiple_of(s * BLOCK, BLOCK), BLOCK)]
    cells = ((b[1:2] - b[0:1]) * (b[3:4] - b[2:3]) * (b[5:6] - b[4:5]) * 16).astype(F32)
    for m in range(LOCAL):
        for q in range(4):
            count[m * 4 + q : m * 4 + q + 1, :] = cells[:, q * 128 : (q + 1) * 128]
    var = noise[...]
    given[0:LOCAL, :] = observed[...] + jnp.sqrt(var) * perturb[...]
    given[LOCAL : LOCAL + 1, :] = var
    given[LOCAL + 1 : 8, :] = jnp.zeros((5, BLOCK), F32)
    leave.wait()


def window(slab, state, theta, forcing, low, high, boxes, observed, noise, perturb):
    vmem = pl.BlockSpec(memory_space=pltpu.VMEM)
    return pl.pallas_call(
        window_kernel,
        out_shape=(
            jax.ShapeDtypeStruct(state.shape, F32),
            jax.ShapeDtypeStruct((SLABS, 8, 128), F32),
            jax.ShapeDtypeStruct((8, 128), F32),
            jax.ShapeDtypeStruct((8, BLOCK), F32),
        ),
        in_specs=[pl.BlockSpec(memory_space=pltpu.SMEM)]
        + [vmem] * 8
        + [pl.BlockSpec(memory_space=pltpu.HBM)],
        out_specs=(pl.BlockSpec(memory_space=pltpu.HBM), vmem, vmem, vmem),
        compiler_params=pltpu.CompilerParams(vmem_limit_bytes=12 * MIB),
        scratch_shapes=[
            pltpu.VMEM((2, LOCAL * (COARSE + 2) * ROWS, 128), F32),
            pltpu.VMEM((LOCAL * (PLANES + 2), ROWS, COLS), F32),
            pltpu.VMEM((LOCAL, PLANES, ROWS, COLS), F32),
            pltpu.VMEM((2, LOCAL * PLANES * ROWS, 128), F32),
            pltpu.VMEM(boxes.shape, jnp.int32),
            pltpu.SemaphoreType.DMA((2,)),
        ],
        name="window",
    )(
        slab, state, theta, forcing, low, high, observed, noise, perturb,
        pltpu.with_memory_space_constraint(boxes, pltpu.HBM),
    )


def gather_kernel(arrived, count, copies, own):
    pred = jnp.sum(arrived[...], axis=0) / count[...]
    own[...] = pred
    for g in range(GROUPS):
        copies[g] = pred


def own_predictions(arrived, count):
    return pl.pallas_call(
        gather_kernel,
        out_shape=(
            jax.ShapeDtypeStruct((GROUPS, 8, 128), F32),
            jax.ShapeDtypeStruct((8, 128), F32),
        ),
        compiler_params=pltpu.CompilerParams(vmem_limit_bytes=4 * MIB),
        name="own_predictions",
    )(arrived, count)


def moments_kernel(preds, own, given, out):
    scale = 1.0 / (float(MEMBERS - 1) ** 0.5)
    everyone = jnp.concatenate(
        [preds[pl.ds(q, MEMBERS, stride=4), :] for q in range(4)], axis=1
    )
    mine = jnp.concatenate([own[pl.ds(q, LOCAL, stride=4), :] for q in range(4)], axis=1)
    anomaly = (everyone - jnp.mean(everyone, axis=0, keepdims=True)) * scale
    misfit = given[0:LOCAL, :] - mine
    var = given[LOCAL : LOCAL + 1, :]
    weighted = anomaly / var
    pad = jnp.zeros((6, BLOCK), F32)
    right = jnp.concatenate(
        [anomaly, anomaly[8:], anomaly[16:], anomaly[24:]]
        + [misfit, pad] * 4
        + [jnp.zeros((16, BLOCK), F32)],
        axis=0,
    )
    product = lax.dot_general(
        weighted, right, (((1,), (1,)), ((), ())), precision=lax.Precision.HIGHEST,
        preferred_element_type=F32,
    )
    lane = lax.broadcasted_iota(jnp.int32, (8, 128), 1)
    packed = product[0:8]
    for c, start, stop in ((1, 32, 56), (2, 56, 72), (3, 72, 80)):
        mine = ((lane >= start) & (lane < stop)) | (lane // 8 == 10 + c)
        packed = jnp.where(mine, product[8 * c : 8 * c + 8], packed)
    for d in range(SLABS):
        out[d] = packed


def moments(preds, own, given):
    return pl.pallas_call(
        moments_kernel,
        out_shape=jax.ShapeDtypeStruct((SLABS, 8, 128), F32),
        compiler_params=pltpu.CompilerParams(vmem_limit_bytes=4 * MIB),
        name="moments",
    )(preds, own, given)


def update_kernel(group, arrived, even, odd, even_other, odd_other, out):
    parts = [arrived[d] for d in range(SLABS)]
    while len(parts) > 1:
        parts = [x + y for x, y in zip(parts[::2], parts[1::2])]
    packed = parts[0]
    lane8 = lax.broadcasted_iota(jnp.int32, (8, 128), 1)
    uppers, cross = [], []
    for c, start in enumerate((0, 32, 56, 72)):
        moved = pltpu.roll(packed, (8 * c - start) % 128, 1)
        uppers.append(jnp.where((lane8 >= 8 * c) & (lane8 < MEMBERS), moved, 0.0))
        cross.append(pltpu.roll(packed, (MEMBERS - 80 - 8 * c) % 128, 1))
    upper = jnp.concatenate(uppers, axis=0)
    cross = jnp.concatenate(cross, axis=0)
    tall = jnp.concatenate([upper, jnp.zeros((96, 128), F32)], axis=0)
    mirrored = tall.T[0:MEMBERS]
    row = lax.broadcasted_iota(jnp.int32, (MEMBERS, 128), 0)
    lane = lax.broadcasted_iota(jnp.int32, (MEMBERS, 128), 1)
    work = jnp.where(lane // 8 >= row // 8, upper, mirrored)
    work = jnp.where(row == lane, work + 1.0, work)
    work = jnp.where(lane < MEMBERS, work, jnp.where(lane < MEMBERS + LOCAL, cross, 0.0))
    for first in range(0, MEMBERS, 8):
        columns = [
            jnp.broadcast_to(work[:, k : k + 1], (MEMBERS, 128)) for k in range(first, first + 8)
        ]
        for i in range(8):
            k = first + i
            column = columns[i]
            inverse = 1.0 / column[k : k + 1, :]
            line = work[k : k + 1, :] * inverse
            work = jnp.where(row == k, line, work - column * line)
            for later in range(i + 1, 8):
                line = columns[later][k : k + 1, :] * inverse
                columns[later] = jnp.where(row == k, line, columns[later] - column * line)
    mixing = work - jnp.mean(work, axis=0, keepdims=True)
    mixing = mixing * (1.0 / float(MEMBERS - 1) ** 0.5)
    mixing = jnp.where(row - group[0] * LOCAL == lane - MEMBERS, mixing + 1.0, mixing)
    south = group[0] % 2 == 0
    turn = MEMBERS - LOCAL * group[0]
    totals = [jnp.zeros((64, 128), F32) for _ in range(LOCAL)]
    for j in range(LOCAL):
        column = jnp.broadcast_to(mixing[:, MEMBERS + j : MEMBERS + j + 1], (MEMBERS, 128))
        here = pltpu.roll(column, turn, 0)
        there = jnp.where(south, pltpu.roll(here, MEMBERS - 2, 0), pltpu.roll(here, 2, 0))
        for rows, fields, offsets in (
            (here, even, EVEN),
            (here, odd, ODD),
            (there, even_other, EVEN),
            (there, odd_other, ODD),
        ):
            for i, offset in enumerate(offsets):
                for m in range(LOCAL):
                    at = (4 * offset + m) % MEMBERS
                    totals[j] = totals[j] + rows[at : at + 1, :] * fields[2 * i + m]
    for j in range(LOCAL):
        out[j] = totals[j]


def update(group, arrived, *fields):
    vmem = pl.BlockSpec(memory_space=pltpu.VMEM)
    return pl.pallas_call(
        update_kernel,
        out_shape=jax.ShapeDtypeStruct((LOCAL, 64, 128), F32),
        in_specs=[pl.BlockSpec(memory_space=pltpu.SMEM)] + [vmem] * 5,
        out_specs=vmem,
        compiler_params=pltpu.CompilerParams(vmem_limit_bytes=4 * MIB),
        name="update",
    )(group, arrived, *fields)


def local(state, theta, forcing, boxes, observed, noise_var, perturb):
    slab = lax.axis_index("slab").astype(jnp.int32).reshape(1)
    group = lax.axis_index("group").astype(jnp.int32).reshape(1)
    first, last = pack(state, theta, forcing)
    low = lax.ppermute(last, "slab", [(i, i + 1) for i in range(SLABS - 1)])
    high = lax.ppermute(first, "slab", [(i + 1, i) for i in range(SLABS - 1)])
    field = theta.reshape(LOCAL, 64, 128)

    def along_y(value, chips):
        moves = [(i, (i + 2 * chips) % GROUPS) for i in range(GROUPS)]
        return lax.ppermute(value, "group", moves)

    def other_core(value):
        return lax.ppermute(value, "group", [(i, i ^ 1) for i in range(GROUPS)])

    before = along_y(field, 2)
    after = along_y(field, -2)
    across = along_y(field, 4)
    final, part, count, given = window(
        slab, state, theta, forcing, low, high, boxes,
        observed.reshape(1, BLOCK), noise_var.reshape(1, BLOCK), perturb,
    )
    arrived = lax.all_to_all(part, "slab", 0, 0, tiled=True)
    even = jnp.concatenate([field, before, after, across], axis=0)
    odd = along_y(even, 1)
    even_other = other_core(even)
    copies, own = own_predictions(arrived, count)
    preds = lax.all_to_all(copies, "group", 0, 0, tiled=True).reshape(GROUPS * 8, 128)
    odd_other = other_core(odd)
    sums = moments(preds, own, given)
    sums = lax.all_to_all(sums, "slab", 0, 0, tiled=True)
    updated = update(group, sums, even, odd, even_other, odd_other)
    return final, updated.reshape(theta.shape)


def solution(mesh):
    return jax.shard_map(
        local,
        mesh=mesh,
        in_specs=(
            P("group", "slab", None, None),
            P("group", "slab", None, None),
            P("slab", None, None),
            P(),
            P("slab"),
            P("slab"),
            P("group", "slab"),
        ),
        out_specs=(P("group", "slab", None, None), P("group", "slab", None, None)),
        check_vma=False,
    )
```

```python
import jax
import jax.numpy as jnp
from jax import lax
from jax.experimental import pallas as pl
from jax.experimental.pallas import tpu as pltpu
from jax.sharding import PartitionSpec as P


STEP_SIZE = 0.1
F32 = jnp.float32
BF16 = jnp.bfloat16

LOCAL = 2
PLANES = 8
ROWS = 32
COLS = 256
COARSE = 4
SLABS = 32
GROUPS = 16
MEMBERS = 32
BLOCK = 512
MIB = 1 << 20
PARTS = (0, 1, 2, 3, -3, -2, -1, 4)
HALO_ROWS = 176


def split3(value):
    a = value.astype(BF16)
    rest = value - a.astype(F32)
    b = rest.astype(BF16)
    c = (rest - b.astype(F32)).astype(BF16)
    return a, b, c


def pack_kernel(state, theta, forcing, first, last, sems):
    copies = []

    def copy(src, dst):
        copies.append(pltpu.make_async_copy(src, dst, sems.at[len(copies)]))

    for out, plane, coarse, force in ((first, 0, 0, 0), (last, PLANES - 2, COARSE - 1, PLANES - 1)):
        for m in range(LOCAL):
            for p in range(2):
                at = (m * 2 + p) * ROWS
                copy(state.at[m, plane + p], out.at[pl.ds(at, ROWS), :])
            copy(theta.at[m, coarse], out.at[pl.ds(160, 16), pl.ds(m * 128, 128)])
        copy(forcing.at[force], out.at[pl.ds(128, ROWS), :])
    for c in copies:
        c.start()
    for c in copies:
        c.wait()


def pack(state, theta, forcing):
    shape = jax.ShapeDtypeStruct((HALO_ROWS, COLS), F32)
    vmem = pl.BlockSpec(memory_space=pltpu.VMEM)
    return pl.pallas_call(
        pack_kernel,
        out_shape=(shape, shape),
        in_specs=[pl.BlockSpec(memory_space=pltpu.HBM)] * 3,
        out_specs=(vmem, vmem),
        compiler_params=pltpu.CompilerParams(vmem_limit_bytes=2 * MIB),
        scratch_shapes=[pltpu.SemaphoreType.DMA((14,))],
        name="pack",
    )(*(pltpu.with_memory_space_constraint(a, pltpu.HBM) for a in (state, theta, forcing)))


def window_kernel(
    slab, state, theta, forcing, low, high, observed, noise, perturb, footprints,
    final, part, count, given, diff, mid, fresh, done, boxes, target, spread, draws, sems,
):
    enter = [
        pltpu.make_async_copy(src, dst, sems.at[i])
        for i, (src, dst) in enumerate(
            ((footprints, boxes), (observed, target), (noise, spread), (perturb, draws))
        )
    ]
    for e in enter:
        e.start()
    s = slab[0]
    keep_low = jnp.where(s > 0, 0.5, 0.0).astype(F32)
    keep_high = jnp.where(s < SLABS - 1, 0.5, 0.0).astype(F32)
    pieces = []
    for m in range(LOCAL):
        pieces.append(keep_low * jnp.exp(low[160:176, m * 128 : (m + 1) * 128]))
        for c in range(COARSE):
            pieces.append(0.5 * jnp.exp(theta[m, c]))
        pieces.append(keep_high * jnp.exp(high[160:176, m * 128 : (m + 1) * 128]))
    coarse = jnp.concatenate(pieces, axis=0)
    up = (
        lax.broadcasted_iota(jnp.int32, (128, COLS), 1) // 2
        == lax.broadcasted_iota(jnp.int32, (128, COLS), 0)
    ).astype(F32).astype(BF16)
    wide = sum(jnp.dot(part_, up, preferred_element_type=F32) for part_ in split3(coarse))
    rows = LOCAL * (COARSE + 2) * 16
    for h in range(2):
        diff[h, pl.ds(0, rows, stride=2), :] = wide[:, h * 128 : (h + 1) * 128]
        diff[h, pl.ds(1, rows, stride=2), :] = wide[:, h * 128 : (h + 1) * 128]

    row = lax.broadcasted_iota(jnp.int32, (ROWS, COLS), 0)
    col = lax.broadcasted_iota(jnp.int32, (ROWS, COLS), 1)

    def step(below, center, above, d, f):
        beside = above + below
        beside = beside + jnp.where(row == ROWS - 1, 0.0, pltpu.roll(center, ROWS - 1, 0))
        beside = beside + jnp.where(row == 0, 0.0, pltpu.roll(center, 1, 0))
        beside = beside + jnp.where(col == COLS - 1, 0.0, pltpu.roll(center, COLS - 1, 1))
        beside = beside + jnp.where(col == 0, 0.0, pltpu.roll(center, 1, 1))
        change = d * (beside - 6.0 * center) + 0.5 * center * (1.0 - center * center) + f
        return center + STEP_SIZE * change

    def plane(m, p):
        if p < 0:
            at = (m * 2 + p + 2) * ROWS
            return low[at : at + ROWS, :]
        if p >= PLANES:
            at = (m * 2 + p - PLANES) * ROWS
            return high[at : at + ROWS, :]
        return state[m, p]

    def force(p):
        if p < 0:
            return low[128:160, :]
        if p >= PLANES:
            return high[128:160, :]
        return forcing[p]

    def diffusivity(m, p):
        at = (m * (COARSE + 2) + (p + 2) // 2) * ROWS
        return jnp.concatenate([diff[h, at : at + ROWS, :] for h in range(2)], axis=1)

    for m in range(LOCAL):
        for p in range(-1, PLANES + 1):
            mid[m * (PLANES + 2) + p + 1] = step(
                plane(m, p - 1), plane(m, p), plane(m, p + 1), diffusivity(m, p), force(p)
            )
        for p in range(PLANES):
            at = m * (PLANES + 2) + p
            new = step(mid[at], mid[at + 1], mid[at + 2], diffusivity(m, p), forcing[p])
            fresh[m, p] = new
            to = (m * PLANES + p) * ROWS
            for h in range(2):
                done[h, to : to + ROWS, :] = new[:, h * 128 : (h + 1) * 128]

    leave = pltpu.make_async_copy(fresh, final, sems.at[4])
    leave.start()

    tall = LOCAL * PLANES * 8
    sums = jnp.concatenate(
        [sum(done[h, pl.ds(q, tall, stride=4), :] for q in range(4)) for h in range(2)], axis=1
    )
    fold = (
        lax.broadcasted_iota(jnp.int32, (COLS, 128), 0) // 4
        == lax.broadcasted_iota(jnp.int32, (COLS, 128), 1) % 64
    ).astype(F32).astype(BF16)
    tiles = sum(jnp.dot(part_, fold, preferred_element_type=F32) for part_ in split3(sums))
    top = tiles.astype(BF16).astype(F32)
    lane = lax.broadcasted_iota(jnp.int32, (tall, 128), 1)
    left = jnp.where(lane < 64, top, tiles - top).astype(BF16)

    for e in enter:
        e.wait()
    iota_x = lax.broadcasted_iota(jnp.int32, (64, BLOCK), 0)
    iota_y = lax.broadcasted_iota(jnp.int32, (8, BLOCK), 0)

    def observe(d, carry):
        here = pl.ds(pl.multiple_of(d * BLOCK, BLOCK), BLOCK)
        b = boxes[:, here]
        in_x = ((iota_x >= b[4:5]) & (iota_x < b[5:6])).astype(F32).astype(BF16)
        along = jnp.dot(left, jnp.concatenate([in_x, in_x], axis=0), preferred_element_type=F32)
        z0 = jnp.broadcast_to(b[0:1], (8, BLOCK)) - s * PLANES
        z1 = jnp.broadcast_to(b[1:2], (8, BLOCK)) - s * PLANES
        in_y = (iota_y >= b[2:3]) & (iota_y < b[3:4])
        sums = [jnp.zeros((8, BLOCK), F32) for _ in range(LOCAL)]
        for z in range(PLANES):
            in_z = (z0 <= z) & (z1 > z)
            for m in range(LOCAL):
                at = (m * PLANES + z) * 8
                sums[m] = sums[m] + jnp.where(in_z, along[at : at + 8], 0.0)
        for m in range(LOCAL):
            total = jnp.sum(jnp.where(in_y, sums[m], 0.0), axis=0, keepdims=True)
            for q in range(4):
                part[d, m * 4 + q : m * 4 + q + 1, :] = total[:, q * 128 : (q + 1) * 128]
        return carry

    lax.fori_loop(0, SLABS, observe, 0, unroll=4)

    b = boxes[:, pl.ds(pl.multiple_of(s * BLOCK, BLOCK), BLOCK)]
    cells = ((b[1:2] - b[0:1]) * (b[3:4] - b[2:3]) * (b[5:6] - b[4:5]) * 16).astype(F32)
    for m in range(LOCAL):
        for q in range(4):
            count[m * 4 + q : m * 4 + q + 1, :] = cells[:, q * 128 : (q + 1) * 128]
    var = spread[...]
    given[0:LOCAL, :] = target[...] + jnp.sqrt(var) * draws[...]
    given[LOCAL : LOCAL + 1, :] = var
    given[LOCAL + 1 : 8, :] = jnp.zeros((5, BLOCK), F32)
    leave.wait()


def window(slab, state, theta, forcing, low, high, *kept):
    vmem = pl.BlockSpec(memory_space=pltpu.VMEM)
    return pl.pallas_call(
        window_kernel,
        out_shape=(
            jax.ShapeDtypeStruct(state.shape, F32),
            jax.ShapeDtypeStruct((SLABS, 8, 128), F32),
            jax.ShapeDtypeStruct((8, 128), F32),
            jax.ShapeDtypeStruct((8, BLOCK), F32),
        ),
        in_specs=[pl.BlockSpec(memory_space=pltpu.SMEM)]
        + [vmem] * 5
        + [pl.BlockSpec(memory_space=pltpu.HBM)] * 4,
        out_specs=(pl.BlockSpec(memory_space=pltpu.HBM), vmem, vmem, vmem),
        compiler_params=pltpu.CompilerParams(vmem_limit_bytes=12 * MIB),
        scratch_shapes=[
            pltpu.VMEM((2, LOCAL * (COARSE + 2) * ROWS, 128), F32),
            pltpu.VMEM((LOCAL * (PLANES + 2), ROWS, COLS), F32),
            pltpu.VMEM((LOCAL, PLANES, ROWS, COLS), F32),
            pltpu.VMEM((2, LOCAL * PLANES * ROWS, 128), F32),
            pltpu.VMEM(kept[-1].shape, jnp.int32),
            pltpu.VMEM((1, BLOCK), F32),
            pltpu.VMEM((1, BLOCK), F32),
            pltpu.VMEM((LOCAL, BLOCK), F32),
            pltpu.SemaphoreType.DMA((5,)),
        ],
        name="window",
    )(
        slab, state, theta, forcing, low, high,
        *(pltpu.with_memory_space_constraint(a, pltpu.HBM) for a in kept),
    )


def gather_kernel(arrived, count, copies, own):
    pred = jnp.sum(arrived[...], axis=0) / count[...]
    own[...] = pred
    for g in range(GROUPS):
        copies[g] = pred


def own_predictions(arrived, count):
    return pl.pallas_call(
        gather_kernel,
        out_shape=(
            jax.ShapeDtypeStruct((GROUPS, 8, 128), F32),
            jax.ShapeDtypeStruct((8, 128), F32),
        ),
        compiler_params=pltpu.CompilerParams(vmem_limit_bytes=4 * MIB),
        name="own_predictions",
    )(arrived, count)


def moments_kernel(preds, own, given, out):
    scale = 1.0 / (float(MEMBERS - 1) ** 0.5)
    everyone = jnp.concatenate(
        [preds[pl.ds(q, MEMBERS, stride=4), :] for q in range(4)], axis=1
    )
    mine = jnp.concatenate([own[pl.ds(q, LOCAL, stride=4), :] for q in range(4)], axis=1)
    anomaly = (everyone - jnp.mean(everyone, axis=0, keepdims=True)) * scale
    misfit = given[0:LOCAL, :] - mine
    var = given[LOCAL : LOCAL + 1, :]
    weighted = anomaly / var
    pad = jnp.zeros((6, BLOCK), F32)
    right = jnp.concatenate(
        [anomaly, anomaly[8:], anomaly[16:], anomaly[24:]]
        + [misfit, pad] * 4
        + [jnp.zeros((16, BLOCK), F32)],
        axis=0,
    )
    product = lax.dot_general(
        weighted, right, (((1,), (1,)), ((), ())), precision=lax.Precision.HIGHEST,
        preferred_element_type=F32,
    )
    lane = lax.broadcasted_iota(jnp.int32, (8, 128), 1)
    packed = product[0:8]
    for c, start, stop in ((1, 32, 56), (2, 56, 72), (3, 72, 80)):
        mine = ((lane >= start) & (lane < stop)) | (lane // 8 == 10 + c)
        packed = jnp.where(mine, product[8 * c : 8 * c + 8], packed)
    for d in range(SLABS):
        out[d] = packed


def moments(preds, own, given):
    return pl.pallas_call(
        moments_kernel,
        out_shape=jax.ShapeDtypeStruct((SLABS, 8, 128), F32),
        compiler_params=pltpu.CompilerParams(vmem_limit_bytes=4 * MIB),
        name="moments",
    )(preds, own, given)


def update_kernel(group, arrived, here, there, out):
    parts = [arrived[d] for d in range(SLABS)]
    while len(parts) > 1:
        parts = [x + y for x, y in zip(parts[::2], parts[1::2])]
    packed = parts[0]
    lane8 = lax.broadcasted_iota(jnp.int32, (8, 128), 1)
    uppers, cross = [], []
    for c, start in enumerate((0, 32, 56, 72)):
        moved = pltpu.roll(packed, (8 * c - start) % 128, 1)
        uppers.append(jnp.where((lane8 >= 8 * c) & (lane8 < MEMBERS), moved, 0.0))
        cross.append(pltpu.roll(packed, (MEMBERS - 80 - 8 * c) % 128, 1))
    upper = jnp.concatenate(uppers, axis=0)
    cross = jnp.concatenate(cross, axis=0)
    tall = jnp.concatenate([upper, jnp.zeros((96, 128), F32)], axis=0)
    mirrored = tall.T[0:MEMBERS]
    row = lax.broadcasted_iota(jnp.int32, (MEMBERS, 128), 0)
    lane = lax.broadcasted_iota(jnp.int32, (MEMBERS, 128), 1)
    work = jnp.where(lane // 8 >= row // 8, upper, mirrored)
    work = jnp.where(row == lane, work + 1.0, work)
    work = jnp.where(lane < MEMBERS, work, jnp.where(lane < MEMBERS + LOCAL, cross, 0.0))
    for first in range(0, MEMBERS, 8):
        columns = [
            jnp.broadcast_to(work[:, k : k + 1], (MEMBERS, 128)) for k in range(first, first + 8)
        ]
        for i in range(8):
            k = first + i
            column = columns[i]
            inverse = 1.0 / column[k : k + 1, :]
            line = work[k : k + 1, :] * inverse
            work = jnp.where(row == k, line, work - column * line)
            for later in range(i + 1, 8):
                line = columns[later][k : k + 1, :] * inverse
                columns[later] = jnp.where(row == k, line, columns[later] - column * line)
    mixing = work - jnp.mean(work, axis=0, keepdims=True)
    mixing = mixing * (1.0 / float(MEMBERS - 1) ** 0.5)
    mixing = jnp.where(row - group[0] * LOCAL == lane - MEMBERS, mixing + 1.0, mixing)
    south = group[0] % 2 == 0
    turn = MEMBERS - LOCAL * group[0]
    totals = [jnp.zeros((64, 128), F32) for _ in range(LOCAL)]
    for j in range(LOCAL):
        column = jnp.broadcast_to(mixing[:, MEMBERS + j : MEMBERS + j + 1], (MEMBERS, 128))
        rows = pltpu.roll(column, turn, 0)

        def weight(at_south, at_north):
            at_south, at_north = at_south % MEMBERS, at_north % MEMBERS
            return jnp.where(
                south, rows[at_south : at_south + 1, :], rows[at_north : at_north + 1, :]
            )

        for i, d in enumerate(PARTS):
            for m in range(LOCAL):
                totals[j] = totals[j] + weight(4 * d + m, m - 4 * d) * here[2 * i + m]
                totals[j] = totals[j] + weight(2 + m - 4 * d, 4 * d + m - 2) * there[2 * i + m]
    for j in range(LOCAL):
        out[j] = totals[j]


def update(group, arrived, *fields):
    vmem = pl.BlockSpec(memory_space=pltpu.VMEM)
    return pl.pallas_call(
        update_kernel,
        out_shape=jax.ShapeDtypeStruct((LOCAL, 64, 128), F32),
        in_specs=[pl.BlockSpec(memory_space=pltpu.SMEM)] + [vmem] * 3,
        out_specs=vmem,
        compiler_params=pltpu.CompilerParams(vmem_limit_bytes=4 * MIB),
        name="update",
    )(group, arrived, *fields)


def local(state, theta, forcing, boxes, observed, noise_var, perturb):
    slab = lax.axis_index("slab").astype(jnp.int32).reshape(1)
    group = lax.axis_index("group").astype(jnp.int32).reshape(1)
    first, last = pack(state, theta, forcing)
    low = lax.ppermute(last, "slab", [(i, i + 1) for i in range(SLABS - 1)])
    high = lax.ppermute(first, "slab", [(i + 1, i) for i in range(SLABS - 1)])
    field = theta.reshape(LOCAL, 64, 128)

    def from_chip(value, chips):
        half = GROUPS // 2
        moves = [
            (((y + (1 - 2 * core) * chips) % half) * 2 + core, y * 2 + core)
            for y in range(half)
            for core in range(2)
        ]
        return lax.ppermute(value, "group", moves)

    one = from_chip(field, 1)
    final, part, count, given = window(
        slab, state, theta, forcing, low, high,
        observed.reshape(1, BLOCK), noise_var.reshape(1, BLOCK), perturb, boxes,
    )
    arrived = lax.all_to_all(part, "slab", 0, 0, tiled=True)
    two = from_chip(jnp.concatenate([field, one], axis=0), 2)
    copies, own = own_predictions(arrived, count)
    preds = lax.all_to_all(copies, "group", 0, 0, tiled=True).reshape(GROUPS * 8, 128)
    back = from_chip(jnp.concatenate([field, one, two[:LOCAL]], axis=0), -3)
    far = from_chip(two[LOCAL:], 1)
    sums = moments(preds, own, given)
    sums = lax.all_to_all(sums, "slab", 0, 0, tiled=True)
    here = jnp.concatenate([field, one, two, back, far], axis=0)
    there = lax.ppermute(here, "group", [(i, i ^ 1) for i in range(GROUPS)])
    updated = update(group, sums, here, there)
    return final, updated.reshape(theta.shape)


def solution(mesh):
    return jax.shard_map(
        local,
        mesh=mesh,
        in_specs=(
            P("group", "slab", None, None),
            P("group", "slab", None, None),
            P("slab", None, None),
            P(),
            P("slab"),
            P("slab"),
            P("group", "slab"),
        ),
        out_specs=(P("group", "slab", None, None), P("group", "slab", None, None)),
        check_vma=False,
    )
```

```python
import jax
import jax.numpy as jnp
from jax import lax
from jax.experimental import pallas as pl
from jax.experimental.pallas import tpu as pltpu
from jax.sharding import PartitionSpec as P


STEP_SIZE = 0.1
F32 = jnp.float32
BF16 = jnp.bfloat16

LOCAL = 2
PLANES = 8
ROWS = 32
COLS = 256
COARSE = 4
SLABS = 32
GROUPS = 16
MEMBERS = 32
BLOCK = 512
MIB = 1 << 20
PARTS = (0, 2, 4, 6, 1, 3, 5, 7)
HALO_ROWS = 176


def split3(value):
    a = value.astype(BF16)
    rest = value - a.astype(F32)
    b = rest.astype(BF16)
    c = (rest - b.astype(F32)).astype(BF16)
    return a, b, c


def pack_kernel(state, theta, forcing, first, last, sems):
    copies = []

    def copy(src, dst):
        copies.append(pltpu.make_async_copy(src, dst, sems.at[len(copies)]))

    for out, plane, coarse, force in ((first, 0, 0, 0), (last, PLANES - 2, COARSE - 1, PLANES - 1)):
        for m in range(LOCAL):
            for p in range(2):
                at = (m * 2 + p) * ROWS
                copy(state.at[m, plane + p], out.at[pl.ds(at, ROWS), :])
            copy(theta.at[m, coarse], out.at[pl.ds(160, 16), pl.ds(m * 128, 128)])
        copy(forcing.at[force], out.at[pl.ds(128, ROWS), :])
    for c in copies:
        c.start()
    for c in copies:
        c.wait()


def pack(state, theta, forcing):
    shape = jax.ShapeDtypeStruct((HALO_ROWS, COLS), F32)
    vmem = pl.BlockSpec(memory_space=pltpu.VMEM)
    return pl.pallas_call(
        pack_kernel,
        out_shape=(shape, shape),
        in_specs=[pl.BlockSpec(memory_space=pltpu.HBM)] * 3,
        out_specs=(vmem, vmem),
        compiler_params=pltpu.CompilerParams(vmem_limit_bytes=2 * MIB),
        scratch_shapes=[pltpu.SemaphoreType.DMA((14,))],
        name="pack",
    )(*(pltpu.with_memory_space_constraint(a, pltpu.HBM) for a in (state, theta, forcing)))


def window_kernel(
    slab, state, theta, forcing, low, high, observed, noise, perturb, footprints,
    final, part, count, given, diff, mid, fresh, done, boxes, target, spread, draws, sems,
):
    enter = [
        pltpu.make_async_copy(src, dst, sems.at[i])
        for i, (src, dst) in enumerate(
            ((footprints, boxes), (observed, target), (noise, spread), (perturb, draws))
        )
    ]
    for e in enter:
        e.start()
    s = slab[0]
    keep_low = jnp.where(s > 0, 0.5, 0.0).astype(F32)
    keep_high = jnp.where(s < SLABS - 1, 0.5, 0.0).astype(F32)
    pieces = []
    for m in range(LOCAL):
        pieces.append(keep_low * jnp.exp(low[160:176, m * 128 : (m + 1) * 128]))
        for c in range(COARSE):
            pieces.append(0.5 * jnp.exp(theta[m, c]))
        pieces.append(keep_high * jnp.exp(high[160:176, m * 128 : (m + 1) * 128]))
    coarse = jnp.concatenate(pieces, axis=0)
    up = (
        lax.broadcasted_iota(jnp.int32, (128, COLS), 1) // 2
        == lax.broadcasted_iota(jnp.int32, (128, COLS), 0)
    ).astype(F32).astype(BF16)
    wide = sum(jnp.dot(part_, up, preferred_element_type=F32) for part_ in split3(coarse))
    rows = LOCAL * (COARSE + 2) * 16
    for h in range(2):
        diff[h, pl.ds(0, rows, stride=2), :] = wide[:, h * 128 : (h + 1) * 128]
        diff[h, pl.ds(1, rows, stride=2), :] = wide[:, h * 128 : (h + 1) * 128]

    row = lax.broadcasted_iota(jnp.int32, (ROWS, COLS), 0)
    col = lax.broadcasted_iota(jnp.int32, (ROWS, COLS), 1)

    def step(below, center, above, d, f):
        beside = above + below
        beside = beside + jnp.where(row == ROWS - 1, 0.0, pltpu.roll(center, ROWS - 1, 0))
        beside = beside + jnp.where(row == 0, 0.0, pltpu.roll(center, 1, 0))
        beside = beside + jnp.where(col == COLS - 1, 0.0, pltpu.roll(center, COLS - 1, 1))
        beside = beside + jnp.where(col == 0, 0.0, pltpu.roll(center, 1, 1))
        change = d * (beside - 6.0 * center) + 0.5 * center * (1.0 - center * center) + f
        return center + STEP_SIZE * change

    def plane(m, p):
        if p < 0:
            at = (m * 2 + p + 2) * ROWS
            return low[at : at + ROWS, :]
        if p >= PLANES:
            at = (m * 2 + p - PLANES) * ROWS
            return high[at : at + ROWS, :]
        return state[m, p]

    def force(p):
        if p < 0:
            return low[128:160, :]
        if p >= PLANES:
            return high[128:160, :]
        return forcing[p]

    def diffusivity(m, p):
        at = (m * (COARSE + 2) + (p + 2) // 2) * ROWS
        return jnp.concatenate([diff[h, at : at + ROWS, :] for h in range(2)], axis=1)

    for m in range(LOCAL):
        for p in range(-1, PLANES + 1):
            mid[m * (PLANES + 2) + p + 1] = step(
                plane(m, p - 1), plane(m, p), plane(m, p + 1), diffusivity(m, p), force(p)
            )
        for p in range(PLANES):
            at = m * (PLANES + 2) + p
            new = step(mid[at], mid[at + 1], mid[at + 2], diffusivity(m, p), forcing[p])
            fresh[m, p] = new
            to = (m * PLANES + p) * ROWS
            for h in range(2):
                done[h, to : to + ROWS, :] = new[:, h * 128 : (h + 1) * 128]

    leave = pltpu.make_async_copy(fresh, final, sems.at[4])
    leave.start()

    tall = LOCAL * PLANES * 8
    sums = jnp.concatenate(
        [sum(done[h, pl.ds(q, tall, stride=4), :] for q in range(4)) for h in range(2)], axis=1
    )
    fold = (
        lax.broadcasted_iota(jnp.int32, (COLS, 128), 0) // 4
        == lax.broadcasted_iota(jnp.int32, (COLS, 128), 1) % 64
    ).astype(F32).astype(BF16)
    tiles = sum(jnp.dot(part_, fold, preferred_element_type=F32) for part_ in split3(sums))
    top = tiles.astype(BF16).astype(F32)
    lane = lax.broadcasted_iota(jnp.int32, (tall, 128), 1)
    left = jnp.where(lane < 64, top, tiles - top).astype(BF16)

    for e in enter:
        e.wait()
    iota_x = lax.broadcasted_iota(jnp.int32, (64, BLOCK), 0)
    iota_y = lax.broadcasted_iota(jnp.int32, (8, BLOCK), 0)

    def observe(d, carry):
        here = pl.ds(pl.multiple_of(d * BLOCK, BLOCK), BLOCK)
        b = boxes[:, here]
        in_x = ((iota_x >= b[4:5]) & (iota_x < b[5:6])).astype(F32).astype(BF16)
        along = jnp.dot(left, jnp.concatenate([in_x, in_x], axis=0), preferred_element_type=F32)
        z0 = jnp.broadcast_to(b[0:1], (8, BLOCK)) - s * PLANES
        z1 = jnp.broadcast_to(b[1:2], (8, BLOCK)) - s * PLANES
        in_y = (iota_y >= b[2:3]) & (iota_y < b[3:4])
        sums = [jnp.zeros((8, BLOCK), F32) for _ in range(LOCAL)]
        for z in range(PLANES):
            in_z = (z0 <= z) & (z1 > z)
            for m in range(LOCAL):
                at = (m * PLANES + z) * 8
                sums[m] = sums[m] + jnp.where(in_z, along[at : at + 8], 0.0)
        for m in range(LOCAL):
            total = jnp.sum(jnp.where(in_y, sums[m], 0.0), axis=0, keepdims=True)
            for q in range(4):
                part[d, m * 4 + q : m * 4 + q + 1, :] = total[:, q * 128 : (q + 1) * 128]
        return carry

    lax.fori_loop(0, SLABS, observe, 0, unroll=4)

    b = boxes[:, pl.ds(pl.multiple_of(s * BLOCK, BLOCK), BLOCK)]
    cells = ((b[1:2] - b[0:1]) * (b[3:4] - b[2:3]) * (b[5:6] - b[4:5]) * 16).astype(F32)
    for m in range(LOCAL):
        for q in range(4):
            count[m * 4 + q : m * 4 + q + 1, :] = cells[:, q * 128 : (q + 1) * 128]
    var = spread[...]
    given[0:LOCAL, :] = target[...] + jnp.sqrt(var) * draws[...]
    given[LOCAL : LOCAL + 1, :] = var
    given[LOCAL + 1 : 8, :] = jnp.zeros((5, BLOCK), F32)
    leave.wait()


def window(slab, state, theta, forcing, low, high, *kept):
    vmem = pl.BlockSpec(memory_space=pltpu.VMEM)
    return pl.pallas_call(
        window_kernel,
        out_shape=(
            jax.ShapeDtypeStruct(state.shape, F32),
            jax.ShapeDtypeStruct((SLABS, 8, 128), F32),
            jax.ShapeDtypeStruct((8, 128), F32),
            jax.ShapeDtypeStruct((8, BLOCK), F32),
        ),
        in_specs=[pl.BlockSpec(memory_space=pltpu.SMEM)]
        + [vmem] * 5
        + [pl.BlockSpec(memory_space=pltpu.HBM)] * 4,
        out_specs=(pl.BlockSpec(memory_space=pltpu.HBM), vmem, vmem, vmem),
        compiler_params=pltpu.CompilerParams(vmem_limit_bytes=12 * MIB),
        scratch_shapes=[
            pltpu.VMEM((2, LOCAL * (COARSE + 2) * ROWS, 128), F32),
            pltpu.VMEM((LOCAL * (PLANES + 2), ROWS, COLS), F32),
            pltpu.VMEM((LOCAL, PLANES, ROWS, COLS), F32),
            pltpu.VMEM((2, LOCAL * PLANES * ROWS, 128), F32),
            pltpu.VMEM(kept[-1].shape, jnp.int32),
            pltpu.VMEM((1, BLOCK), F32),
            pltpu.VMEM((1, BLOCK), F32),
            pltpu.VMEM((LOCAL, BLOCK), F32),
            pltpu.SemaphoreType.DMA((5,)),
        ],
        name="window",
    )(
        slab, state, theta, forcing, low, high,
        *(pltpu.with_memory_space_constraint(a, pltpu.HBM) for a in kept),
    )


def gather_kernel(arrived, count, copies, own):
    pred = jnp.sum(arrived[...], axis=0) / count[...]
    own[...] = pred
    for g in range(GROUPS):
        copies[g] = pred


def own_predictions(arrived, count):
    return pl.pallas_call(
        gather_kernel,
        out_shape=(
            jax.ShapeDtypeStruct((GROUPS, 8, 128), F32),
            jax.ShapeDtypeStruct((8, 128), F32),
        ),
        compiler_params=pltpu.CompilerParams(vmem_limit_bytes=4 * MIB),
        name="own_predictions",
    )(arrived, count)


def moments_kernel(preds, own, given, out):
    scale = 1.0 / (float(MEMBERS - 1) ** 0.5)
    everyone = jnp.concatenate(
        [preds[pl.ds(q, MEMBERS, stride=4), :] for q in range(4)], axis=1
    )
    mine = jnp.concatenate([own[pl.ds(q, LOCAL, stride=4), :] for q in range(4)], axis=1)
    anomaly = (everyone - jnp.mean(everyone, axis=0, keepdims=True)) * scale
    misfit = given[0:LOCAL, :] - mine
    var = given[LOCAL : LOCAL + 1, :]
    weighted = anomaly / var
    pad = jnp.zeros((6, BLOCK), F32)
    right = jnp.concatenate(
        [anomaly, anomaly[8:], anomaly[16:], anomaly[24:]]
        + [misfit, pad] * 4
        + [jnp.zeros((16, BLOCK), F32)],
        axis=0,
    )
    product = lax.dot_general(
        weighted, right, (((1,), (1,)), ((), ())), precision=lax.Precision.HIGHEST,
        preferred_element_type=F32,
    )
    lane = lax.broadcasted_iota(jnp.int32, (8, 128), 1)
    packed = product[0:8]
    for c, start, stop in ((1, 32, 56), (2, 56, 72), (3, 72, 80)):
        mine = ((lane >= start) & (lane < stop)) | (lane // 8 == 10 + c)
        packed = jnp.where(mine, product[8 * c : 8 * c + 8], packed)
    for d in range(SLABS):
        out[d] = packed


def moments(preds, own, given):
    return pl.pallas_call(
        moments_kernel,
        out_shape=jax.ShapeDtypeStruct((SLABS, 8, 128), F32),
        compiler_params=pltpu.CompilerParams(vmem_limit_bytes=4 * MIB),
        name="moments",
    )(preds, own, given)


def update_kernel(group, arrived, here, there, out):
    parts = [arrived[d] for d in range(SLABS)]
    while len(parts) > 1:
        parts = [x + y for x, y in zip(parts[::2], parts[1::2])]
    packed = parts[0]
    lane8 = lax.broadcasted_iota(jnp.int32, (8, 128), 1)
    uppers, cross = [], []
    for c, start in enumerate((0, 32, 56, 72)):
        moved = pltpu.roll(packed, (8 * c - start) % 128, 1)
        uppers.append(jnp.where((lane8 >= 8 * c) & (lane8 < MEMBERS), moved, 0.0))
        cross.append(pltpu.roll(packed, (MEMBERS - 80 - 8 * c) % 128, 1))
    upper = jnp.concatenate(uppers, axis=0)
    cross = jnp.concatenate(cross, axis=0)
    tall = jnp.concatenate([upper, jnp.zeros((96, 128), F32)], axis=0)
    mirrored = tall.T[0:MEMBERS]
    row = lax.broadcasted_iota(jnp.int32, (MEMBERS, 128), 0)
    lane = lax.broadcasted_iota(jnp.int32, (MEMBERS, 128), 1)
    work = jnp.where(lane // 8 >= row // 8, upper, mirrored)
    work = jnp.where(row == lane, work + 1.0, work)
    work = jnp.where(lane < MEMBERS, work, jnp.where(lane < MEMBERS + LOCAL, cross, 0.0))
    for first in range(0, MEMBERS, 8):
        columns = [
            jnp.broadcast_to(work[:, k : k + 1], (MEMBERS, 128)) for k in range(first, first + 8)
        ]
        for i in range(8):
            k = first + i
            column = columns[i]
            inverse = 1.0 / column[k : k + 1, :]
            line = work[k : k + 1, :] * inverse
            work = jnp.where(row == k, line, work - column * line)
            for later in range(i + 1, 8):
                line = columns[later][k : k + 1, :] * inverse
                columns[later] = jnp.where(row == k, line, columns[later] - column * line)
    mixing = work - jnp.mean(work, axis=0, keepdims=True)
    mixing = mixing * (1.0 / float(MEMBERS - 1) ** 0.5)
    mixing = jnp.where(row - group[0] * LOCAL == lane - MEMBERS, mixing + 1.0, mixing)
    south = group[0] % 2 == 0
    turn = MEMBERS - LOCAL * group[0]
    totals = [jnp.zeros((64, 128), F32) for _ in range(LOCAL)]
    for j in range(LOCAL):
        column = jnp.broadcast_to(mixing[:, MEMBERS + j : MEMBERS + j + 1], (MEMBERS, 128))
        rows = pltpu.roll(column, turn, 0)

        def weight(at_south, at_north):
            at_south, at_north = at_south % MEMBERS, at_north % MEMBERS
            return jnp.where(
                south, rows[at_south : at_south + 1, :], rows[at_north : at_north + 1, :]
            )

        for i, d in enumerate(PARTS):
            for m in range(LOCAL):
                totals[j] = totals[j] + weight(4 * d + m, m - 4 * d) * here[2 * i + m]
                totals[j] = totals[j] + weight(2 + m - 4 * d, 4 * d + m - 2) * there[2 * i + m]
    for j in range(LOCAL):
        out[j] = totals[j]


def update(group, arrived, *fields):
    vmem = pl.BlockSpec(memory_space=pltpu.VMEM)
    return pl.pallas_call(
        update_kernel,
        out_shape=jax.ShapeDtypeStruct((LOCAL, 64, 128), F32),
        in_specs=[pl.BlockSpec(memory_space=pltpu.SMEM)] + [vmem] * 3,
        out_specs=vmem,
        compiler_params=pltpu.CompilerParams(vmem_limit_bytes=4 * MIB),
        name="update",
    )(group, arrived, *fields)


def local(state, theta, forcing, boxes, observed, noise_var, perturb):
    slab = lax.axis_index("slab").astype(jnp.int32).reshape(1)
    group = lax.axis_index("group").astype(jnp.int32).reshape(1)
    first, last = pack(state, theta, forcing)
    low = lax.ppermute(last, "slab", [(i, i + 1) for i in range(SLABS - 1)])
    high = lax.ppermute(first, "slab", [(i + 1, i) for i in range(SLABS - 1)])
    field = theta.reshape(LOCAL, 64, 128)

    def from_chip(value, chips):
        half = GROUPS // 2
        moves = [
            (((y + (1 - 2 * core) * chips) % half) * 2 + core, y * 2 + core)
            for y in range(half)
            for core in range(2)
        ]
        return lax.ppermute(value, "group", moves)

    pair = from_chip(field, 2)
    final, part, count, given = window(
        slab, state, theta, forcing, low, high,
        observed.reshape(1, BLOCK), noise_var.reshape(1, BLOCK), perturb, boxes,
    )
    arrived = lax.all_to_all(part, "slab", 0, 0, tiled=True)
    pair = jnp.concatenate([field, pair], axis=0)
    across = from_chip(pair, 4)
    copies, own = own_predictions(arrived, count)
    preds = lax.all_to_all(copies, "group", 0, 0, tiled=True).reshape(GROUPS * 8, 128)
    even = jnp.concatenate([pair, across], axis=0)
    odd = from_chip(even, 1)
    sums = moments(preds, own, given)
    sums = lax.all_to_all(sums, "slab", 0, 0, tiled=True)
    here = jnp.concatenate([even, odd], axis=0)
    there = lax.ppermute(here, "group", [(i, i ^ 1) for i in range(GROUPS)])
    updated = update(group, sums, here, there)
    return final, updated.reshape(theta.shape)


def solution(mesh):
    return jax.shard_map(
        local,
        mesh=mesh,
        in_specs=(
            P("group", "slab", None, None),
            P("group", "slab", None, None),
            P("slab", None, None),
            P(),
            P("slab"),
            P("slab"),
            P("group", "slab"),
        ),
        out_specs=(P("group", "slab", None, None), P("group", "slab", None, None)),
        check_vma=False,
    )
```

```python
import jax
import jax.numpy as jnp
from jax import lax
from jax.experimental import pallas as pl
from jax.experimental.pallas import tpu as pltpu
from jax.sharding import PartitionSpec as P


STEP_SIZE = 0.1
F32 = jnp.float32
BF16 = jnp.bfloat16

LOCAL = 2
PLANES = 8
ROWS = 32
COLS = 256
COARSE = 4
SLABS = 32
GROUPS = 16
MEMBERS = 32
BLOCK = 512
OBS = SLABS * BLOCK
MIB = 1 << 20
PARTS = (0, 2, 4, 6, 1, 3, 5, 7)
HALO_ROWS = 176


def split3(value):
    a = value.astype(BF16)
    rest = value - a.astype(F32)
    b = rest.astype(BF16)
    c = (rest - b.astype(F32)).astype(BF16)
    return a, b, c


def pack_kernel(state, theta, forcing, first, last, sems):
    copies = []

    def copy(src, dst):
        copies.append(pltpu.make_async_copy(src, dst, sems.at[len(copies)]))

    for out, plane, coarse, force in ((first, 0, 0, 0), (last, PLANES - 2, COARSE - 1, PLANES - 1)):
        for m in range(LOCAL):
            for p in range(2):
                at = (m * 2 + p) * ROWS
                copy(state.at[m, plane + p], out.at[pl.ds(at, ROWS), :])
            copy(theta.at[m, coarse], out.at[pl.ds(160, 16), pl.ds(m * 128, 128)])
        copy(forcing.at[force], out.at[pl.ds(128, ROWS), :])
    for c in copies:
        c.start()
    for c in copies:
        c.wait()


def pack(state, theta, forcing):
    shape = jax.ShapeDtypeStruct((HALO_ROWS, COLS), F32)
    vmem = pl.BlockSpec(memory_space=pltpu.VMEM)
    return pl.pallas_call(
        pack_kernel,
        out_shape=(shape, shape),
        in_specs=[pl.BlockSpec(memory_space=pltpu.HBM)] * 3,
        out_specs=(vmem, vmem),
        compiler_params=pltpu.CompilerParams(vmem_limit_bytes=2 * MIB),
        scratch_shapes=[pltpu.SemaphoreType.DMA((14,))],
        name="pack",
    )(*(pltpu.with_memory_space_constraint(a, pltpu.HBM) for a in (state, theta, forcing)))


def masks_kernel(
    slab, observed, noise, perturb, footprints, state, theta, forcing,
    in_x, in_z, in_y, count, given, state_here, theta_here, forcing_here,
    boxes, target, spread, draws, sems,
):
    quarter = OBS // 4
    chunks = [pl.ds(i * quarter, quarter) for i in range(4)]
    enter = [
        pltpu.make_async_copy(footprints.at[:, c], boxes.at[:, c], sems.at[i])
        for i, c in enumerate(chunks)
    ]
    small = [
        pltpu.make_async_copy(src, dst, sems.at[4 + i])
        for i, (src, dst) in enumerate(
            (
                (observed, target),
                (noise, spread),
                (perturb, draws),
                (state, state_here),
                (theta, theta_here),
                (forcing, forcing_here),
            )
        )
    ]
    for e in enter + small:
        e.start()
    first = slab[0] * PLANES
    iota_x = lax.broadcasted_iota(jnp.int32, (64, BLOCK), 0)
    iota = lax.broadcasted_iota(jnp.int32, (8, BLOCK), 0)
    for i, e in enumerate(enter):
        e.wait()

        def build(d, carry):
            at = pl.ds(pl.multiple_of(i * quarter + d * BLOCK, BLOCK), BLOCK)
            b = boxes[:, at]
            in_x[:, at] = ((iota_x >= b[4:5]) & (iota_x < b[5:6])).astype(F32).astype(BF16)
            in_z[:, at] = ((iota + first >= b[0:1]) & (iota + first < b[1:2])).astype(F32)
            in_y[:, at] = ((iota >= b[2:3]) & (iota < b[3:4])).astype(F32)
            return carry

        lax.fori_loop(0, quarter // BLOCK, build, 0, unroll=8)
    b = boxes[:, pl.ds(pl.multiple_of(slab[0] * BLOCK, BLOCK), BLOCK)]
    cells = ((b[1:2] - b[0:1]) * (b[3:4] - b[2:3]) * (b[5:6] - b[4:5]) * 16).astype(F32)
    for m in range(LOCAL):
        for q in range(4):
            count[m * 4 + q : m * 4 + q + 1, :] = cells[:, q * 128 : (q + 1) * 128]
    for e in small:
        e.wait()
    var = spread[...]
    given[0:LOCAL, :] = target[...] + jnp.sqrt(var) * draws[...]
    given[LOCAL : LOCAL + 1, :] = var
    given[LOCAL + 1 : 8, :] = jnp.zeros((5, BLOCK), F32)


def masks(slab, *kept):
    vmem = pl.BlockSpec(memory_space=pltpu.VMEM)
    return pl.pallas_call(
        masks_kernel,
        out_shape=(
            jax.ShapeDtypeStruct((64, OBS), BF16),
            jax.ShapeDtypeStruct((8, OBS), F32),
            jax.ShapeDtypeStruct((8, OBS), F32),
            jax.ShapeDtypeStruct((8, 128), F32),
            jax.ShapeDtypeStruct((8, BLOCK), F32),
            *(jax.ShapeDtypeStruct(a.shape, F32) for a in kept[-3:]),
        ),
        in_specs=[pl.BlockSpec(memory_space=pltpu.SMEM)]
        + [pl.BlockSpec(memory_space=pltpu.HBM)] * 7,
        out_specs=(vmem,) * 8,
        compiler_params=pltpu.CompilerParams(vmem_limit_bytes=8 * MIB),
        scratch_shapes=[
            pltpu.VMEM((6, OBS), jnp.int32),
            pltpu.VMEM((1, BLOCK), F32),
            pltpu.VMEM((1, BLOCK), F32),
            pltpu.VMEM((LOCAL, BLOCK), F32),
            pltpu.SemaphoreType.DMA((10,)),
        ],
        name="masks",
    )(slab, *(pltpu.with_memory_space_constraint(a, pltpu.HBM) for a in kept))


def window_kernel(
    slab, state, theta, forcing, low, high, in_x, in_z, in_y,
    final, part, diff, mid, fresh, done, sem,
):
    s = slab[0]
    keep_low = jnp.where(s > 0, 0.5, 0.0).astype(F32)
    keep_high = jnp.where(s < SLABS - 1, 0.5, 0.0).astype(F32)
    pieces = []
    for m in range(LOCAL):
        pieces.append(keep_low * jnp.exp(low[160:176, m * 128 : (m + 1) * 128]))
        for c in range(COARSE):
            pieces.append(0.5 * jnp.exp(theta[m, c]))
        pieces.append(keep_high * jnp.exp(high[160:176, m * 128 : (m + 1) * 128]))
    coarse = jnp.concatenate(pieces, axis=0)
    up = (
        lax.broadcasted_iota(jnp.int32, (128, COLS), 1) // 2
        == lax.broadcasted_iota(jnp.int32, (128, COLS), 0)
    ).astype(F32).astype(BF16)
    wide = sum(jnp.dot(part_, up, preferred_element_type=F32) for part_ in split3(coarse))
    rows = LOCAL * (COARSE + 2) * 16
    for h in range(2):
        diff[h, pl.ds(0, rows, stride=2), :] = wide[:, h * 128 : (h + 1) * 128]
        diff[h, pl.ds(1, rows, stride=2), :] = wide[:, h * 128 : (h + 1) * 128]

    row = lax.broadcasted_iota(jnp.int32, (ROWS, COLS), 0)
    col = lax.broadcasted_iota(jnp.int32, (ROWS, COLS), 1)

    def step(below, center, above, d, f):
        beside = above + below
        beside = beside + jnp.where(row == ROWS - 1, 0.0, pltpu.roll(center, ROWS - 1, 0))
        beside = beside + jnp.where(row == 0, 0.0, pltpu.roll(center, 1, 0))
        beside = beside + jnp.where(col == COLS - 1, 0.0, pltpu.roll(center, COLS - 1, 1))
        beside = beside + jnp.where(col == 0, 0.0, pltpu.roll(center, 1, 1))
        change = d * (beside - 6.0 * center) + 0.5 * center * (1.0 - center * center) + f
        return center + STEP_SIZE * change

    def plane(m, p):
        if p < 0:
            at = (m * 2 + p + 2) * ROWS
            return low[at : at + ROWS, :]
        if p >= PLANES:
            at = (m * 2 + p - PLANES) * ROWS
            return high[at : at + ROWS, :]
        return state[m, p]

    def force(p):
        if p < 0:
            return low[128:160, :]
        if p >= PLANES:
            return high[128:160, :]
        return forcing[p]

    def diffusivity(m, p):
        at = (m * (COARSE + 2) + (p + 2) // 2) * ROWS
        return jnp.concatenate([diff[h, at : at + ROWS, :] for h in range(2)], axis=1)

    for m in range(LOCAL):
        for p in range(-1, PLANES + 1):
            mid[m * (PLANES + 2) + p + 1] = step(
                plane(m, p - 1), plane(m, p), plane(m, p + 1), diffusivity(m, p), force(p)
            )
        for p in range(PLANES):
            at = m * (PLANES + 2) + p
            new = step(mid[at], mid[at + 1], mid[at + 2], diffusivity(m, p), forcing[p])
            fresh[m, p] = new
            to = (m * PLANES + p) * ROWS
            for h in range(2):
                done[h, to : to + ROWS, :] = new[:, h * 128 : (h + 1) * 128]

    leave = pltpu.make_async_copy(fresh, final, sem)
    leave.start()

    tall = LOCAL * PLANES * 8
    sums = jnp.concatenate(
        [sum(done[h, pl.ds(q, tall, stride=4), :] for q in range(4)) for h in range(2)], axis=1
    )
    fold = (
        lax.broadcasted_iota(jnp.int32, (COLS, 128), 0) // 4
        == lax.broadcasted_iota(jnp.int32, (COLS, 128), 1) % 64
    ).astype(F32).astype(BF16)
    tiles = sum(jnp.dot(part_, fold, preferred_element_type=F32) for part_ in split3(sums))
    top = tiles.astype(BF16).astype(F32)
    lane = lax.broadcasted_iota(jnp.int32, (tall, 128), 1)
    left = jnp.where(lane < 64, top, tiles - top).astype(BF16)

    def observe(d, carry):
        at = pl.ds(pl.multiple_of(d * BLOCK, BLOCK), BLOCK)
        wide_x = in_x[:, at]
        along = jnp.dot(left, jnp.concatenate([wide_x, wide_x], axis=0), preferred_element_type=F32)
        sums = [jnp.zeros((8, BLOCK), F32) for _ in range(LOCAL)]
        for z in range(PLANES):
            plane_z = jnp.broadcast_to(in_z[z : z + 1, at], (8, BLOCK))
            for m in range(LOCAL):
                row0 = (m * PLANES + z) * 8
                sums[m] = sums[m] + plane_z * along[row0 : row0 + 8]
        rows_y = in_y[:, at]
        for m in range(LOCAL):
            total = jnp.sum(rows_y * sums[m], axis=0, keepdims=True)
            for q in range(4):
                part[d, m * 4 + q : m * 4 + q + 1, :] = total[:, q * 128 : (q + 1) * 128]
        return carry

    lax.fori_loop(0, SLABS, observe, 0, unroll=8)
    leave.wait()


def window(slab, *given):
    vmem = pl.BlockSpec(memory_space=pltpu.VMEM)
    return pl.pallas_call(
        window_kernel,
        out_shape=(
            jax.ShapeDtypeStruct(given[0].shape, F32),
            jax.ShapeDtypeStruct((SLABS, 8, 128), F32),
        ),
        in_specs=[pl.BlockSpec(memory_space=pltpu.SMEM)] + [vmem] * 8,
        out_specs=(pl.BlockSpec(memory_space=pltpu.HBM), vmem),
        compiler_params=pltpu.CompilerParams(vmem_limit_bytes=12 * MIB),
        scratch_shapes=[
            pltpu.VMEM((2, LOCAL * (COARSE + 2) * ROWS, 128), F32),
            pltpu.VMEM((LOCAL * (PLANES + 2), ROWS, COLS), F32),
            pltpu.VMEM((LOCAL, PLANES, ROWS, COLS), F32),
            pltpu.VMEM((2, LOCAL * PLANES * ROWS, 128), F32),
            pltpu.SemaphoreType.DMA,
        ],
        name="window",
    )(slab, *given)


def gather_kernel(arrived, count, copies, own):
    pred = jnp.sum(arrived[...], axis=0) / count[...]
    own[...] = pred
    for g in range(GROUPS):
        copies[g] = pred


def own_predictions(arrived, count):
    return pl.pallas_call(
        gather_kernel,
        out_shape=(
            jax.ShapeDtypeStruct((GROUPS, 8, 128), F32),
            jax.ShapeDtypeStruct((8, 128), F32),
        ),
        compiler_params=pltpu.CompilerParams(vmem_limit_bytes=4 * MIB),
        name="own_predictions",
    )(arrived, count)


def moments_kernel(preds, own, given, out):
    scale = 1.0 / (float(MEMBERS - 1) ** 0.5)
    everyone = jnp.concatenate(
        [preds[pl.ds(q, MEMBERS, stride=4), :] for q in range(4)], axis=1
    )
    mine = jnp.concatenate([own[pl.ds(q, LOCAL, stride=4), :] for q in range(4)], axis=1)
    anomaly = (everyone - jnp.mean(everyone, axis=0, keepdims=True)) * scale
    misfit = given[0:LOCAL, :] - mine
    var = given[LOCAL : LOCAL + 1, :]
    weighted = anomaly / var
    pad = jnp.zeros((6, BLOCK), F32)
    right = jnp.concatenate(
        [anomaly, anomaly[8:], anomaly[16:], anomaly[24:]]
        + [misfit, pad] * 4
        + [jnp.zeros((16, BLOCK), F32)],
        axis=0,
    )
    product = lax.dot_general(
        weighted, right, (((1,), (1,)), ((), ())), precision=lax.Precision.HIGHEST,
        preferred_element_type=F32,
    )
    lane = lax.broadcasted_iota(jnp.int32, (8, 128), 1)
    packed = product[0:8]
    for c, start, stop in ((1, 32, 56), (2, 56, 72), (3, 72, 80)):
        mine = ((lane >= start) & (lane < stop)) | (lane // 8 == 10 + c)
        packed = jnp.where(mine, product[8 * c : 8 * c + 8], packed)
    for d in range(SLABS):
        out[d] = packed


def moments(preds, own, given):
    return pl.pallas_call(
        moments_kernel,
        out_shape=jax.ShapeDtypeStruct((SLABS, 8, 128), F32),
        compiler_params=pltpu.CompilerParams(vmem_limit_bytes=4 * MIB),
        name="moments",
    )(preds, own, given)


def update_kernel(group, arrived, here, there, out):
    parts = [arrived[d] for d in range(SLABS)]
    while len(parts) > 1:
        parts = [x + y for x, y in zip(parts[::2], parts[1::2])]
    packed = parts[0]
    lane8 = lax.broadcasted_iota(jnp.int32, (8, 128), 1)
    uppers, cross = [], []
    for c, start in enumerate((0, 32, 56, 72)):
        moved = pltpu.roll(packed, (8 * c - start) % 128, 1)
        uppers.append(jnp.where((lane8 >= 8 * c) & (lane8 < MEMBERS), moved, 0.0))
        cross.append(pltpu.roll(packed, (MEMBERS - 80 - 8 * c) % 128, 1))
    upper = jnp.concatenate(uppers, axis=0)
    cross = jnp.concatenate(cross, axis=0)
    tall = jnp.concatenate([upper, jnp.zeros((96, 128), F32)], axis=0)
    mirrored = tall.T[0:MEMBERS]
    row = lax.broadcasted_iota(jnp.int32, (MEMBERS, 128), 0)
    lane = lax.broadcasted_iota(jnp.int32, (MEMBERS, 128), 1)
    work = jnp.where(lane // 8 >= row // 8, upper, mirrored)
    work = jnp.where(row == lane, work + 1.0, work)
    work = jnp.where(lane < MEMBERS, work, jnp.where(lane < MEMBERS + LOCAL, cross, 0.0))
    for first in range(0, MEMBERS, 8):
        columns = [
            jnp.broadcast_to(work[:, k : k + 1], (MEMBERS, 128)) for k in range(first, first + 8)
        ]
        for i in range(8):
            k = first + i
            column = columns[i]
            inverse = 1.0 / column[k : k + 1, :]
            line = work[k : k + 1, :] * inverse
            work = jnp.where(row == k, line, work - column * line)
            for later in range(i + 1, 8):
                line = columns[later][k : k + 1, :] * inverse
                columns[later] = jnp.where(row == k, line, columns[later] - column * line)
    mixing = work - jnp.mean(work, axis=0, keepdims=True)
    mixing = mixing * (1.0 / float(MEMBERS - 1) ** 0.5)
    mixing = jnp.where(row - group[0] * LOCAL == lane - MEMBERS, mixing + 1.0, mixing)
    south = group[0] % 2 == 0
    turn = MEMBERS - LOCAL * group[0]
    totals = [jnp.zeros((64, 128), F32) for _ in range(LOCAL)]
    for j in range(LOCAL):
        column = jnp.broadcast_to(mixing[:, MEMBERS + j : MEMBERS + j + 1], (MEMBERS, 128))
        rows = pltpu.roll(column, turn, 0)

        def weight(at_south, at_north):
            at_south, at_north = at_south % MEMBERS, at_north % MEMBERS
            return jnp.where(
                south, rows[at_south : at_south + 1, :], rows[at_north : at_north + 1, :]
            )

        for i, d in enumerate(PARTS):
            for m in range(LOCAL):
                totals[j] = totals[j] + weight(4 * d + m, m - 4 * d) * here[2 * i + m]
                totals[j] = totals[j] + weight(2 + m - 4 * d, 4 * d + m - 2) * there[2 * i + m]
    for j in range(LOCAL):
        out[j] = totals[j]


def update(group, arrived, *fields):
    vmem = pl.BlockSpec(memory_space=pltpu.VMEM)
    return pl.pallas_call(
        update_kernel,
        out_shape=jax.ShapeDtypeStruct((LOCAL, 64, 128), F32),
        in_specs=[pl.BlockSpec(memory_space=pltpu.SMEM)] + [vmem] * 3,
        out_specs=vmem,
        compiler_params=pltpu.CompilerParams(vmem_limit_bytes=4 * MIB),
        name="update",
    )(group, arrived, *fields)


def local(state, theta, forcing, boxes, observed, noise_var, perturb):
    slab = lax.axis_index("slab").astype(jnp.int32).reshape(1)
    group = lax.axis_index("group").astype(jnp.int32).reshape(1)
    first, last = pack(state, theta, forcing)
    low = lax.ppermute(last, "slab", [(i, i + 1) for i in range(SLABS - 1)])
    high = lax.ppermute(first, "slab", [(i + 1, i) for i in range(SLABS - 1)])
    field = theta.reshape(LOCAL, 64, 128)

    def from_chip(value, chips):
        half = GROUPS // 2
        moves = [
            (((y + (1 - 2 * core) * chips) % half) * 2 + core, y * 2 + core)
            for y in range(half)
            for core in range(2)
        ]
        return lax.ppermute(value, "group", moves)

    pair = from_chip(field, 2)
    in_x, in_z, in_y, count, given, *fields = masks(
        slab, observed.reshape(1, BLOCK), noise_var.reshape(1, BLOCK), perturb, boxes,
        state, theta, forcing,
    )
    final, part = window(slab, *fields, low, high, in_x, in_z, in_y)
    arrived = lax.all_to_all(part, "slab", 0, 0, tiled=True)
    pair = jnp.concatenate([fields[1].reshape(field.shape), pair], axis=0)
    across = from_chip(pair, 4)
    copies, own = own_predictions(arrived, count)
    preds = lax.all_to_all(copies, "group", 0, 0, tiled=True).reshape(GROUPS * 8, 128)
    even = jnp.concatenate([pair, across], axis=0)
    odd = from_chip(even, 1)
    sums = moments(preds, own, given)
    sums = lax.all_to_all(sums, "slab", 0, 0, tiled=True)
    here = jnp.concatenate([even, odd], axis=0)
    there = lax.ppermute(here, "group", [(i, i ^ 1) for i in range(GROUPS)])
    updated = update(group, sums, here, there)
    return final, updated.reshape(theta.shape)


def solution(mesh):
    return jax.shard_map(
        local,
        mesh=mesh,
        in_specs=(
            P("group", "slab", None, None),
            P("group", "slab", None, None),
            P("slab", None, None),
            P(),
            P("slab"),
            P("slab"),
            P("group", "slab"),
        ),
        out_specs=(P("group", "slab", None, None), P("group", "slab", None, None)),
        check_vma=False,
    )
```

```python
import jax
import jax.numpy as jnp
from jax import lax
from jax.experimental import pallas as pl
from jax.experimental.pallas import tpu as pltpu
from jax.sharding import PartitionSpec as P


STEP_SIZE = 0.1
F32 = jnp.float32
BF16 = jnp.bfloat16

LOCAL = 2
PLANES = 8
ROWS = 32
COLS = 256
COARSE = 4
SLABS = 32
GROUPS = 16
MEMBERS = 32
BLOCK = 512
OBS = SLABS * BLOCK
MIB = 1 << 20
PARTS = (0, 2, 4, 6, 1, 3, 5, 7)
HALO_ROWS = 176


def split3(value):
    a = value.astype(BF16)
    rest = value - a.astype(F32)
    b = rest.astype(BF16)
    c = (rest - b.astype(F32)).astype(BF16)
    return a, b, c


def upsampled(coarse):
    up = (
        lax.broadcasted_iota(jnp.int32, (128, COLS), 1) // 2
        == lax.broadcasted_iota(jnp.int32, (128, COLS), 0)
    ).astype(F32).astype(BF16)
    wide = sum(jnp.dot(part_, up, preferred_element_type=F32) for part_ in split3(coarse))
    return [wide[:, h * 128 : (h + 1) * 128] for h in range(2)]


def spread_rows(ref, coarse, rows):
    for h, half in enumerate(upsampled(coarse)):
        ref[h, pl.ds(0, rows, stride=2), :] = half
        ref[h, pl.ds(1, rows, stride=2), :] = half


def plane_of(ref, at):
    return jnp.concatenate([ref[h, at : at + ROWS, :] for h in range(2)], axis=1)


def step(below, center, above, d, f):
    row = lax.broadcasted_iota(jnp.int32, (ROWS, COLS), 0)
    col = lax.broadcasted_iota(jnp.int32, (ROWS, COLS), 1)
    beside = jnp.where(row == ROWS - 1, 0.0, pltpu.roll(center, ROWS - 1, 0))
    beside = beside + jnp.where(row == 0, 0.0, pltpu.roll(center, 1, 0))
    beside = beside + jnp.where(col == COLS - 1, 0.0, pltpu.roll(center, COLS - 1, 1))
    beside = beside + jnp.where(col == 0, 0.0, pltpu.roll(center, 1, 1))
    for side in (below, above):
        if side is not None:
            beside = beside + side
    change = d * (beside - 6.0 * center) + 0.5 * center * (1.0 - center * center) + f
    return center + STEP_SIZE * change


def store_halves(ref, at, plane):
    for h in range(2):
        ref[h, at : at + ROWS, :] = plane[:, h * 128 : (h + 1) * 128]


def sums_of_four(ref, rows):
    return jnp.concatenate(
        [sum(ref[h, pl.ds(q, rows, stride=4), :] for q in range(4)) for h in range(2)], axis=1
    )


def pack_kernel(state, theta, forcing, first, last, sems):
    copies = []

    def copy(src, dst):
        copies.append(pltpu.make_async_copy(src, dst, sems.at[len(copies)]))

    for out, plane, coarse, force in ((first, 0, 0, 0), (last, PLANES - 2, COARSE - 1, PLANES - 1)):
        for m in range(LOCAL):
            for p in range(2):
                at = (m * 2 + p) * ROWS
                copy(state.at[m, plane + p], out.at[pl.ds(at, ROWS), :])
            copy(theta.at[m, coarse], out.at[pl.ds(160, 16), pl.ds(m * 128, 128)])
        copy(forcing.at[force], out.at[pl.ds(128, ROWS), :])
    for c in copies:
        c.start()
    for c in copies:
        c.wait()


def pack(state, theta, forcing):
    shape = jax.ShapeDtypeStruct((HALO_ROWS, COLS), F32)
    vmem = pl.BlockSpec(memory_space=pltpu.VMEM)
    return pl.pallas_call(
        pack_kernel,
        out_shape=(shape, shape),
        in_specs=[pl.BlockSpec(memory_space=pltpu.HBM)] * 3,
        out_specs=(vmem, vmem),
        compiler_params=pltpu.CompilerParams(vmem_limit_bytes=2 * MIB),
        scratch_shapes=[pltpu.SemaphoreType.DMA((14,))],
        name="pack",
    )(*(pltpu.with_memory_space_constraint(a, pltpu.HBM) for a in (state, theta, forcing)))


def masks_kernel(
    slab, observed, noise, perturb, footprints, state, theta, forcing,
    in_x, in_z, in_y, count, given, state_here, theta_here, forcing_here,
    diff, mid, inner, inner_sums, boxes, target, spread, draws, done, sems,
):
    quarter = OBS // 4
    chunks = [pl.ds(i * quarter, quarter) for i in range(4)]
    enter = [
        pltpu.make_async_copy(footprints.at[:, c], boxes.at[:, c], sems.at[i])
        for i, c in enumerate(chunks)
    ]
    small = [
        pltpu.make_async_copy(src, dst, sems.at[4 + i])
        for i, (src, dst) in enumerate(
            (
                (observed, target),
                (noise, spread),
                (perturb, draws),
                (state, state_here),
                (theta, theta_here),
                (forcing, forcing_here),
            )
        )
    ]
    for e in enter + small:
        e.start()
    first = slab[0] * PLANES
    iota_x = lax.broadcasted_iota(jnp.int32, (64, BLOCK), 0)
    iota = lax.broadcasted_iota(jnp.int32, (8, BLOCK), 0)
    for i, e in enumerate(enter):
        e.wait()

        def build(d, carry):
            at = pl.ds(pl.multiple_of(i * quarter + d * BLOCK, BLOCK), BLOCK)
            b = boxes[:, at]
            in_x[:, at] = ((iota_x >= b[4:5]) & (iota_x < b[5:6])).astype(F32).astype(BF16)
            in_z[:, at] = ((iota + first >= b[0:1]) & (iota + first < b[1:2])).astype(F32)
            in_y[:, at] = ((iota >= b[2:3]) & (iota < b[3:4])).astype(F32)
            return carry

        lax.fori_loop(0, quarter // BLOCK, build, 0, unroll=8)
    b = boxes[:, pl.ds(pl.multiple_of(slab[0] * BLOCK, BLOCK), BLOCK)]
    cells = ((b[1:2] - b[0:1]) * (b[3:4] - b[2:3]) * (b[5:6] - b[4:5]) * 16).astype(F32)
    for m in range(LOCAL):
        for q in range(4):
            count[m * 4 + q : m * 4 + q + 1, :] = cells[:, q * 128 : (q + 1) * 128]
    for e in small:
        e.wait()
    spread_rows(diff, 0.5 * jnp.exp(theta_here[...].reshape(-1, 128)), LOCAL * COARSE * 16)
    for m in range(LOCAL):
        for p in range(PLANES):
            mid[m, p] = step(
                state_here[m, p - 1] if p > 0 else None,
                state_here[m, p],
                state_here[m, p + 1] if p < PLANES - 1 else None,
                plane_of(diff, (m * COARSE + p // 2) * ROWS),
                forcing_here[p],
            )
        for p in range(2, PLANES - 2):
            new = step(
                mid[m, p - 1],
                mid[m, p],
                mid[m, p + 1],
                plane_of(diff, (m * COARSE + p // 2) * ROWS),
                forcing_here[p],
            )
            inner[m, p - 2] = new
            store_halves(done, (m * 4 + p - 2) * ROWS, new)
    inner_sums[...] = sums_of_four(done, LOCAL * 4 * 8)
    var = spread[...]
    given[0:LOCAL, :] = target[...] + jnp.sqrt(var) * draws[...]
    given[LOCAL : LOCAL + 1, :] = var
    given[LOCAL + 1 : 8, :] = jnp.zeros((5, BLOCK), F32)


def masks(slab, *kept):
    vmem = pl.BlockSpec(memory_space=pltpu.VMEM)
    return pl.pallas_call(
        masks_kernel,
        out_shape=(
            jax.ShapeDtypeStruct((64, OBS), BF16),
            jax.ShapeDtypeStruct((8, OBS), F32),
            jax.ShapeDtypeStruct((8, OBS), F32),
            jax.ShapeDtypeStruct((8, 128), F32),
            jax.ShapeDtypeStruct((8, BLOCK), F32),
            *(jax.ShapeDtypeStruct(a.shape, F32) for a in kept[-3:]),
            jax.ShapeDtypeStruct((2, LOCAL * COARSE * ROWS, 128), F32),
            jax.ShapeDtypeStruct((LOCAL, PLANES, ROWS, COLS), F32),
            jax.ShapeDtypeStruct((LOCAL, 4, ROWS, COLS), F32),
            jax.ShapeDtypeStruct((LOCAL * 4 * 8, COLS), F32),
        ),
        in_specs=[pl.BlockSpec(memory_space=pltpu.SMEM)]
        + [pl.BlockSpec(memory_space=pltpu.HBM)] * 7,
        out_specs=(vmem,) * 12,
        compiler_params=pltpu.CompilerParams(vmem_limit_bytes=8 * MIB),
        scratch_shapes=[
            pltpu.VMEM((6, OBS), jnp.int32),
            pltpu.VMEM((1, BLOCK), F32),
            pltpu.VMEM((1, BLOCK), F32),
            pltpu.VMEM((LOCAL, BLOCK), F32),
            pltpu.VMEM((2, LOCAL * 4 * ROWS, 128), F32),
            pltpu.SemaphoreType.DMA((10,)),
        ],
        name="masks",
    )(slab, *(pltpu.with_memory_space_constraint(a, pltpu.HBM) for a in kept))


def window_kernel(
    slab, low, high, in_x, in_z, in_y, state, forcing, diff, mid, inner, inner_sums,
    final, part, outer, edge, done, sems,
):
    middle = pltpu.make_async_copy(inner, final.at[:, pl.ds(2, 4)], sems.at[0])
    middle.start()
    s = slab[0]
    pieces = []
    for m in range(LOCAL):
        for halo, inside in ((low, s > 0), (high, s < SLABS - 1)):
            keep = jnp.where(inside, 0.5, 0.0).astype(F32)
            pieces.append(keep * jnp.exp(halo[160:176, m * 128 : (m + 1) * 128]))
    spread_rows(outer, jnp.concatenate(pieces, axis=0), LOCAL * 2 * 16)

    def own(m, p):
        return plane_of(diff, (m * COARSE + p // 2) * ROWS)

    leaving = []
    for m in range(LOCAL):
        below = [low[(m * 2 + p) * ROWS : (m * 2 + p + 1) * ROWS, :] for p in range(2)]
        above = [high[(m * 2 + p) * ROWS : (m * 2 + p + 1) * ROWS, :] for p in range(2)]
        ahead = step(
            below[0], below[1], state[m, 0], plane_of(outer, m * 2 * ROWS), low[128:160, :]
        )
        behind = step(
            state[m, PLANES - 1], above[0], above[1], plane_of(outer, (m * 2 + 1) * ROWS),
            high[128:160, :],
        )
        bottom = mid[m, 0] + STEP_SIZE * (own(m, 0) * below[1])
        top = mid[m, PLANES - 1] + STEP_SIZE * (own(m, PLANES - 1) * above[0])
        news = (
            step(ahead, bottom, mid[m, 1], own(m, 0), forcing[0]),
            step(bottom, mid[m, 1], mid[m, 2], own(m, 1), forcing[1]),
            step(mid[m, 5], mid[m, 6], top, own(m, 6), forcing[6]),
            step(mid[m, 6], top, behind, own(m, 7), forcing[7]),
        )
        for i, new in enumerate(news):
            edge[m, i // 2, i % 2] = new
            store_halves(done, (m * 4 + i) * ROWS, new)
        for i in range(2):
            leaving.append(
                pltpu.make_async_copy(
                    edge.at[m, i], final.at[m, pl.ds(6 * i, 2)], sems.at[1 + 2 * m + i]
                )
            )
            leaving[-1].start()

    tall = LOCAL * PLANES * 8
    outer_sums = sums_of_four(done, LOCAL * 4 * 8)
    inside = inner_sums[...]
    sums = jnp.concatenate(
        [
            x
            for m in range(LOCAL)
            for x in (
                outer_sums[m * 32 : m * 32 + 16],
                inside[m * 32 : m * 32 + 32],
                outer_sums[m * 32 + 16 : m * 32 + 32],
            )
        ],
        axis=0,
    )
    fold = (
        lax.broadcasted_iota(jnp.int32, (COLS, 128), 0) // 4
        == lax.broadcasted_iota(jnp.int32, (COLS, 128), 1) % 64
    ).astype(F32).astype(BF16)
    tiles = sum(jnp.dot(part_, fold, preferred_element_type=F32) for part_ in split3(sums))
    top = tiles.astype(BF16).astype(F32)
    lane = lax.broadcasted_iota(jnp.int32, (tall, 128), 1)
    left = jnp.where(lane < 64, top, tiles - top).astype(BF16)

    def observe(d, carry):
        at = pl.ds(pl.multiple_of(d * BLOCK, BLOCK), BLOCK)
        wide_x = in_x[:, at]
        along = jnp.dot(left, jnp.concatenate([wide_x, wide_x], axis=0), preferred_element_type=F32)
        sums = [jnp.zeros((8, BLOCK), F32) for _ in range(LOCAL)]
        for z in range(PLANES):
            plane_z = jnp.broadcast_to(in_z[z : z + 1, at], (8, BLOCK))
            for m in range(LOCAL):
                row0 = (m * PLANES + z) * 8
                sums[m] = sums[m] + plane_z * along[row0 : row0 + 8]
        rows_y = in_y[:, at]
        for m in range(LOCAL):
            total = jnp.sum(rows_y * sums[m], axis=0, keepdims=True)
            for q in range(4):
                part[d, m * 4 + q : m * 4 + q + 1, :] = total[:, q * 128 : (q + 1) * 128]
        return carry

    lax.fori_loop(0, SLABS, observe, 0, unroll=8)
    middle.wait()
    for copy in leaving:
        copy.wait()


def window(slab, *given):
    vmem = pl.BlockSpec(memory_space=pltpu.VMEM)
    return pl.pallas_call(
        window_kernel,
        out_shape=(
            jax.ShapeDtypeStruct((LOCAL, PLANES, ROWS, COLS), F32),
            jax.ShapeDtypeStruct((SLABS, 8, 128), F32),
        ),
        in_specs=[pl.BlockSpec(memory_space=pltpu.SMEM)] + [vmem] * 11,
        out_specs=(pl.BlockSpec(memory_space=pltpu.HBM), vmem),
        compiler_params=pltpu.CompilerParams(vmem_limit_bytes=8 * MIB),
        scratch_shapes=[
            pltpu.VMEM((2, LOCAL * 2 * ROWS, 128), F32),
            pltpu.VMEM((LOCAL, 2, 2, ROWS, COLS), F32),
            pltpu.VMEM((2, LOCAL * 4 * ROWS, 128), F32),
            pltpu.SemaphoreType.DMA((5,)),
        ],
        name="window",
    )(slab, *given)


def gather_kernel(arrived, count, copies, own):
    pred = jnp.sum(arrived[...], axis=0) / count[...]
    own[...] = pred
    for g in range(GROUPS):
        copies[g] = pred


def own_predictions(arrived, count):
    return pl.pallas_call(
        gather_kernel,
        out_shape=(
            jax.ShapeDtypeStruct((GROUPS, 8, 128), F32),
            jax.ShapeDtypeStruct((8, 128), F32),
        ),
        compiler_params=pltpu.CompilerParams(vmem_limit_bytes=4 * MIB),
        name="own_predictions",
    )(arrived, count)


def moments_kernel(preds, own, given, out):
    scale = 1.0 / (float(MEMBERS - 1) ** 0.5)
    everyone = jnp.concatenate(
        [preds[pl.ds(q, MEMBERS, stride=4), :] for q in range(4)], axis=1
    )
    mine = jnp.concatenate([own[pl.ds(q, LOCAL, stride=4), :] for q in range(4)], axis=1)
    anomaly = (everyone - jnp.mean(everyone, axis=0, keepdims=True)) * scale
    misfit = given[0:LOCAL, :] - mine
    var = given[LOCAL : LOCAL + 1, :]
    weighted = anomaly / var
    pad = jnp.zeros((6, BLOCK), F32)
    right = jnp.concatenate(
        [anomaly, anomaly[8:], anomaly[16:], anomaly[24:]]
        + [misfit, pad] * 4
        + [jnp.zeros((16, BLOCK), F32)],
        axis=0,
    )
    product = lax.dot_general(
        weighted, right, (((1,), (1,)), ((), ())), precision=lax.Precision.HIGHEST,
        preferred_element_type=F32,
    )
    lane = lax.broadcasted_iota(jnp.int32, (8, 128), 1)
    packed = product[0:8]
    for c, start, stop in ((1, 32, 56), (2, 56, 72), (3, 72, 80)):
        mine = ((lane >= start) & (lane < stop)) | (lane // 8 == 10 + c)
        packed = jnp.where(mine, product[8 * c : 8 * c + 8], packed)
    for d in range(SLABS):
        out[d] = packed


def moments(preds, own, given):
    return pl.pallas_call(
        moments_kernel,
        out_shape=jax.ShapeDtypeStruct((SLABS, 8, 128), F32),
        compiler_params=pltpu.CompilerParams(vmem_limit_bytes=4 * MIB),
        name="moments",
    )(preds, own, given)


def update_kernel(group, arrived, here, there, out):
    parts = [arrived[d] for d in range(SLABS)]
    while len(parts) > 1:
        parts = [x + y for x, y in zip(parts[::2], parts[1::2])]
    packed = parts[0]
    lane8 = lax.broadcasted_iota(jnp.int32, (8, 128), 1)
    uppers, cross = [], []
    for c, start in enumerate((0, 32, 56, 72)):
        moved = pltpu.roll(packed, (8 * c - start) % 128, 1)
        uppers.append(jnp.where((lane8 >= 8 * c) & (lane8 < MEMBERS), moved, 0.0))
        cross.append(pltpu.roll(packed, (MEMBERS - 80 - 8 * c) % 128, 1))
    upper = jnp.concatenate(uppers, axis=0)
    cross = jnp.concatenate(cross, axis=0)
    tall = jnp.concatenate([upper, jnp.zeros((96, 128), F32)], axis=0)
    mirrored = tall.T[0:MEMBERS]
    row = lax.broadcasted_iota(jnp.int32, (MEMBERS, 128), 0)
    lane = lax.broadcasted_iota(jnp.int32, (MEMBERS, 128), 1)
    work = jnp.where(lane // 8 >= row // 8, upper, mirrored)
    work = jnp.where(row == lane, work + 1.0, work)
    work = jnp.where(lane < MEMBERS, work, jnp.where(lane < MEMBERS + LOCAL, cross, 0.0))
    for first in range(0, MEMBERS, 8):
        columns = [
            jnp.broadcast_to(work[:, k : k + 1], (MEMBERS, 128)) for k in range(first, first + 8)
        ]
        for i in range(8):
            k = first + i
            column = columns[i]
            inverse = 1.0 / column[k : k + 1, :]
            line = work[k : k + 1, :] * inverse
            work = jnp.where(row == k, line, work - column * line)
            for later in range(i + 1, 8):
                line = columns[later][k : k + 1, :] * inverse
                columns[later] = jnp.where(row == k, line, columns[later] - column * line)
    mixing = work - jnp.mean(work, axis=0, keepdims=True)
    mixing = mixing * (1.0 / float(MEMBERS - 1) ** 0.5)
    mixing = jnp.where(row - group[0] * LOCAL == lane - MEMBERS, mixing + 1.0, mixing)
    south = group[0] % 2 == 0
    turn = MEMBERS - LOCAL * group[0]
    totals = [jnp.zeros((64, 128), F32) for _ in range(LOCAL)]
    for j in range(LOCAL):
        column = jnp.broadcast_to(mixing[:, MEMBERS + j : MEMBERS + j + 1], (MEMBERS, 128))
        rows = pltpu.roll(column, turn, 0)

        def weight(at_south, at_north):
            at_south, at_north = at_south % MEMBERS, at_north % MEMBERS
            return jnp.where(
                south, rows[at_south : at_south + 1, :], rows[at_north : at_north + 1, :]
            )

        for i, d in enumerate(PARTS):
            for m in range(LOCAL):
                totals[j] = totals[j] + weight(4 * d + m, m - 4 * d) * here[2 * i + m]
                totals[j] = totals[j] + weight(2 + m - 4 * d, 4 * d + m - 2) * there[2 * i + m]
    for j in range(LOCAL):
        out[j] = totals[j]


def update(group, arrived, *fields):
    vmem = pl.BlockSpec(memory_space=pltpu.VMEM)
    return pl.pallas_call(
        update_kernel,
        out_shape=jax.ShapeDtypeStruct((LOCAL, 64, 128), F32),
        in_specs=[pl.BlockSpec(memory_space=pltpu.SMEM)] + [vmem] * 3,
        out_specs=vmem,
        compiler_params=pltpu.CompilerParams(vmem_limit_bytes=4 * MIB),
        name="update",
    )(group, arrived, *fields)


def local(state, theta, forcing, boxes, observed, noise_var, perturb):
    slab = lax.axis_index("slab").astype(jnp.int32).reshape(1)
    group = lax.axis_index("group").astype(jnp.int32).reshape(1)
    first, last = pack(state, theta, forcing)
    low = lax.ppermute(last, "slab", [(i, i + 1) for i in range(SLABS - 1)])
    high = lax.ppermute(first, "slab", [(i + 1, i) for i in range(SLABS - 1)])
    field = theta.reshape(LOCAL, 64, 128)

    def from_chip(value, chips):
        half = GROUPS // 2
        moves = [
            (((y + (1 - 2 * core) * chips) % half) * 2 + core, y * 2 + core)
            for y in range(half)
            for core in range(2)
        ]
        return lax.ppermute(value, "group", moves)

    pair = from_chip(field, 2)
    in_x, in_z, in_y, count, given, state, here, forcing, *inside = masks(
        slab, observed.reshape(1, BLOCK), noise_var.reshape(1, BLOCK), perturb, boxes,
        state, theta, forcing,
    )
    final, part = window(slab, low, high, in_x, in_z, in_y, state, forcing, *inside)
    arrived = lax.all_to_all(part, "slab", 0, 0, tiled=True)
    pair = jnp.concatenate([here.reshape(field.shape), pair], axis=0)
    across = from_chip(pair, 4)
    copies, own = own_predictions(arrived, count)
    preds = lax.all_to_all(copies, "group", 0, 0, tiled=True).reshape(GROUPS * 8, 128)
    even = jnp.concatenate([pair, across], axis=0)
    odd = from_chip(even, 1)
    sums = moments(preds, own, given)
    sums = lax.all_to_all(sums, "slab", 0, 0, tiled=True)
    here = jnp.concatenate([even, odd], axis=0)
    there = lax.ppermute(here, "group", [(i, i ^ 1) for i in range(GROUPS)])
    updated = update(group, sums, here, there)
    return final, updated.reshape(theta.shape)


def solution(mesh):
    return jax.shard_map(
        local,
        mesh=mesh,
        in_specs=(
            P("group", "slab", None, None),
            P("group", "slab", None, None),
            P("slab", None, None),
            P(),
            P("slab"),
            P("slab"),
            P("group", "slab"),
        ),
        out_specs=(P("group", "slab", None, None), P("group", "slab", None, None)),
        check_vma=False,
    )
```

```python
import jax
import jax.numpy as jnp
from jax import lax
from jax.experimental import pallas as pl
from jax.experimental.pallas import tpu as pltpu
from jax.sharding import PartitionSpec as P


STEP_SIZE = 0.1
F32 = jnp.float32
BF16 = jnp.bfloat16

LOCAL = 2
PLANES = 8
ROWS = 32
COLS = 256
COARSE = 4
SLABS = 32
GROUPS = 16
MEMBERS = 32
BLOCK = 512
OBS = SLABS * BLOCK
MIB = 1 << 20
PARTS = (0, 2, 4, 6, 1, 3, 5, 7)
HALO_ROWS = 176


def split3(value):
    a = value.astype(BF16)
    rest = value - a.astype(F32)
    b = rest.astype(BF16)
    c = (rest - b.astype(F32)).astype(BF16)
    return a, b, c


def upsampled(coarse):
    up = (
        lax.broadcasted_iota(jnp.int32, (128, COLS), 1) // 2
        == lax.broadcasted_iota(jnp.int32, (128, COLS), 0)
    ).astype(F32).astype(BF16)
    wide = sum(jnp.dot(part_, up, preferred_element_type=F32) for part_ in split3(coarse))
    return [wide[:, h * 128 : (h + 1) * 128] for h in range(2)]


def spread_rows(ref, coarse, rows):
    for h, half in enumerate(upsampled(coarse)):
        ref[h, pl.ds(0, rows, stride=2), :] = half
        ref[h, pl.ds(1, rows, stride=2), :] = half


def plane_of(ref, at):
    return jnp.concatenate([ref[h, at : at + ROWS, :] for h in range(2)], axis=1)


def step(below, center, above, d, f):
    row = lax.broadcasted_iota(jnp.int32, (ROWS, COLS), 0)
    col = lax.broadcasted_iota(jnp.int32, (ROWS, COLS), 1)
    beside = jnp.where(row == ROWS - 1, 0.0, pltpu.roll(center, ROWS - 1, 0))
    beside = beside + jnp.where(row == 0, 0.0, pltpu.roll(center, 1, 0))
    beside = beside + jnp.where(col == COLS - 1, 0.0, pltpu.roll(center, COLS - 1, 1))
    beside = beside + jnp.where(col == 0, 0.0, pltpu.roll(center, 1, 1))
    for side in (below, above):
        if side is not None:
            beside = beside + side
    change = d * (beside - 6.0 * center) + 0.5 * center * (1.0 - center * center) + f
    return center + STEP_SIZE * change


def store_halves(ref, at, plane):
    for h in range(2):
        ref[h, at : at + ROWS, :] = plane[:, h * 128 : (h + 1) * 128]


def sums_of_four(ref, rows):
    return jnp.concatenate(
        [sum(ref[h, pl.ds(q, rows, stride=4), :] for q in range(4)) for h in range(2)], axis=1
    )


def pack_kernel(state, theta, forcing, first, last, sems):
    copies = []

    def copy(src, dst):
        copies.append(pltpu.make_async_copy(src, dst, sems.at[len(copies)]))

    for out, plane, coarse, force in ((first, 0, 0, 0), (last, PLANES - 2, COARSE - 1, PLANES - 1)):
        for m in range(LOCAL):
            for p in range(2):
                at = (m * 2 + p) * ROWS
                copy(state.at[m, plane + p], out.at[pl.ds(at, ROWS), :])
            copy(theta.at[m, coarse], out.at[pl.ds(160, 16), pl.ds(m * 128, 128)])
        copy(forcing.at[force], out.at[pl.ds(128, ROWS), :])
    for c in copies:
        c.start()
    for c in copies:
        c.wait()


def pack(state, theta, forcing):
    shape = jax.ShapeDtypeStruct((HALO_ROWS, COLS), F32)
    vmem = pl.BlockSpec(memory_space=pltpu.VMEM)
    return pl.pallas_call(
        pack_kernel,
        out_shape=(shape, shape),
        in_specs=[pl.BlockSpec(memory_space=pltpu.HBM)] * 3,
        out_specs=(vmem, vmem),
        compiler_params=pltpu.CompilerParams(vmem_limit_bytes=2 * MIB),
        scratch_shapes=[pltpu.SemaphoreType.DMA((14,))],
        name="pack",
    )(*(pltpu.with_memory_space_constraint(a, pltpu.HBM) for a in (state, theta, forcing)))


def masks_kernel(
    slab, observed, noise, perturb, footprints, state, theta, forcing,
    in_x, in_z, in_y, count, given, state_here, theta_here, forcing_here,
    diff, mid, inner, inner_sums, boxes, target, spread, draws, done, sems,
):
    quarter = OBS // 4
    chunks = [pl.ds(i * quarter, quarter) for i in range(4)]
    enter = [
        pltpu.make_async_copy(footprints.at[:, c], boxes.at[:, c], sems.at[i])
        for i, c in enumerate(chunks)
    ]
    small = [
        pltpu.make_async_copy(src, dst, sems.at[4 + i])
        for i, (src, dst) in enumerate(
            (
                (observed, target),
                (noise, spread),
                (perturb, draws),
                (state, state_here),
                (theta, theta_here),
                (forcing, forcing_here),
            )
        )
    ]
    for e in enter + small:
        e.start()
    first = slab[0] * PLANES
    iota_x = lax.broadcasted_iota(jnp.int32, (64, BLOCK), 0)
    iota = lax.broadcasted_iota(jnp.int32, (8, BLOCK), 0)
    for i, e in enumerate(enter):
        e.wait()

        def build(d, carry):
            at = pl.ds(pl.multiple_of(i * quarter + d * BLOCK, BLOCK), BLOCK)
            b = boxes[:, at]
            in_x[:, at] = ((iota_x >= b[4:5]) & (iota_x < b[5:6])).astype(F32).astype(BF16)
            in_z[:, at] = ((iota + first >= b[0:1]) & (iota + first < b[1:2])).astype(F32)
            in_y[:, at] = ((iota >= b[2:3]) & (iota < b[3:4])).astype(F32)
            return carry

        lax.fori_loop(0, quarter // BLOCK, build, 0, unroll=8)
    b = boxes[:, pl.ds(pl.multiple_of(slab[0] * BLOCK, BLOCK), BLOCK)]
    cells = ((b[1:2] - b[0:1]) * (b[3:4] - b[2:3]) * (b[5:6] - b[4:5]) * 16).astype(F32)
    for m in range(LOCAL):
        for q in range(4):
            count[m * 4 + q : m * 4 + q + 1, :] = cells[:, q * 128 : (q + 1) * 128]
    for e in small:
        e.wait()
    spread_rows(diff, 0.5 * jnp.exp(theta_here[...].reshape(-1, 128)), LOCAL * COARSE * 16)
    for m in range(LOCAL):
        for p in range(PLANES):
            mid[m, p] = step(
                state_here[m, p - 1] if p > 0 else None,
                state_here[m, p],
                state_here[m, p + 1] if p < PLANES - 1 else None,
                plane_of(diff, (m * COARSE + p // 2) * ROWS),
                forcing_here[p],
            )
        for p in range(2, PLANES - 2):
            new = step(
                mid[m, p - 1],
                mid[m, p],
                mid[m, p + 1],
                plane_of(diff, (m * COARSE + p // 2) * ROWS),
                forcing_here[p],
            )
            inner[m, p - 2] = new
            store_halves(done, (m * 4 + p - 2) * ROWS, new)
    inner_sums[...] = sums_of_four(done, LOCAL * 4 * 8)
    var = spread[...]
    given[0:LOCAL, :] = target[...] + jnp.sqrt(var) * draws[...]
    given[LOCAL : LOCAL + 1, :] = var
    given[LOCAL + 1 : 8, :] = jnp.zeros((5, BLOCK), F32)


def masks(slab, *kept):
    vmem = pl.BlockSpec(memory_space=pltpu.VMEM)
    return pl.pallas_call(
        masks_kernel,
        out_shape=(
            jax.ShapeDtypeStruct((64, OBS), BF16),
            jax.ShapeDtypeStruct((8, OBS), F32),
            jax.ShapeDtypeStruct((8, OBS), F32),
            jax.ShapeDtypeStruct((8, 128), F32),
            jax.ShapeDtypeStruct((8, BLOCK), F32),
            *(jax.ShapeDtypeStruct(a.shape, F32) for a in kept[-3:]),
            jax.ShapeDtypeStruct((2, LOCAL * COARSE * ROWS, 128), F32),
            jax.ShapeDtypeStruct((LOCAL, PLANES, ROWS, COLS), F32),
            jax.ShapeDtypeStruct((LOCAL, 4, ROWS, COLS), F32),
            jax.ShapeDtypeStruct((LOCAL * 4 * 8, COLS), F32),
        ),
        in_specs=[pl.BlockSpec(memory_space=pltpu.SMEM)]
        + [pl.BlockSpec(memory_space=pltpu.HBM)] * 7,
        out_specs=(vmem,) * 12,
        compiler_params=pltpu.CompilerParams(vmem_limit_bytes=8 * MIB),
        scratch_shapes=[
            pltpu.VMEM((6, OBS), jnp.int32),
            pltpu.VMEM((1, BLOCK), F32),
            pltpu.VMEM((1, BLOCK), F32),
            pltpu.VMEM((LOCAL, BLOCK), F32),
            pltpu.VMEM((2, LOCAL * 4 * ROWS, 128), F32),
            pltpu.SemaphoreType.DMA((10,)),
        ],
        name="masks",
    )(slab, *(pltpu.with_memory_space_constraint(a, pltpu.HBM) for a in kept))


def window_kernel(
    slab, low, high, in_x, in_z, in_y, state, forcing, diff, mid, inner, inner_sums,
    final, part, outer, edge, done, sems,
):
    middle = pltpu.make_async_copy(inner, final.at[:, pl.ds(2, 4)], sems.at[0])
    middle.start()
    s = slab[0]
    pieces = []
    for m in range(LOCAL):
        for halo, inside in ((low, s > 0), (high, s < SLABS - 1)):
            keep = jnp.where(inside, 0.5, 0.0).astype(F32)
            pieces.append(keep * jnp.exp(halo[160:176, m * 128 : (m + 1) * 128]))
    spread_rows(outer, jnp.concatenate(pieces, axis=0), LOCAL * 2 * 16)

    def own(m, p):
        return plane_of(diff, (m * COARSE + p // 2) * ROWS)

    leaving = []
    for m in range(LOCAL):
        below = [low[(m * 2 + p) * ROWS : (m * 2 + p + 1) * ROWS, :] for p in range(2)]
        above = [high[(m * 2 + p) * ROWS : (m * 2 + p + 1) * ROWS, :] for p in range(2)]
        ahead = step(
            below[0], below[1], state[m, 0], plane_of(outer, m * 2 * ROWS), low[128:160, :]
        )
        behind = step(
            state[m, PLANES - 1], above[0], above[1], plane_of(outer, (m * 2 + 1) * ROWS),
            high[128:160, :],
        )
        bottom = mid[m, 0] + STEP_SIZE * (own(m, 0) * below[1])
        top = mid[m, PLANES - 1] + STEP_SIZE * (own(m, PLANES - 1) * above[0])
        news = (
            step(ahead, bottom, mid[m, 1], own(m, 0), forcing[0]),
            step(bottom, mid[m, 1], mid[m, 2], own(m, 1), forcing[1]),
            step(mid[m, 5], mid[m, 6], top, own(m, 6), forcing[6]),
            step(mid[m, 6], top, behind, own(m, 7), forcing[7]),
        )
        for i, new in enumerate(news):
            edge[m, i // 2, i % 2] = new
            store_halves(done, (m * 4 + i) * ROWS, new)
        for i in range(2):
            leaving.append(
                pltpu.make_async_copy(
                    edge.at[m, i], final.at[m, pl.ds(6 * i, 2)], sems.at[1 + 2 * m + i]
                )
            )
            leaving[-1].start()

    tall = LOCAL * PLANES * 8
    outer_sums = sums_of_four(done, LOCAL * 4 * 8)
    inside = inner_sums[...]
    sums = jnp.concatenate(
        [
            x
            for m in range(LOCAL)
            for x in (
                outer_sums[m * 32 : m * 32 + 16],
                inside[m * 32 : m * 32 + 32],
                outer_sums[m * 32 + 16 : m * 32 + 32],
            )
        ],
        axis=0,
    )
    fold = (
        lax.broadcasted_iota(jnp.int32, (COLS, 128), 0) // 4
        == lax.broadcasted_iota(jnp.int32, (COLS, 128), 1) % 64
    ).astype(F32).astype(BF16)
    tiles = sum(jnp.dot(part_, fold, preferred_element_type=F32) for part_ in split3(sums))
    top = tiles.astype(BF16).astype(F32)
    lane = lax.broadcasted_iota(jnp.int32, (tall, 128), 1)
    left = jnp.where(lane < 64, top, tiles - top).astype(BF16)

    def observe(d, carry):
        at = pl.ds(pl.multiple_of(d * BLOCK, BLOCK), BLOCK)
        wide_x = in_x[:, at]
        along = jnp.dot(left, jnp.concatenate([wide_x, wide_x], axis=0), preferred_element_type=F32)
        sums = [jnp.zeros((8, BLOCK), F32) for _ in range(LOCAL)]
        for z in range(PLANES):
            plane_z = jnp.broadcast_to(in_z[z : z + 1, at], (8, BLOCK))
            for m in range(LOCAL):
                row0 = (m * PLANES + z) * 8
                sums[m] = sums[m] + plane_z * along[row0 : row0 + 8]
        rows_y = in_y[:, at]
        for m in range(LOCAL):
            total = jnp.sum(rows_y * sums[m], axis=0, keepdims=True)
            for q in range(4):
                part[d, m * 4 + q : m * 4 + q + 1, :] = total[:, q * 128 : (q + 1) * 128]
        return carry

    lax.fori_loop(0, SLABS, observe, 0, unroll=8)
    middle.wait()
    for copy in leaving:
        copy.wait()


def window(slab, *given):
    vmem = pl.BlockSpec(memory_space=pltpu.VMEM)
    return pl.pallas_call(
        window_kernel,
        out_shape=(
            jax.ShapeDtypeStruct((LOCAL, PLANES, ROWS, COLS), F32),
            jax.ShapeDtypeStruct((SLABS, 8, 128), F32),
        ),
        in_specs=[pl.BlockSpec(memory_space=pltpu.SMEM)] + [vmem] * 11,
        out_specs=(pl.BlockSpec(memory_space=pltpu.HBM), vmem),
        compiler_params=pltpu.CompilerParams(vmem_limit_bytes=8 * MIB),
        scratch_shapes=[
            pltpu.VMEM((2, LOCAL * 2 * ROWS, 128), F32),
            pltpu.VMEM((LOCAL, 2, 2, ROWS, COLS), F32),
            pltpu.VMEM((2, LOCAL * 4 * ROWS, 128), F32),
            pltpu.SemaphoreType.DMA((5,)),
        ],
        name="window",
    )(slab, *given)


def gather_kernel(arrived, count, copies, own):
    pred = jnp.sum(arrived[...], axis=0) / count[...]
    own[...] = pred
    for g in range(GROUPS):
        copies[g] = pred


def own_predictions(arrived, count):
    return pl.pallas_call(
        gather_kernel,
        out_shape=(
            jax.ShapeDtypeStruct((GROUPS, 8, 128), F32),
            jax.ShapeDtypeStruct((8, 128), F32),
        ),
        compiler_params=pltpu.CompilerParams(vmem_limit_bytes=4 * MIB),
        name="own_predictions",
    )(arrived, count)


def moments_kernel(preds, own, given, out):
    scale = 1.0 / (float(MEMBERS - 1) ** 0.5)
    everyone = jnp.concatenate(
        [preds[pl.ds(q, MEMBERS, stride=4), :] for q in range(4)], axis=1
    )
    mine = jnp.concatenate([own[pl.ds(q, LOCAL, stride=4), :] for q in range(4)], axis=1)
    anomaly = (everyone - jnp.mean(everyone, axis=0, keepdims=True)) * scale
    misfit = given[0:LOCAL, :] - mine
    var = given[LOCAL : LOCAL + 1, :]
    weighted = anomaly / var
    pad = jnp.zeros((6, BLOCK), F32)
    right = jnp.concatenate(
        [anomaly, anomaly[8:], anomaly[16:], anomaly[24:]]
        + [misfit, pad] * 4
        + [jnp.zeros((16, BLOCK), F32)],
        axis=0,
    )
    product = lax.dot_general(
        weighted, right, (((1,), (1,)), ((), ())), precision=lax.Precision.HIGHEST,
        preferred_element_type=F32,
    )
    lane = lax.broadcasted_iota(jnp.int32, (8, 128), 1)
    packed = product[0:8]
    for c, start, stop in ((1, 32, 56), (2, 56, 72), (3, 72, 80)):
        mine = ((lane >= start) & (lane < stop)) | (lane // 8 == 10 + c)
        packed = jnp.where(mine, product[8 * c : 8 * c + 8], packed)
    for d in range(SLABS):
        out[d] = packed


def moments(preds, own, given):
    return pl.pallas_call(
        moments_kernel,
        out_shape=jax.ShapeDtypeStruct((SLABS, 8, 128), F32),
        compiler_params=pltpu.CompilerParams(vmem_limit_bytes=4 * MIB),
        name="moments",
    )(preds, own, given)


def update_kernel(group, arrived, here, there, out):
    parts = [arrived[d] for d in range(SLABS)]
    while len(parts) > 1:
        parts = [x + y for x, y in zip(parts[::2], parts[1::2])]
    packed = parts[0]
    lane8 = lax.broadcasted_iota(jnp.int32, (8, 128), 1)
    uppers, cross = [], []
    for c, start in enumerate((0, 32, 56, 72)):
        moved = pltpu.roll(packed, (8 * c - start) % 128, 1)
        uppers.append(jnp.where((lane8 >= 8 * c) & (lane8 < MEMBERS), moved, 0.0))
        cross.append(pltpu.roll(packed, (MEMBERS - 80 - 8 * c) % 128, 1))
    upper = jnp.concatenate(uppers, axis=0)
    cross = jnp.concatenate(cross, axis=0)
    tall = jnp.concatenate([upper, jnp.zeros((96, 128), F32)], axis=0)
    mirrored = tall.T[0:MEMBERS]
    row = lax.broadcasted_iota(jnp.int32, (MEMBERS, 128), 0)
    lane = lax.broadcasted_iota(jnp.int32, (MEMBERS, 128), 1)
    work = jnp.where(lane // 8 >= row // 8, upper, mirrored)
    work = jnp.where(row == lane, work + 1.0, work)
    work = jnp.where(lane < MEMBERS, work, jnp.where(lane < MEMBERS + LOCAL, cross, 0.0))
    for first in range(0, MEMBERS, 16):
        columns = [
            jnp.broadcast_to(work[:, k : k + 1], (MEMBERS, 128)) for k in range(first, first + 16)
        ]
        for i in range(16):
            k = first + i
            column = columns[i]
            inverse = 1.0 / column[k : k + 1, :]
            line = work[k : k + 1, :] * inverse
            work = jnp.where(row == k, line, work - column * line)
            for later in range(i + 1, 16):
                line = columns[later][k : k + 1, :] * inverse
                columns[later] = jnp.where(row == k, line, columns[later] - column * line)
    mixing = work - jnp.mean(work, axis=0, keepdims=True)
    mixing = mixing * (1.0 / float(MEMBERS - 1) ** 0.5)
    mixing = jnp.where(row - group[0] * LOCAL == lane - MEMBERS, mixing + 1.0, mixing)
    south = group[0] % 2 == 0
    turn = MEMBERS - LOCAL * group[0]
    totals = [jnp.zeros((64, 128), F32) for _ in range(LOCAL)]
    for j in range(LOCAL):
        column = jnp.broadcast_to(mixing[:, MEMBERS + j : MEMBERS + j + 1], (MEMBERS, 128))
        rows = pltpu.roll(column, turn, 0)

        def weight(at_south, at_north):
            at_south, at_north = at_south % MEMBERS, at_north % MEMBERS
            return jnp.where(
                south, rows[at_south : at_south + 1, :], rows[at_north : at_north + 1, :]
            )

        for i, d in enumerate(PARTS):
            for m in range(LOCAL):
                totals[j] = totals[j] + weight(4 * d + m, m - 4 * d) * here[2 * i + m]
                totals[j] = totals[j] + weight(2 + m - 4 * d, 4 * d + m - 2) * there[2 * i + m]
    for j in range(LOCAL):
        out[j] = totals[j]


def update(group, arrived, *fields):
    vmem = pl.BlockSpec(memory_space=pltpu.VMEM)
    return pl.pallas_call(
        update_kernel,
        out_shape=jax.ShapeDtypeStruct((LOCAL, 64, 128), F32),
        in_specs=[pl.BlockSpec(memory_space=pltpu.SMEM)] + [vmem] * 3,
        out_specs=vmem,
        compiler_params=pltpu.CompilerParams(vmem_limit_bytes=4 * MIB),
        name="update",
    )(group, arrived, *fields)


def local(state, theta, forcing, boxes, observed, noise_var, perturb):
    slab = lax.axis_index("slab").astype(jnp.int32).reshape(1)
    group = lax.axis_index("group").astype(jnp.int32).reshape(1)
    first, last = pack(state, theta, forcing)
    low = lax.ppermute(last, "slab", [(i, i + 1) for i in range(SLABS - 1)])
    high = lax.ppermute(first, "slab", [(i + 1, i) for i in range(SLABS - 1)])
    field = theta.reshape(LOCAL, 64, 128)

    def from_chip(value, chips):
        half = GROUPS // 2
        moves = [
            (((y + (1 - 2 * core) * chips) % half) * 2 + core, y * 2 + core)
            for y in range(half)
            for core in range(2)
        ]
        return lax.ppermute(value, "group", moves)

    pair = from_chip(field, 2)
    in_x, in_z, in_y, count, given, state, here, forcing, *inside = masks(
        slab, observed.reshape(1, BLOCK), noise_var.reshape(1, BLOCK), perturb, boxes,
        state, theta, forcing,
    )
    final, part = window(slab, low, high, in_x, in_z, in_y, state, forcing, *inside)
    arrived = lax.all_to_all(part, "slab", 0, 0, tiled=True)
    pair = jnp.concatenate([here.reshape(field.shape), pair], axis=0)
    across = from_chip(pair, 4)
    copies, own = own_predictions(arrived, count)
    preds = lax.all_to_all(copies, "group", 0, 0, tiled=True).reshape(GROUPS * 8, 128)
    even = jnp.concatenate([pair, across], axis=0)
    odd = from_chip(even, 1)
    sums = moments(preds, own, given)
    sums = lax.all_to_all(sums, "slab", 0, 0, tiled=True)
    here = jnp.concatenate([even, odd], axis=0)
    there = lax.ppermute(here, "group", [(i, i ^ 1) for i in range(GROUPS)])
    updated = update(group, sums, here, there)
    return final, updated.reshape(theta.shape)


def solution(mesh):
    return jax.shard_map(
        local,
        mesh=mesh,
        in_specs=(
            P("group", "slab", None, None),
            P("group", "slab", None, None),
            P("slab", None, None),
            P(),
            P("slab"),
            P("slab"),
            P("group", "slab"),
        ),
        out_specs=(P("group", "slab", None, None), P("group", "slab", None, None)),
        check_vma=False,
    )
```

```python
import jax
import jax.numpy as jnp
from jax import lax
from jax.experimental import pallas as pl
from jax.experimental.pallas import tpu as pltpu
from jax.sharding import PartitionSpec as P


STEP_SIZE = 0.1
F32 = jnp.float32
BF16 = jnp.bfloat16

LOCAL = 2
PLANES = 8
ROWS = 32
COLS = 256
COARSE = 4
SLABS = 32
GROUPS = 16
MEMBERS = 32
BLOCK = 512
OBS = SLABS * BLOCK
MIB = 1 << 20
PARTS = (0, 2, 4, 6, 1, 3, 5, 7)
HALO_ROWS = 176


def split3(value):
    a = value.astype(BF16)
    rest = value - a.astype(F32)
    b = rest.astype(BF16)
    c = (rest - b.astype(F32)).astype(BF16)
    return a, b, c


def upsampled(coarse):
    up = (
        lax.broadcasted_iota(jnp.int32, (128, COLS), 1) // 2
        == lax.broadcasted_iota(jnp.int32, (128, COLS), 0)
    ).astype(F32).astype(BF16)
    wide = sum(jnp.dot(part_, up, preferred_element_type=F32) for part_ in split3(coarse))
    return [wide[:, h * 128 : (h + 1) * 128] for h in range(2)]


def spread_rows(ref, coarse, rows):
    for h, half in enumerate(upsampled(coarse)):
        ref[h, pl.ds(0, rows, stride=2), :] = half
        ref[h, pl.ds(1, rows, stride=2), :] = half


def plane_of(ref, at):
    return jnp.concatenate([ref[h, at : at + ROWS, :] for h in range(2)], axis=1)


def step(below, center, above, d, f):
    row = lax.broadcasted_iota(jnp.int32, (ROWS, COLS), 0)
    col = lax.broadcasted_iota(jnp.int32, (ROWS, COLS), 1)
    beside = jnp.where(row == ROWS - 1, 0.0, pltpu.roll(center, ROWS - 1, 0))
    beside = beside + jnp.where(row == 0, 0.0, pltpu.roll(center, 1, 0))
    beside = beside + jnp.where(col == COLS - 1, 0.0, pltpu.roll(center, COLS - 1, 1))
    beside = beside + jnp.where(col == 0, 0.0, pltpu.roll(center, 1, 1))
    for side in (below, above):
        if side is not None:
            beside = beside + side
    change = d * (beside - 6.0 * center) + 0.5 * center * (1.0 - center * center) + f
    return center + STEP_SIZE * change


def store_halves(ref, at, plane):
    for h in range(2):
        ref[h, at : at + ROWS, :] = plane[:, h * 128 : (h + 1) * 128]


def sums_of_four(ref, rows):
    return jnp.concatenate(
        [sum(ref[h, pl.ds(q, rows, stride=4), :] for q in range(4)) for h in range(2)], axis=1
    )


def pack_kernel(state, theta, forcing, first, last, sems):
    copies = []

    def copy(src, dst):
        copies.append(pltpu.make_async_copy(src, dst, sems.at[len(copies)]))

    for out, plane, coarse, force in ((first, 0, 0, 0), (last, PLANES - 2, COARSE - 1, PLANES - 1)):
        for m in range(LOCAL):
            for p in range(2):
                at = (m * 2 + p) * ROWS
                copy(state.at[m, plane + p], out.at[pl.ds(at, ROWS), :])
            copy(theta.at[m, coarse], out.at[pl.ds(160, 16), pl.ds(m * 128, 128)])
        copy(forcing.at[force], out.at[pl.ds(128, ROWS), :])
    for c in copies:
        c.start()
    for c in copies:
        c.wait()


def pack(state, theta, forcing):
    shape = jax.ShapeDtypeStruct((HALO_ROWS, COLS), F32)
    vmem = pl.BlockSpec(memory_space=pltpu.VMEM)
    return pl.pallas_call(
        pack_kernel,
        out_shape=(shape, shape),
        in_specs=[pl.BlockSpec(memory_space=pltpu.HBM)] * 3,
        out_specs=(vmem, vmem),
        compiler_params=pltpu.CompilerParams(vmem_limit_bytes=2 * MIB),
        scratch_shapes=[pltpu.SemaphoreType.DMA((14,))],
        name="pack",
    )(*(pltpu.with_memory_space_constraint(a, pltpu.HBM) for a in (state, theta, forcing)))


def masks_kernel(
    slab, observed, noise, perturb, footprints, state, theta, forcing,
    in_x, in_z, in_y, count, given, state_here, theta_here, forcing_here,
    diff, mid, inner, inner_sums, boxes, target, spread, draws, done, sems,
):
    quarter = OBS // 4
    chunks = [pl.ds(i * quarter, quarter) for i in range(4)]
    enter = [
        pltpu.make_async_copy(footprints.at[:, c], boxes.at[:, c], sems.at[i])
        for i, c in enumerate(chunks)
    ]
    small = [
        pltpu.make_async_copy(src, dst, sems.at[4 + i])
        for i, (src, dst) in enumerate(
            (
                (observed, target),
                (noise, spread),
                (perturb, draws),
                (state, state_here),
                (theta, theta_here),
                (forcing, forcing_here),
            )
        )
    ]
    for e in enter + small:
        e.start()
    first = slab[0] * PLANES
    iota_x = lax.broadcasted_iota(jnp.int32, (64, BLOCK), 0)
    iota = lax.broadcasted_iota(jnp.int32, (8, BLOCK), 0)
    for i, e in enumerate(enter):
        e.wait()

        def build(d, carry):
            at = pl.ds(pl.multiple_of(i * quarter + d * BLOCK, BLOCK), BLOCK)
            b = boxes[:, at]
            in_x[:, at] = ((iota_x >= b[4:5]) & (iota_x < b[5:6])).astype(F32).astype(BF16)
            in_z[:, at] = ((iota + first >= b[0:1]) & (iota + first < b[1:2])).astype(F32)
            in_y[:, at] = ((iota >= b[2:3]) & (iota < b[3:4])).astype(F32)
            return carry

        lax.fori_loop(0, quarter // BLOCK, build, 0, unroll=8)
    b = boxes[:, pl.ds(pl.multiple_of(slab[0] * BLOCK, BLOCK), BLOCK)]
    cells = ((b[1:2] - b[0:1]) * (b[3:4] - b[2:3]) * (b[5:6] - b[4:5]) * 16).astype(F32)
    for m in range(LOCAL):
        for q in range(4):
            count[m * 4 + q : m * 4 + q + 1, :] = cells[:, q * 128 : (q + 1) * 128]
    for e in small:
        e.wait()
    spread_rows(diff, 0.5 * jnp.exp(theta_here[...].reshape(-1, 128)), LOCAL * COARSE * 16)
    for m in range(LOCAL):
        for p in range(PLANES):
            mid[m, p] = step(
                state_here[m, p - 1] if p > 0 else None,
                state_here[m, p],
                state_here[m, p + 1] if p < PLANES - 1 else None,
                plane_of(diff, (m * COARSE + p // 2) * ROWS),
                forcing_here[p],
            )
        for p in range(2, PLANES - 2):
            new = step(
                mid[m, p - 1],
                mid[m, p],
                mid[m, p + 1],
                plane_of(diff, (m * COARSE + p // 2) * ROWS),
                forcing_here[p],
            )
            inner[m, p - 2] = new
            store_halves(done, (m * 4 + p - 2) * ROWS, new)
    inner_sums[...] = sums_of_four(done, LOCAL * 4 * 8)
    var = spread[...]
    given[0:LOCAL, :] = target[...] + jnp.sqrt(var) * draws[...]
    given[LOCAL : LOCAL + 1, :] = var
    given[LOCAL + 1 : 8, :] = jnp.zeros((5, BLOCK), F32)


def masks(slab, *kept):
    vmem = pl.BlockSpec(memory_space=pltpu.VMEM)
    return pl.pallas_call(
        masks_kernel,
        out_shape=(
            jax.ShapeDtypeStruct((64, OBS), BF16),
            jax.ShapeDtypeStruct((8, OBS), F32),
            jax.ShapeDtypeStruct((8, OBS), F32),
            jax.ShapeDtypeStruct((8, 128), F32),
            jax.ShapeDtypeStruct((8, BLOCK), F32),
            *(jax.ShapeDtypeStruct(a.shape, F32) for a in kept[-3:]),
            jax.ShapeDtypeStruct((2, LOCAL * COARSE * ROWS, 128), F32),
            jax.ShapeDtypeStruct((LOCAL, PLANES, ROWS, COLS), F32),
            jax.ShapeDtypeStruct((LOCAL, 4, ROWS, COLS), F32),
            jax.ShapeDtypeStruct((LOCAL * 4 * 8, COLS), F32),
        ),
        in_specs=[pl.BlockSpec(memory_space=pltpu.SMEM)]
        + [pl.BlockSpec(memory_space=pltpu.HBM)] * 7,
        out_specs=(vmem,) * 12,
        compiler_params=pltpu.CompilerParams(vmem_limit_bytes=8 * MIB),
        scratch_shapes=[
            pltpu.VMEM((6, OBS), jnp.int32),
            pltpu.VMEM((1, BLOCK), F32),
            pltpu.VMEM((1, BLOCK), F32),
            pltpu.VMEM((LOCAL, BLOCK), F32),
            pltpu.VMEM((2, LOCAL * 4 * ROWS, 128), F32),
            pltpu.SemaphoreType.DMA((10,)),
        ],
        name="masks",
    )(slab, *(pltpu.with_memory_space_constraint(a, pltpu.HBM) for a in kept))


def window_kernel(
    slab, low, high, in_x, in_z, in_y, state, forcing, diff, mid, inner, inner_sums,
    final, part, outer, edge, done, sems,
):
    middle = pltpu.make_async_copy(inner, final.at[:, pl.ds(2, 4)], sems.at[0])
    middle.start()
    s = slab[0]
    pieces = []
    for m in range(LOCAL):
        for halo, inside in ((low, s > 0), (high, s < SLABS - 1)):
            keep = jnp.where(inside, 0.5, 0.0).astype(F32)
            pieces.append(keep * jnp.exp(halo[160:176, m * 128 : (m + 1) * 128]))
    spread_rows(outer, jnp.concatenate(pieces, axis=0), LOCAL * 2 * 16)

    def own(m, p):
        return plane_of(diff, (m * COARSE + p // 2) * ROWS)

    leaving = []
    for m in range(LOCAL):
        below = [low[(m * 2 + p) * ROWS : (m * 2 + p + 1) * ROWS, :] for p in range(2)]
        above = [high[(m * 2 + p) * ROWS : (m * 2 + p + 1) * ROWS, :] for p in range(2)]
        ahead = step(
            below[0], below[1], state[m, 0], plane_of(outer, m * 2 * ROWS), low[128:160, :]
        )
        behind = step(
            state[m, PLANES - 1], above[0], above[1], plane_of(outer, (m * 2 + 1) * ROWS),
            high[128:160, :],
        )
        bottom = mid[m, 0] + STEP_SIZE * (own(m, 0) * below[1])
        top = mid[m, PLANES - 1] + STEP_SIZE * (own(m, PLANES - 1) * above[0])
        news = (
            step(ahead, bottom, mid[m, 1], own(m, 0), forcing[0]),
            step(bottom, mid[m, 1], mid[m, 2], own(m, 1), forcing[1]),
            step(mid[m, 5], mid[m, 6], top, own(m, 6), forcing[6]),
            step(mid[m, 6], top, behind, own(m, 7), forcing[7]),
        )
        for i, new in enumerate(news):
            edge[m, i // 2, i % 2] = new
            store_halves(done, (m * 4 + i) * ROWS, new)
        for i in range(2):
            leaving.append(
                pltpu.make_async_copy(
                    edge.at[m, i], final.at[m, pl.ds(6 * i, 2)], sems.at[1 + 2 * m + i]
                )
            )
            leaving[-1].start()

    tall = LOCAL * PLANES * 8
    outer_sums = sums_of_four(done, LOCAL * 4 * 8)
    inside = inner_sums[...]
    sums = jnp.concatenate(
        [
            x
            for m in range(LOCAL)
            for x in (
                outer_sums[m * 32 : m * 32 + 16],
                inside[m * 32 : m * 32 + 32],
                outer_sums[m * 32 + 16 : m * 32 + 32],
            )
        ],
        axis=0,
    )
    fold = (
        lax.broadcasted_iota(jnp.int32, (COLS, 128), 0) // 4
        == lax.broadcasted_iota(jnp.int32, (COLS, 128), 1) % 64
    ).astype(F32).astype(BF16)
    tiles = sum(jnp.dot(part_, fold, preferred_element_type=F32) for part_ in split3(sums))
    top = tiles.astype(BF16).astype(F32)
    lane = lax.broadcasted_iota(jnp.int32, (tall, 128), 1)
    left = jnp.where(lane < 64, top, tiles - top).astype(BF16)

    def observe(d, carry):
        at = pl.ds(pl.multiple_of(d * BLOCK, BLOCK), BLOCK)
        wide_x = in_x[:, at]
        along = jnp.dot(left, jnp.concatenate([wide_x, wide_x], axis=0), preferred_element_type=F32)
        sums = [jnp.zeros((8, BLOCK), F32) for _ in range(LOCAL)]
        for z in range(PLANES):
            plane_z = jnp.broadcast_to(in_z[z : z + 1, at], (8, BLOCK))
            for m in range(LOCAL):
                row0 = (m * PLANES + z) * 8
                sums[m] = sums[m] + plane_z * along[row0 : row0 + 8]
        rows_y = in_y[:, at]
        for m in range(LOCAL):
            total = jnp.sum(rows_y * sums[m], axis=0, keepdims=True)
            for q in range(4):
                part[d, m * 4 + q : m * 4 + q + 1, :] = total[:, q * 128 : (q + 1) * 128]
        return carry

    lax.fori_loop(0, SLABS, observe, 0, unroll=8)
    middle.wait()
    for copy in leaving:
        copy.wait()


def window(slab, *given):
    vmem = pl.BlockSpec(memory_space=pltpu.VMEM)
    return pl.pallas_call(
        window_kernel,
        out_shape=(
            jax.ShapeDtypeStruct((LOCAL, PLANES, ROWS, COLS), F32),
            jax.ShapeDtypeStruct((SLABS, 8, 128), F32),
        ),
        in_specs=[pl.BlockSpec(memory_space=pltpu.SMEM)] + [vmem] * 11,
        out_specs=(pl.BlockSpec(memory_space=pltpu.HBM), vmem),
        compiler_params=pltpu.CompilerParams(vmem_limit_bytes=8 * MIB),
        scratch_shapes=[
            pltpu.VMEM((2, LOCAL * 2 * ROWS, 128), F32),
            pltpu.VMEM((LOCAL, 2, 2, ROWS, COLS), F32),
            pltpu.VMEM((2, LOCAL * 4 * ROWS, 128), F32),
            pltpu.SemaphoreType.DMA((5,)),
        ],
        name="window",
    )(slab, *given)


def gather_kernel(arrived, count, copies, own):
    pred = jnp.sum(arrived[...], axis=0) / count[...]
    own[...] = pred
    for g in range(GROUPS):
        copies[g] = pred


def own_predictions(arrived, count):
    return pl.pallas_call(
        gather_kernel,
        out_shape=(
            jax.ShapeDtypeStruct((GROUPS, 8, 128), F32),
            jax.ShapeDtypeStruct((8, 128), F32),
        ),
        compiler_params=pltpu.CompilerParams(vmem_limit_bytes=4 * MIB),
        name="own_predictions",
    )(arrived, count)


def moments_kernel(preds, own, given, out):
    scale = 1.0 / (float(MEMBERS - 1) ** 0.5)
    everyone = jnp.concatenate(
        [preds[pl.ds(q, MEMBERS, stride=4), :] for q in range(4)], axis=1
    )
    mine = jnp.concatenate([own[pl.ds(q, LOCAL, stride=4), :] for q in range(4)], axis=1)
    anomaly = (everyone - jnp.mean(everyone, axis=0, keepdims=True)) * scale
    misfit = given[0:LOCAL, :] - mine
    var = given[LOCAL : LOCAL + 1, :]
    weighted = anomaly / var
    pad = jnp.zeros((6, BLOCK), F32)
    right = jnp.concatenate(
        [anomaly, anomaly[8:], anomaly[16:], anomaly[24:]]
        + [misfit, pad] * 4
        + [jnp.zeros((16, BLOCK), F32)],
        axis=0,
    )
    product = lax.dot_general(
        weighted, right, (((1,), (1,)), ((), ())), precision=lax.Precision.HIGHEST,
        preferred_element_type=F32,
    )
    lane = lax.broadcasted_iota(jnp.int32, (8, 128), 1)
    packed = product[0:8]
    for c, start, stop in ((1, 32, 56), (2, 56, 72), (3, 72, 80)):
        mine = ((lane >= start) & (lane < stop)) | (lane // 8 == 10 + c)
        packed = jnp.where(mine, product[8 * c : 8 * c + 8], packed)
    for d in range(SLABS):
        out[d] = packed


def moments(preds, own, given):
    return pl.pallas_call(
        moments_kernel,
        out_shape=jax.ShapeDtypeStruct((SLABS, 8, 128), F32),
        compiler_params=pltpu.CompilerParams(vmem_limit_bytes=4 * MIB),
        name="moments",
    )(preds, own, given)


def update_kernel(group, arrived, here, there, out):
    parts = [arrived[d] for d in range(SLABS)]
    while len(parts) > 1:
        parts = [x + y for x, y in zip(parts[::2], parts[1::2])]
    packed = parts[0]
    lane8 = lax.broadcasted_iota(jnp.int32, (8, 128), 1)
    uppers, cross = [], []
    for c, start in enumerate((0, 32, 56, 72)):
        moved = pltpu.roll(packed, (8 * c - start) % 128, 1)
        uppers.append(jnp.where((lane8 >= 8 * c) & (lane8 < MEMBERS), moved, 0.0))
        cross.append(pltpu.roll(packed, (MEMBERS - 80 - 8 * c) % 128, 1))
    upper = jnp.concatenate(uppers, axis=0)
    cross = jnp.concatenate(cross, axis=0)
    tall = jnp.concatenate([upper, jnp.zeros((96, 128), F32)], axis=0)
    mirrored = tall.T[0:MEMBERS]
    row = lax.broadcasted_iota(jnp.int32, (MEMBERS, 128), 0)
    lane = lax.broadcasted_iota(jnp.int32, (MEMBERS, 128), 1)
    work = jnp.where(lane // 8 >= row // 8, upper, mirrored)
    work = jnp.where(row == lane, work + 1.0, work)
    work = jnp.where(lane < MEMBERS, work, jnp.where(lane < MEMBERS + LOCAL, cross, 0.0))
    for first in range(0, MEMBERS, 16):
        columns = [
            jnp.broadcast_to(work[:, k : k + 1], (MEMBERS, 128)) for k in range(first, first + 16)
        ]
        for i in range(16):
            k = first + i
            column = columns[i]
            inverse = 1.0 / column[k : k + 1, :]
            line = work[k : k + 1, :] * inverse
            work = jnp.where(row == k, line, work - column * line)
            for later in range(i + 1, 16):
                line = columns[later][k : k + 1, :] * inverse
                columns[later] = jnp.where(row == k, line, columns[later] - column * line)
    mixing = work - jnp.mean(work, axis=0, keepdims=True)
    mixing = mixing * (1.0 / float(MEMBERS - 1) ** 0.5)
    mixing = jnp.where(row - group[0] * LOCAL == lane - MEMBERS, mixing + 1.0, mixing)
    totals = [jnp.zeros((64, 128), F32) for _ in range(LOCAL)]
    for j in range(LOCAL):
        rows = jnp.broadcast_to(mixing[:, MEMBERS + j : MEMBERS + j + 1], (MEMBERS, 128))
        for size in (2, 4, 8, 16):
            swapped = jnp.where(
                row & size == 0, pltpu.roll(rows, MEMBERS - size, 0), pltpu.roll(rows, size, 0)
            )
            rows = jnp.where((LOCAL * group[0]) & size != 0, swapped, rows)
        for i, d in enumerate(PARTS):
            for m in range(LOCAL):
                at = 4 * d + m
                totals[j] = totals[j] + rows[at : at + 1, :] * here[2 * i + m]
                totals[j] = totals[j] + rows[at + 2 : at + 3, :] * there[2 * i + m]
    for j in range(LOCAL):
        out[j] = totals[j]


def update(group, arrived, *fields):
    vmem = pl.BlockSpec(memory_space=pltpu.VMEM)
    return pl.pallas_call(
        update_kernel,
        out_shape=jax.ShapeDtypeStruct((LOCAL, 64, 128), F32),
        in_specs=[pl.BlockSpec(memory_space=pltpu.SMEM)] + [vmem] * 3,
        out_specs=vmem,
        compiler_params=pltpu.CompilerParams(vmem_limit_bytes=4 * MIB),
        name="update",
    )(group, arrived, *fields)


def local(state, theta, forcing, boxes, observed, noise_var, perturb):
    slab = lax.axis_index("slab").astype(jnp.int32).reshape(1)
    group = lax.axis_index("group").astype(jnp.int32).reshape(1)
    first, last = pack(state, theta, forcing)
    low = lax.ppermute(last, "slab", [(i, i + 1) for i in range(SLABS - 1)])
    high = lax.ppermute(first, "slab", [(i + 1, i) for i in range(SLABS - 1)])
    field = theta.reshape(LOCAL, 64, 128)

    def from_chip(value, bit):
        return lax.ppermute(value, "group", [(i, i ^ (2 * bit)) for i in range(GROUPS)])

    pair = from_chip(field, 2)
    in_x, in_z, in_y, count, given, state, here, forcing, *inside = masks(
        slab, observed.reshape(1, BLOCK), noise_var.reshape(1, BLOCK), perturb, boxes,
        state, theta, forcing,
    )
    final, part = window(slab, low, high, in_x, in_z, in_y, state, forcing, *inside)
    arrived = lax.all_to_all(part, "slab", 0, 0, tiled=True)
    pair = jnp.concatenate([here.reshape(field.shape), pair], axis=0)
    across = from_chip(pair, 4)
    copies, own = own_predictions(arrived, count)
    preds = lax.all_to_all(copies, "group", 0, 0, tiled=True).reshape(GROUPS * 8, 128)
    even = jnp.concatenate([pair, across], axis=0)
    odd = from_chip(even, 1)
    sums = moments(preds, own, given)
    sums = lax.all_to_all(sums, "slab", 0, 0, tiled=True)
    here = jnp.concatenate([even, odd], axis=0)
    there = lax.ppermute(here, "group", [(i, i ^ 1) for i in range(GROUPS)])
    updated = update(group, sums, here, there)
    return final, updated.reshape(theta.shape)


def solution(mesh):
    return jax.shard_map(
        local,
        mesh=mesh,
        in_specs=(
            P("group", "slab", None, None),
            P("group", "slab", None, None),
            P("slab", None, None),
            P(),
            P("slab"),
            P("slab"),
            P("group", "slab"),
        ),
        out_specs=(P("group", "slab", None, None), P("group", "slab", None, None)),
        check_vma=False,
    )
```

```python
import jax
import jax.numpy as jnp
from jax import lax
from jax.experimental import pallas as pl
from jax.experimental.pallas import tpu as pltpu
from jax.sharding import PartitionSpec as P


STEP_SIZE = 0.1
F32 = jnp.float32
BF16 = jnp.bfloat16

LOCAL = 2
PLANES = 8
ROWS = 32
COLS = 256
COARSE = 4
SLABS = 32
GROUPS = 16
MEMBERS = 32
BLOCK = 512
OBS = SLABS * BLOCK
MIB = 1 << 20
PARTS = (0, 2, 4, 6, 1, 3, 5, 7)
HALO_ROWS = 176


def split3(value):
    a = value.astype(BF16)
    rest = value - a.astype(F32)
    b = rest.astype(BF16)
    c = (rest - b.astype(F32)).astype(BF16)
    return a, b, c


def upsampled(coarse):
    up = (
        lax.broadcasted_iota(jnp.int32, (128, COLS), 1) // 2
        == lax.broadcasted_iota(jnp.int32, (128, COLS), 0)
    ).astype(F32).astype(BF16)
    wide = sum(jnp.dot(part_, up, preferred_element_type=F32) for part_ in split3(coarse))
    return [wide[:, h * 128 : (h + 1) * 128] for h in range(2)]


def spread_rows(ref, coarse, rows):
    for h, half in enumerate(upsampled(coarse)):
        ref[h, pl.ds(0, rows, stride=2), :] = half
        ref[h, pl.ds(1, rows, stride=2), :] = half


def plane_of(ref, at):
    return jnp.concatenate([ref[h, at : at + ROWS, :] for h in range(2)], axis=1)


def step(below, center, above, d, f):
    row = lax.broadcasted_iota(jnp.int32, (ROWS, COLS), 0)
    col = lax.broadcasted_iota(jnp.int32, (ROWS, COLS), 1)
    beside = jnp.where(row == ROWS - 1, 0.0, pltpu.roll(center, ROWS - 1, 0))
    beside = beside + jnp.where(row == 0, 0.0, pltpu.roll(center, 1, 0))
    beside = beside + jnp.where(col == COLS - 1, 0.0, pltpu.roll(center, COLS - 1, 1))
    beside = beside + jnp.where(col == 0, 0.0, pltpu.roll(center, 1, 1))
    for side in (below, above):
        if side is not None:
            beside = beside + side
    change = d * (beside - 6.0 * center) + 0.5 * center * (1.0 - center * center) + f
    return center + STEP_SIZE * change


def store_halves(ref, at, plane):
    for h in range(2):
        ref[h, at : at + ROWS, :] = plane[:, h * 128 : (h + 1) * 128]


def sums_of_four(ref, rows):
    return jnp.concatenate(
        [sum(ref[h, pl.ds(q, rows, stride=4), :] for q in range(4)) for h in range(2)], axis=1
    )


def pack_kernel(slab, state, theta, forcing, near, far, sems):
    copies = []

    def copy(src, dst):
        copies.append(pltpu.make_async_copy(src, dst, sems.at[len(copies)]))

    even = slab[0] % 2 == 0
    for out, is_last in ((near, even), (far, jnp.logical_not(even))):
        plane = jnp.where(is_last, PLANES - 2, 0)
        for m in range(LOCAL):
            for p in range(2):
                at = (m * 2 + p) * ROWS
                copy(state.at[m, plane + p], out.at[pl.ds(at, ROWS), :])
            coarse = jnp.where(is_last, COARSE - 1, 0)
            copy(theta.at[m, coarse], out.at[pl.ds(160, 16), pl.ds(m * 128, 128)])
        copy(forcing.at[jnp.where(is_last, PLANES - 1, 0)], out.at[pl.ds(128, ROWS), :])
    for c in copies:
        c.start()
    for c in copies:
        c.wait()


def pack(slab, state, theta, forcing):
    shape = jax.ShapeDtypeStruct((HALO_ROWS, COLS), F32)
    vmem = pl.BlockSpec(memory_space=pltpu.VMEM)
    return pl.pallas_call(
        pack_kernel,
        out_shape=(shape, shape),
        in_specs=[pl.BlockSpec(memory_space=pltpu.SMEM)]
        + [pl.BlockSpec(memory_space=pltpu.HBM)] * 3,
        out_specs=(vmem, vmem),
        compiler_params=pltpu.CompilerParams(vmem_limit_bytes=2 * MIB),
        scratch_shapes=[pltpu.SemaphoreType.DMA((14,))],
        name="pack",
    )(slab, *(pltpu.with_memory_space_constraint(a, pltpu.HBM) for a in (state, theta, forcing)))


def masks_kernel(
    slab, observed, noise, perturb, footprints, state, theta, forcing,
    in_x, in_z, in_y, count, given, state_here, theta_here, forcing_here,
    diff, mid, inner, inner_sums, boxes, target, spread, draws, done, sems,
):
    quarter = OBS // 4
    chunks = [pl.ds(i * quarter, quarter) for i in range(4)]
    enter = [
        pltpu.make_async_copy(footprints.at[:, c], boxes.at[:, c], sems.at[i])
        for i, c in enumerate(chunks)
    ]
    small = [
        pltpu.make_async_copy(src, dst, sems.at[4 + i])
        for i, (src, dst) in enumerate(
            (
                (observed, target),
                (noise, spread),
                (perturb, draws),
                (state, state_here),
                (theta, theta_here),
                (forcing, forcing_here),
            )
        )
    ]
    for e in enter + small:
        e.start()
    first = slab[0] * PLANES
    iota_x = lax.broadcasted_iota(jnp.int32, (64, BLOCK), 0)
    iota = lax.broadcasted_iota(jnp.int32, (8, BLOCK), 0)
    for i, e in enumerate(enter):
        e.wait()

        def build(d, carry):
            at = pl.ds(pl.multiple_of(i * quarter + d * BLOCK, BLOCK), BLOCK)
            b = boxes[:, at]
            in_x[:, at] = ((iota_x >= b[4:5]) & (iota_x < b[5:6])).astype(F32).astype(BF16)
            in_z[:, at] = ((iota + first >= b[0:1]) & (iota + first < b[1:2])).astype(F32)
            in_y[:, at] = ((iota >= b[2:3]) & (iota < b[3:4])).astype(F32)
            return carry

        lax.fori_loop(0, quarter // BLOCK, build, 0, unroll=8)
    b = boxes[:, pl.ds(pl.multiple_of(slab[0] * BLOCK, BLOCK), BLOCK)]
    cells = ((b[1:2] - b[0:1]) * (b[3:4] - b[2:3]) * (b[5:6] - b[4:5]) * 16).astype(F32)
    for m in range(LOCAL):
        for q in range(4):
            count[m * 4 + q : m * 4 + q + 1, :] = cells[:, q * 128 : (q + 1) * 128]
    for e in small:
        e.wait()
    spread_rows(diff, 0.5 * jnp.exp(theta_here[...].reshape(-1, 128)), LOCAL * COARSE * 16)
    for m in range(LOCAL):
        for p in range(PLANES):
            mid[m, p] = step(
                state_here[m, p - 1] if p > 0 else None,
                state_here[m, p],
                state_here[m, p + 1] if p < PLANES - 1 else None,
                plane_of(diff, (m * COARSE + p // 2) * ROWS),
                forcing_here[p],
            )
        for p in range(2, PLANES - 2):
            new = step(
                mid[m, p - 1],
                mid[m, p],
                mid[m, p + 1],
                plane_of(diff, (m * COARSE + p // 2) * ROWS),
                forcing_here[p],
            )
            inner[m, p - 2] = new
            store_halves(done, (m * 4 + p - 2) * ROWS, new)
    inner_sums[...] = sums_of_four(done, LOCAL * 4 * 8)
    var = spread[...]
    given[0:LOCAL, :] = target[...] + jnp.sqrt(var) * draws[...]
    given[LOCAL : LOCAL + 1, :] = var
    given[LOCAL + 1 : 8, :] = jnp.zeros((5, BLOCK), F32)


def masks(slab, *kept):
    vmem = pl.BlockSpec(memory_space=pltpu.VMEM)
    return pl.pallas_call(
        masks_kernel,
        out_shape=(
            jax.ShapeDtypeStruct((64, OBS), BF16),
            jax.ShapeDtypeStruct((8, OBS), F32),
            jax.ShapeDtypeStruct((8, OBS), F32),
            jax.ShapeDtypeStruct((8, 128), F32),
            jax.ShapeDtypeStruct((8, BLOCK), F32),
            *(jax.ShapeDtypeStruct(a.shape, F32) for a in kept[-3:]),
            jax.ShapeDtypeStruct((2, LOCAL * COARSE * ROWS, 128), F32),
            jax.ShapeDtypeStruct((LOCAL, PLANES, ROWS, COLS), F32),
            jax.ShapeDtypeStruct((LOCAL, 4, ROWS, COLS), F32),
            jax.ShapeDtypeStruct((LOCAL * 4 * 8, COLS), F32),
        ),
        in_specs=[pl.BlockSpec(memory_space=pltpu.SMEM)]
        + [pl.BlockSpec(memory_space=pltpu.HBM)] * 7,
        out_specs=(vmem,) * 12,
        compiler_params=pltpu.CompilerParams(vmem_limit_bytes=8 * MIB),
        scratch_shapes=[
            pltpu.VMEM((6, OBS), jnp.int32),
            pltpu.VMEM((1, BLOCK), F32),
            pltpu.VMEM((1, BLOCK), F32),
            pltpu.VMEM((LOCAL, BLOCK), F32),
            pltpu.VMEM((2, LOCAL * 4 * ROWS, 128), F32),
            pltpu.SemaphoreType.DMA((10,)),
        ],
        name="masks",
    )(slab, *(pltpu.with_memory_space_constraint(a, pltpu.HBM) for a in kept))


def window_kernel(
    slab, near, far, in_x, in_z, in_y, state, forcing, diff, mid, inner, inner_sums,
    final, part, outer, edge, done, sems,
):
    middle = pltpu.make_async_copy(inner, final.at[:, pl.ds(2, 4)], sems.at[0])
    middle.start()
    s = slab[0]
    even = s % 2 == 0

    def low(rows, lanes=slice(None)):
        return jnp.where(even, far[rows, lanes], near[rows, lanes])

    def high(rows, lanes=slice(None)):
        return jnp.where(even, near[rows, lanes], far[rows, lanes])

    pieces = []
    for m in range(LOCAL):
        for halo, inside in ((low, s > 0), (high, s < SLABS - 1)):
            keep = jnp.where(inside, 0.5, 0.0).astype(F32)
            pieces.append(keep * jnp.exp(halo(slice(160, 176), slice(m * 128, (m + 1) * 128))))
    spread_rows(outer, jnp.concatenate(pieces, axis=0), LOCAL * 2 * 16)

    def own(m, p):
        return plane_of(diff, (m * COARSE + p // 2) * ROWS)

    leaving = []
    for m in range(LOCAL):
        below = [low(slice((m * 2 + p) * ROWS, (m * 2 + p + 1) * ROWS)) for p in range(2)]
        above = [high(slice((m * 2 + p) * ROWS, (m * 2 + p + 1) * ROWS)) for p in range(2)]
        ahead = step(
            below[0], below[1], state[m, 0], plane_of(outer, m * 2 * ROWS),
            low(slice(128, 160)),
        )
        behind = step(
            state[m, PLANES - 1], above[0], above[1], plane_of(outer, (m * 2 + 1) * ROWS),
            high(slice(128, 160)),
        )
        bottom = mid[m, 0] + STEP_SIZE * (own(m, 0) * below[1])
        top = mid[m, PLANES - 1] + STEP_SIZE * (own(m, PLANES - 1) * above[0])
        news = (
            step(ahead, bottom, mid[m, 1], own(m, 0), forcing[0]),
            step(bottom, mid[m, 1], mid[m, 2], own(m, 1), forcing[1]),
            step(mid[m, 5], mid[m, 6], top, own(m, 6), forcing[6]),
            step(mid[m, 6], top, behind, own(m, 7), forcing[7]),
        )
        for i, new in enumerate(news):
            edge[m, i // 2, i % 2] = new
            store_halves(done, (m * 4 + i) * ROWS, new)
        for i in range(2):
            leaving.append(
                pltpu.make_async_copy(
                    edge.at[m, i], final.at[m, pl.ds(6 * i, 2)], sems.at[1 + 2 * m + i]
                )
            )
            leaving[-1].start()

    tall = LOCAL * PLANES * 8
    outer_sums = sums_of_four(done, LOCAL * 4 * 8)
    inside = inner_sums[...]
    sums = jnp.concatenate(
        [
            x
            for m in range(LOCAL)
            for x in (
                outer_sums[m * 32 : m * 32 + 16],
                inside[m * 32 : m * 32 + 32],
                outer_sums[m * 32 + 16 : m * 32 + 32],
            )
        ],
        axis=0,
    )
    fold = (
        lax.broadcasted_iota(jnp.int32, (COLS, 128), 0) // 4
        == lax.broadcasted_iota(jnp.int32, (COLS, 128), 1) % 64
    ).astype(F32).astype(BF16)
    tiles = sum(jnp.dot(part_, fold, preferred_element_type=F32) for part_ in split3(sums))
    top = tiles.astype(BF16).astype(F32)
    lane = lax.broadcasted_iota(jnp.int32, (tall, 128), 1)
    left = jnp.where(lane < 64, top, tiles - top).astype(BF16)

    def observe(d, carry):
        at = pl.ds(pl.multiple_of(d * BLOCK, BLOCK), BLOCK)
        wide_x = in_x[:, at]
        along = jnp.dot(left, jnp.concatenate([wide_x, wide_x], axis=0), preferred_element_type=F32)
        sums = [jnp.zeros((8, BLOCK), F32) for _ in range(LOCAL)]
        for z in range(PLANES):
            plane_z = jnp.broadcast_to(in_z[z : z + 1, at], (8, BLOCK))
            for m in range(LOCAL):
                row0 = (m * PLANES + z) * 8
                sums[m] = sums[m] + plane_z * along[row0 : row0 + 8]
        rows_y = in_y[:, at]
        for m in range(LOCAL):
            total = jnp.sum(rows_y * sums[m], axis=0, keepdims=True)
            for q in range(4):
                part[d, m * 4 + q : m * 4 + q + 1, :] = total[:, q * 128 : (q + 1) * 128]
        return carry

    lax.fori_loop(0, SLABS, observe, 0, unroll=8)
    middle.wait()
    for copy in leaving:
        copy.wait()


def window(slab, *given):
    vmem = pl.BlockSpec(memory_space=pltpu.VMEM)
    return pl.pallas_call(
        window_kernel,
        out_shape=(
            jax.ShapeDtypeStruct((LOCAL, PLANES, ROWS, COLS), F32),
            jax.ShapeDtypeStruct((SLABS, 8, 128), F32),
        ),
        in_specs=[pl.BlockSpec(memory_space=pltpu.SMEM)] + [vmem] * 11,
        out_specs=(pl.BlockSpec(memory_space=pltpu.HBM), vmem),
        compiler_params=pltpu.CompilerParams(vmem_limit_bytes=8 * MIB),
        scratch_shapes=[
            pltpu.VMEM((2, LOCAL * 2 * ROWS, 128), F32),
            pltpu.VMEM((LOCAL, 2, 2, ROWS, COLS), F32),
            pltpu.VMEM((2, LOCAL * 4 * ROWS, 128), F32),
            pltpu.SemaphoreType.DMA((5,)),
        ],
        name="window",
    )(slab, *given)


def gather_kernel(arrived, count, copies, own):
    pred = jnp.sum(arrived[...], axis=0) / count[...]
    own[...] = pred
    for g in range(GROUPS):
        copies[g] = pred


def own_predictions(arrived, count):
    return pl.pallas_call(
        gather_kernel,
        out_shape=(
            jax.ShapeDtypeStruct((GROUPS, 8, 128), F32),
            jax.ShapeDtypeStruct((8, 128), F32),
        ),
        compiler_params=pltpu.CompilerParams(vmem_limit_bytes=4 * MIB),
        name="own_predictions",
    )(arrived, count)


def moments_kernel(preds, own, given, out):
    scale = 1.0 / (float(MEMBERS - 1) ** 0.5)
    everyone = jnp.concatenate(
        [preds[pl.ds(q, MEMBERS, stride=4), :] for q in range(4)], axis=1
    )
    mine = jnp.concatenate([own[pl.ds(q, LOCAL, stride=4), :] for q in range(4)], axis=1)
    anomaly = (everyone - jnp.mean(everyone, axis=0, keepdims=True)) * scale
    misfit = given[0:LOCAL, :] - mine
    var = given[LOCAL : LOCAL + 1, :]
    weighted = anomaly / var
    pad = jnp.zeros((6, BLOCK), F32)
    right = jnp.concatenate(
        [anomaly, anomaly[8:], anomaly[16:], anomaly[24:]]
        + [misfit, pad] * 4
        + [jnp.zeros((16, BLOCK), F32)],
        axis=0,
    )
    product = lax.dot_general(
        weighted, right, (((1,), (1,)), ((), ())), precision=lax.Precision.HIGHEST,
        preferred_element_type=F32,
    )
    lane = lax.broadcasted_iota(jnp.int32, (8, 128), 1)
    packed = product[0:8]
    for c, start, stop in ((1, 32, 56), (2, 56, 72), (3, 72, 80)):
        mine = ((lane >= start) & (lane < stop)) | (lane // 8 == 10 + c)
        packed = jnp.where(mine, product[8 * c : 8 * c + 8], packed)
    for d in range(SLABS):
        out[d] = packed


def moments(preds, own, given):
    return pl.pallas_call(
        moments_kernel,
        out_shape=jax.ShapeDtypeStruct((SLABS, 8, 128), F32),
        compiler_params=pltpu.CompilerParams(vmem_limit_bytes=4 * MIB),
        name="moments",
    )(preds, own, given)


def update_kernel(group, arrived, here, there, out):
    parts = [arrived[d] for d in range(SLABS)]
    while len(parts) > 1:
        parts = [x + y for x, y in zip(parts[::2], parts[1::2])]
    packed = parts[0]
    lane8 = lax.broadcasted_iota(jnp.int32, (8, 128), 1)
    uppers, cross = [], []
    for c, start in enumerate((0, 32, 56, 72)):
        moved = pltpu.roll(packed, (8 * c - start) % 128, 1)
        uppers.append(jnp.where((lane8 >= 8 * c) & (lane8 < MEMBERS), moved, 0.0))
        cross.append(pltpu.roll(packed, (MEMBERS - 80 - 8 * c) % 128, 1))
    upper = jnp.concatenate(uppers, axis=0)
    cross = jnp.concatenate(cross, axis=0)
    tall = jnp.concatenate([upper, jnp.zeros((96, 128), F32)], axis=0)
    mirrored = tall.T[0:MEMBERS]
    row = lax.broadcasted_iota(jnp.int32, (MEMBERS, 128), 0)
    lane = lax.broadcasted_iota(jnp.int32, (MEMBERS, 128), 1)
    work = jnp.where(lane // 8 >= row // 8, upper, mirrored)
    work = jnp.where(row == lane, work + 1.0, work)
    work = jnp.where(lane < MEMBERS, work, jnp.where(lane < MEMBERS + LOCAL, cross, 0.0))
    for first in range(0, MEMBERS, 16):
        columns = [
            jnp.broadcast_to(work[:, k : k + 1], (MEMBERS, 128)) for k in range(first, first + 16)
        ]
        for i in range(16):
            k = first + i
            column = columns[i]
            inverse = 1.0 / column[k : k + 1, :]
            line = work[k : k + 1, :] * inverse
            work = jnp.where(row == k, line, work - column * line)
            for later in range(i + 1, 16):
                line = columns[later][k : k + 1, :] * inverse
                columns[later] = jnp.where(row == k, line, columns[later] - column * line)
    mixing = work - jnp.mean(work, axis=0, keepdims=True)
    mixing = mixing * (1.0 / float(MEMBERS - 1) ** 0.5)
    mixing = jnp.where(row - group[0] * LOCAL == lane - MEMBERS, mixing + 1.0, mixing)
    totals = [jnp.zeros((64, 128), F32) for _ in range(LOCAL)]
    for j in range(LOCAL):
        rows = jnp.broadcast_to(mixing[:, MEMBERS + j : MEMBERS + j + 1], (MEMBERS, 128))
        for size in (2, 4, 8, 16):
            swapped = jnp.where(
                row & size == 0, pltpu.roll(rows, MEMBERS - size, 0), pltpu.roll(rows, size, 0)
            )
            rows = jnp.where((LOCAL * group[0]) & size != 0, swapped, rows)
        for i, d in enumerate(PARTS):
            for m in range(LOCAL):
                at = 4 * d + m
                totals[j] = totals[j] + rows[at : at + 1, :] * here[2 * i + m]
                totals[j] = totals[j] + rows[at + 2 : at + 3, :] * there[2 * i + m]
    for j in range(LOCAL):
        out[j] = totals[j]


def update(group, arrived, *fields):
    vmem = pl.BlockSpec(memory_space=pltpu.VMEM)
    return pl.pallas_call(
        update_kernel,
        out_shape=jax.ShapeDtypeStruct((LOCAL, 64, 128), F32),
        in_specs=[pl.BlockSpec(memory_space=pltpu.SMEM)] + [vmem] * 3,
        out_specs=vmem,
        compiler_params=pltpu.CompilerParams(vmem_limit_bytes=4 * MIB),
        name="update",
    )(group, arrived, *fields)


def local(state, theta, forcing, boxes, observed, noise_var, perturb):
    slab = lax.axis_index("slab").astype(jnp.int32).reshape(1)
    group = lax.axis_index("group").astype(jnp.int32).reshape(1)
    near, far = pack(slab, state, theta, forcing)
    pairs = [(i, i + 1) for i in range(1, SLABS - 1, 2)]
    far = lax.ppermute(far, "slab", pairs + [(j, i) for i, j in pairs])
    near = lax.ppermute(near, "slab", [(i, i ^ 1) for i in range(SLABS)])
    field = theta.reshape(LOCAL, 64, 128)

    def from_chip(value, bit):
        return lax.ppermute(value, "group", [(i, i ^ (2 * bit)) for i in range(GROUPS)])

    pair = from_chip(field, 2)
    in_x, in_z, in_y, count, given, state, here, forcing, *inside = masks(
        slab, observed.reshape(1, BLOCK), noise_var.reshape(1, BLOCK), perturb, boxes,
        state, theta, forcing,
    )
    final, part = window(slab, near, far, in_x, in_z, in_y, state, forcing, *inside)
    arrived = lax.all_to_all(part, "slab", 0, 0, tiled=True)
    pair = jnp.concatenate([here.reshape(field.shape), pair], axis=0)
    across = from_chip(pair, 4)
    copies, own = own_predictions(arrived, count)
    preds = lax.all_to_all(copies, "group", 0, 0, tiled=True).reshape(GROUPS * 8, 128)
    even = jnp.concatenate([pair, across], axis=0)
    odd = from_chip(even, 1)
    sums = moments(preds, own, given)
    sums = lax.all_to_all(sums, "slab", 0, 0, tiled=True)
    here = jnp.concatenate([even, odd], axis=0)
    there = lax.ppermute(here, "group", [(i, i ^ 1) for i in range(GROUPS)])
    updated = update(group, sums, here, there)
    return final, updated.reshape(theta.shape)


def solution(mesh):
    return jax.shard_map(
        local,
        mesh=mesh,
        in_specs=(
            P("group", "slab", None, None),
            P("group", "slab", None, None),
            P("slab", None, None),
            P(),
            P("slab"),
            P("slab"),
            P("group", "slab"),
        ),
        out_specs=(P("group", "slab", None, None), P("group", "slab", None, None)),
        check_vma=False,
    )
```

```python
import jax
import jax.numpy as jnp
from jax import lax
from jax.experimental import pallas as pl
from jax.experimental.pallas import tpu as pltpu
from jax.sharding import PartitionSpec as P


STEP_SIZE = 0.1
F32 = jnp.float32
BF16 = jnp.bfloat16

LOCAL = 2
PLANES = 8
ROWS = 32
COLS = 256
COARSE = 4
SLABS = 32
GROUPS = 16
MEMBERS = 32
BLOCK = 512
OBS = SLABS * BLOCK
MIB = 1 << 20
PARTS = (0, 1, 4, 5, 2, 3, 6, 7)
HALO_ROWS = 176


def split3(value):
    a = value.astype(BF16)
    rest = value - a.astype(F32)
    b = rest.astype(BF16)
    c = (rest - b.astype(F32)).astype(BF16)
    return a, b, c


def upsampled(coarse):
    up = (
        lax.broadcasted_iota(jnp.int32, (128, COLS), 1) // 2
        == lax.broadcasted_iota(jnp.int32, (128, COLS), 0)
    ).astype(F32).astype(BF16)
    wide = sum(jnp.dot(part_, up, preferred_element_type=F32) for part_ in split3(coarse))
    return [wide[:, h * 128 : (h + 1) * 128] for h in range(2)]


def spread_rows(ref, coarse, rows):
    for h, half in enumerate(upsampled(coarse)):
        ref[h, pl.ds(0, rows, stride=2), :] = half
        ref[h, pl.ds(1, rows, stride=2), :] = half


def plane_of(ref, at):
    return jnp.concatenate([ref[h, at : at + ROWS, :] for h in range(2)], axis=1)


def step(below, center, above, d, f):
    row = lax.broadcasted_iota(jnp.int32, (ROWS, COLS), 0)
    col = lax.broadcasted_iota(jnp.int32, (ROWS, COLS), 1)
    beside = jnp.where(row == ROWS - 1, 0.0, pltpu.roll(center, ROWS - 1, 0))
    beside = beside + jnp.where(row == 0, 0.0, pltpu.roll(center, 1, 0))
    beside = beside + jnp.where(col == COLS - 1, 0.0, pltpu.roll(center, COLS - 1, 1))
    beside = beside + jnp.where(col == 0, 0.0, pltpu.roll(center, 1, 1))
    for side in (below, above):
        if side is not None:
            beside = beside + side
    change = d * (beside - 6.0 * center) + 0.5 * center * (1.0 - center * center) + f
    return center + STEP_SIZE * change


def store_halves(ref, at, plane):
    for h in range(2):
        ref[h, at : at + ROWS, :] = plane[:, h * 128 : (h + 1) * 128]


def sums_of_four(ref, rows):
    return jnp.concatenate(
        [sum(ref[h, pl.ds(q, rows, stride=4), :] for q in range(4)) for h in range(2)], axis=1
    )


def pack_kernel(slab, state, theta, forcing, near, far, sems):
    copies = []

    def copy(src, dst):
        copies.append(pltpu.make_async_copy(src, dst, sems.at[len(copies)]))

    even = slab[0] % 2 == 0
    for out, is_last in ((near, even), (far, jnp.logical_not(even))):
        plane = jnp.where(is_last, PLANES - 2, 0)
        for m in range(LOCAL):
            for p in range(2):
                at = (m * 2 + p) * ROWS
                copy(state.at[m, plane + p], out.at[pl.ds(at, ROWS), :])
            coarse = jnp.where(is_last, COARSE - 1, 0)
            copy(theta.at[m, coarse], out.at[pl.ds(160, 16), pl.ds(m * 128, 128)])
        copy(forcing.at[jnp.where(is_last, PLANES - 1, 0)], out.at[pl.ds(128, ROWS), :])
    for c in copies:
        c.start()
    for c in copies:
        c.wait()


def pack(slab, state, theta, forcing):
    shape = jax.ShapeDtypeStruct((HALO_ROWS, COLS), F32)
    vmem = pl.BlockSpec(memory_space=pltpu.VMEM)
    return pl.pallas_call(
        pack_kernel,
        out_shape=(shape, shape),
        in_specs=[pl.BlockSpec(memory_space=pltpu.SMEM)]
        + [pl.BlockSpec(memory_space=pltpu.HBM)] * 3,
        out_specs=(vmem, vmem),
        compiler_params=pltpu.CompilerParams(vmem_limit_bytes=2 * MIB),
        scratch_shapes=[pltpu.SemaphoreType.DMA((14,))],
        name="pack",
    )(slab, *(pltpu.with_memory_space_constraint(a, pltpu.HBM) for a in (state, theta, forcing)))


def masks_kernel(
    slab, observed, noise, perturb, footprints, state, theta, forcing,
    in_x, in_z, in_y, count, given, state_here, theta_here, forcing_here,
    diff, mid, inner, inner_sums, boxes, target, spread, draws, done, sems,
):
    quarter = OBS // 4
    chunks = [pl.ds(i * quarter, quarter) for i in range(4)]
    enter = [
        pltpu.make_async_copy(footprints.at[:, c], boxes.at[:, c], sems.at[i])
        for i, c in enumerate(chunks)
    ]
    small = [
        pltpu.make_async_copy(src, dst, sems.at[4 + i])
        for i, (src, dst) in enumerate(
            (
                (observed, target),
                (noise, spread),
                (perturb, draws),
                (state, state_here),
                (theta, theta_here),
                (forcing, forcing_here),
            )
        )
    ]
    for e in enter + small:
        e.start()
    first = slab[0] * PLANES
    iota_x = lax.broadcasted_iota(jnp.int32, (64, BLOCK), 0)
    iota = lax.broadcasted_iota(jnp.int32, (8, BLOCK), 0)
    for i, e in enumerate(enter):
        e.wait()

        def build(d, carry):
            at = pl.ds(pl.multiple_of(i * quarter + d * BLOCK, BLOCK), BLOCK)
            b = boxes[:, at]
            in_x[:, at] = ((iota_x >= b[4:5]) & (iota_x < b[5:6])).astype(F32).astype(BF16)
            in_z[:, at] = ((iota + first >= b[0:1]) & (iota + first < b[1:2])).astype(F32)
            in_y[:, at] = ((iota >= b[2:3]) & (iota < b[3:4])).astype(F32)
            return carry

        lax.fori_loop(0, quarter // BLOCK, build, 0, unroll=8)
    b = boxes[:, pl.ds(pl.multiple_of(slab[0] * BLOCK, BLOCK), BLOCK)]
    cells = ((b[1:2] - b[0:1]) * (b[3:4] - b[2:3]) * (b[5:6] - b[4:5]) * 16).astype(F32)
    for m in range(LOCAL):
        for q in range(4):
            count[m * 4 + q : m * 4 + q + 1, :] = cells[:, q * 128 : (q + 1) * 128]
    for e in small:
        e.wait()
    spread_rows(diff, 0.5 * jnp.exp(theta_here[...].reshape(-1, 128)), LOCAL * COARSE * 16)
    for m in range(LOCAL):
        for p in range(PLANES):
            mid[m, p] = step(
                state_here[m, p - 1] if p > 0 else None,
                state_here[m, p],
                state_here[m, p + 1] if p < PLANES - 1 else None,
                plane_of(diff, (m * COARSE + p // 2) * ROWS),
                forcing_here[p],
            )
        for p in range(2, PLANES - 2):
            new = step(
                mid[m, p - 1],
                mid[m, p],
                mid[m, p + 1],
                plane_of(diff, (m * COARSE + p // 2) * ROWS),
                forcing_here[p],
            )
            inner[m, p - 2] = new
            store_halves(done, (m * 4 + p - 2) * ROWS, new)
    inner_sums[...] = sums_of_four(done, LOCAL * 4 * 8)
    var = spread[...]
    given[0:LOCAL, :] = target[...] + jnp.sqrt(var) * draws[...]
    given[LOCAL : LOCAL + 1, :] = var
    given[LOCAL + 1 : 8, :] = jnp.zeros((5, BLOCK), F32)


def masks(slab, *kept):
    vmem = pl.BlockSpec(memory_space=pltpu.VMEM)
    return pl.pallas_call(
        masks_kernel,
        out_shape=(
            jax.ShapeDtypeStruct((64, OBS), BF16),
            jax.ShapeDtypeStruct((8, OBS), F32),
            jax.ShapeDtypeStruct((8, OBS), F32),
            jax.ShapeDtypeStruct((8, 128), F32),
            jax.ShapeDtypeStruct((8, BLOCK), F32),
            *(jax.ShapeDtypeStruct(a.shape, F32) for a in kept[-3:]),
            jax.ShapeDtypeStruct((2, LOCAL * COARSE * ROWS, 128), F32),
            jax.ShapeDtypeStruct((LOCAL, PLANES, ROWS, COLS), F32),
            jax.ShapeDtypeStruct((LOCAL, 4, ROWS, COLS), F32),
            jax.ShapeDtypeStruct((LOCAL * 4 * 8, COLS), F32),
        ),
        in_specs=[pl.BlockSpec(memory_space=pltpu.SMEM)]
        + [pl.BlockSpec(memory_space=pltpu.HBM)] * 7,
        out_specs=(vmem,) * 12,
        compiler_params=pltpu.CompilerParams(vmem_limit_bytes=8 * MIB),
        scratch_shapes=[
            pltpu.VMEM((6, OBS), jnp.int32),
            pltpu.VMEM((1, BLOCK), F32),
            pltpu.VMEM((1, BLOCK), F32),
            pltpu.VMEM((LOCAL, BLOCK), F32),
            pltpu.VMEM((2, LOCAL * 4 * ROWS, 128), F32),
            pltpu.SemaphoreType.DMA((10,)),
        ],
        name="masks",
    )(slab, *(pltpu.with_memory_space_constraint(a, pltpu.HBM) for a in kept))


def window_kernel(
    slab, near, far, in_x, in_z, in_y, state, forcing, diff, mid, inner, inner_sums,
    final, part, outer, edge, done, sems,
):
    middle = pltpu.make_async_copy(inner, final.at[:, pl.ds(2, 4)], sems.at[0])
    middle.start()
    s = slab[0]
    even = s % 2 == 0

    def low(rows, lanes=slice(None)):
        return jnp.where(even, far[rows, lanes], near[rows, lanes])

    def high(rows, lanes=slice(None)):
        return jnp.where(even, near[rows, lanes], far[rows, lanes])

    pieces = []
    for m in range(LOCAL):
        for halo, inside in ((low, s > 0), (high, s < SLABS - 1)):
            keep = jnp.where(inside, 0.5, 0.0).astype(F32)
            pieces.append(keep * jnp.exp(halo(slice(160, 176), slice(m * 128, (m + 1) * 128))))
    spread_rows(outer, jnp.concatenate(pieces, axis=0), LOCAL * 2 * 16)

    def own(m, p):
        return plane_of(diff, (m * COARSE + p // 2) * ROWS)

    leaving = []
    for m in range(LOCAL):
        below = [low(slice((m * 2 + p) * ROWS, (m * 2 + p + 1) * ROWS)) for p in range(2)]
        above = [high(slice((m * 2 + p) * ROWS, (m * 2 + p + 1) * ROWS)) for p in range(2)]
        ahead = step(
            below[0], below[1], state[m, 0], plane_of(outer, m * 2 * ROWS),
            low(slice(128, 160)),
        )
        behind = step(
            state[m, PLANES - 1], above[0], above[1], plane_of(outer, (m * 2 + 1) * ROWS),
            high(slice(128, 160)),
        )
        bottom = mid[m, 0] + STEP_SIZE * (own(m, 0) * below[1])
        top = mid[m, PLANES - 1] + STEP_SIZE * (own(m, PLANES - 1) * above[0])
        news = (
            step(ahead, bottom, mid[m, 1], own(m, 0), forcing[0]),
            step(bottom, mid[m, 1], mid[m, 2], own(m, 1), forcing[1]),
            step(mid[m, 5], mid[m, 6], top, own(m, 6), forcing[6]),
            step(mid[m, 6], top, behind, own(m, 7), forcing[7]),
        )
        for i, new in enumerate(news):
            edge[m, i // 2, i % 2] = new
            store_halves(done, (m * 4 + i) * ROWS, new)
        for i in range(2):
            leaving.append(
                pltpu.make_async_copy(
                    edge.at[m, i], final.at[m, pl.ds(6 * i, 2)], sems.at[1 + 2 * m + i]
                )
            )
            leaving[-1].start()

    tall = LOCAL * PLANES * 8
    outer_sums = sums_of_four(done, LOCAL * 4 * 8)
    inside = inner_sums[...]
    sums = jnp.concatenate(
        [
            x
            for m in range(LOCAL)
            for x in (
                outer_sums[m * 32 : m * 32 + 16],
                inside[m * 32 : m * 32 + 32],
                outer_sums[m * 32 + 16 : m * 32 + 32],
            )
        ],
        axis=0,
    )
    fold = (
        lax.broadcasted_iota(jnp.int32, (COLS, 128), 0) // 4
        == lax.broadcasted_iota(jnp.int32, (COLS, 128), 1) % 64
    ).astype(F32).astype(BF16)
    tiles = sum(jnp.dot(part_, fold, preferred_element_type=F32) for part_ in split3(sums))
    top = tiles.astype(BF16).astype(F32)
    lane = lax.broadcasted_iota(jnp.int32, (tall, 128), 1)
    left = jnp.where(lane < 64, top, tiles - top).astype(BF16)

    def observe(d, carry):
        at = pl.ds(pl.multiple_of(d * BLOCK, BLOCK), BLOCK)
        wide_x = in_x[:, at]
        along = jnp.dot(left, jnp.concatenate([wide_x, wide_x], axis=0), preferred_element_type=F32)
        sums = [jnp.zeros((8, BLOCK), F32) for _ in range(LOCAL)]
        for z in range(PLANES):
            plane_z = jnp.broadcast_to(in_z[z : z + 1, at], (8, BLOCK))
            for m in range(LOCAL):
                row0 = (m * PLANES + z) * 8
                sums[m] = sums[m] + plane_z * along[row0 : row0 + 8]
        rows_y = in_y[:, at]
        for m in range(LOCAL):
            total = jnp.sum(rows_y * sums[m], axis=0, keepdims=True)
            for q in range(4):
                part[d, m * 4 + q : m * 4 + q + 1, :] = total[:, q * 128 : (q + 1) * 128]
        return carry

    lax.fori_loop(0, SLABS, observe, 0, unroll=8)
    middle.wait()
    for copy in leaving:
        copy.wait()


def window(slab, *given):
    vmem = pl.BlockSpec(memory_space=pltpu.VMEM)
    return pl.pallas_call(
        window_kernel,
        out_shape=(
            jax.ShapeDtypeStruct((LOCAL, PLANES, ROWS, COLS), F32),
            jax.ShapeDtypeStruct((SLABS, 8, 128), F32),
        ),
        in_specs=[pl.BlockSpec(memory_space=pltpu.SMEM)] + [vmem] * 11,
        out_specs=(pl.BlockSpec(memory_space=pltpu.HBM), vmem),
        compiler_params=pltpu.CompilerParams(vmem_limit_bytes=8 * MIB),
        scratch_shapes=[
            pltpu.VMEM((2, LOCAL * 2 * ROWS, 128), F32),
            pltpu.VMEM((LOCAL, 2, 2, ROWS, COLS), F32),
            pltpu.VMEM((2, LOCAL * 4 * ROWS, 128), F32),
            pltpu.SemaphoreType.DMA((5,)),
        ],
        name="window",
    )(slab, *given)


def gather_kernel(arrived, count, copies, own):
    pred = jnp.sum(arrived[...], axis=0) / count[...]
    own[...] = pred
    for g in range(GROUPS):
        copies[g] = pred


def own_predictions(arrived, count):
    return pl.pallas_call(
        gather_kernel,
        out_shape=(
            jax.ShapeDtypeStruct((GROUPS, 8, 128), F32),
            jax.ShapeDtypeStruct((8, 128), F32),
        ),
        compiler_params=pltpu.CompilerParams(vmem_limit_bytes=4 * MIB),
        name="own_predictions",
    )(arrived, count)


def moments_kernel(preds, own, given, out):
    scale = 1.0 / (float(MEMBERS - 1) ** 0.5)
    everyone = jnp.concatenate(
        [preds[pl.ds(q, MEMBERS, stride=4), :] for q in range(4)], axis=1
    )
    mine = jnp.concatenate([own[pl.ds(q, LOCAL, stride=4), :] for q in range(4)], axis=1)
    anomaly = (everyone - jnp.mean(everyone, axis=0, keepdims=True)) * scale
    misfit = given[0:LOCAL, :] - mine
    var = given[LOCAL : LOCAL + 1, :]
    weighted = anomaly / var
    pad = jnp.zeros((6, BLOCK), F32)
    right = jnp.concatenate(
        [anomaly, anomaly[8:], anomaly[16:], anomaly[24:]]
        + [misfit, pad] * 4
        + [jnp.zeros((16, BLOCK), F32)],
        axis=0,
    )
    product = lax.dot_general(
        weighted, right, (((1,), (1,)), ((), ())), precision=lax.Precision.HIGHEST,
        preferred_element_type=F32,
    )
    lane = lax.broadcasted_iota(jnp.int32, (8, 128), 1)
    packed = product[0:8]
    for c, start, stop in ((1, 32, 56), (2, 56, 72), (3, 72, 80)):
        mine = ((lane >= start) & (lane < stop)) | (lane // 8 == 10 + c)
        packed = jnp.where(mine, product[8 * c : 8 * c + 8], packed)
    for d in range(SLABS):
        out[d] = packed


def moments(preds, own, given):
    return pl.pallas_call(
        moments_kernel,
        out_shape=jax.ShapeDtypeStruct((SLABS, 8, 128), F32),
        compiler_params=pltpu.CompilerParams(vmem_limit_bytes=4 * MIB),
        name="moments",
    )(preds, own, given)


def update_kernel(group, arrived, here, there, out):
    parts = [arrived[d] for d in range(SLABS)]
    while len(parts) > 1:
        parts = [x + y for x, y in zip(parts[::2], parts[1::2])]
    packed = parts[0]
    lane8 = lax.broadcasted_iota(jnp.int32, (8, 128), 1)
    uppers, cross = [], []
    for c, start in enumerate((0, 32, 56, 72)):
        moved = pltpu.roll(packed, (8 * c - start) % 128, 1)
        uppers.append(jnp.where((lane8 >= 8 * c) & (lane8 < MEMBERS), moved, 0.0))
        cross.append(pltpu.roll(packed, (MEMBERS - 80 - 8 * c) % 128, 1))
    upper = jnp.concatenate(uppers, axis=0)
    cross = jnp.concatenate(cross, axis=0)
    tall = jnp.concatenate([upper, jnp.zeros((96, 128), F32)], axis=0)
    mirrored = tall.T[0:MEMBERS]
    row = lax.broadcasted_iota(jnp.int32, (MEMBERS, 128), 0)
    lane = lax.broadcasted_iota(jnp.int32, (MEMBERS, 128), 1)
    work = jnp.where(lane // 8 >= row // 8, upper, mirrored)
    work = jnp.where(row == lane, work + 1.0, work)
    work = jnp.where(lane < MEMBERS, work, jnp.where(lane < MEMBERS + LOCAL, cross, 0.0))
    for first in range(0, MEMBERS, 16):
        columns = [
            jnp.broadcast_to(work[:, k : k + 1], (MEMBERS, 128)) for k in range(first, first + 16)
        ]
        for i in range(16):
            k = first + i
            column = columns[i]
            inverse = 1.0 / column[k : k + 1, :]
            line = work[k : k + 1, :] * inverse
            work = jnp.where(row == k, line, work - column * line)
            for later in range(i + 1, 16):
                line = columns[later][k : k + 1, :] * inverse
                columns[later] = jnp.where(row == k, line, columns[later] - column * line)
    mixing = work - jnp.mean(work, axis=0, keepdims=True)
    mixing = mixing * (1.0 / float(MEMBERS - 1) ** 0.5)
    mixing = jnp.where(row - group[0] * LOCAL == lane - MEMBERS, mixing + 1.0, mixing)
    totals = [jnp.zeros((64, 128), F32) for _ in range(LOCAL)]
    for j in range(LOCAL):
        rows = jnp.broadcast_to(mixing[:, MEMBERS + j : MEMBERS + j + 1], (MEMBERS, 128))
        for size in (2, 4, 8, 16):
            swapped = jnp.where(
                row & size == 0, pltpu.roll(rows, MEMBERS - size, 0), pltpu.roll(rows, size, 0)
            )
            rows = jnp.where((LOCAL * group[0]) & size != 0, swapped, rows)
        for i, d in enumerate(PARTS):
            for m in range(LOCAL):
                at = 4 * d + m
                totals[j] = totals[j] + rows[at : at + 1, :] * here[2 * i + m]
                totals[j] = totals[j] + rows[at + 2 : at + 3, :] * there[2 * i + m]
    for j in range(LOCAL):
        out[j] = totals[j]


def update(group, arrived, *fields):
    vmem = pl.BlockSpec(memory_space=pltpu.VMEM)
    return pl.pallas_call(
        update_kernel,
        out_shape=jax.ShapeDtypeStruct((LOCAL, 64, 128), F32),
        in_specs=[pl.BlockSpec(memory_space=pltpu.SMEM)] + [vmem] * 3,
        out_specs=vmem,
        compiler_params=pltpu.CompilerParams(vmem_limit_bytes=4 * MIB),
        name="update",
    )(group, arrived, *fields)


def local(state, theta, forcing, boxes, observed, noise_var, perturb):
    slab = lax.axis_index("slab").astype(jnp.int32).reshape(1)
    group = lax.axis_index("group").astype(jnp.int32).reshape(1)
    near, far = pack(slab, state, theta, forcing)
    pairs = [(i, i + 1) for i in range(1, SLABS - 1, 2)]
    far = lax.ppermute(far, "slab", pairs + [(j, i) for i, j in pairs])
    near = lax.ppermute(near, "slab", [(i, i ^ 1) for i in range(SLABS)])
    field = theta.reshape(LOCAL, 64, 128)

    def from_chip(value, bit):
        return lax.ppermute(value, "group", [(i, i ^ (2 * bit)) for i in range(GROUPS)])

    pair = from_chip(field, 1)
    in_x, in_z, in_y, count, given, state, here, forcing, *inside = masks(
        slab, observed.reshape(1, BLOCK), noise_var.reshape(1, BLOCK), perturb, boxes,
        state, theta, forcing,
    )
    final, part = window(slab, near, far, in_x, in_z, in_y, state, forcing, *inside)
    arrived = lax.all_to_all(part, "slab", 0, 0, tiled=True)
    pair = jnp.concatenate([here.reshape(field.shape), pair], axis=0)
    across = from_chip(pair, 4)
    copies, own = own_predictions(arrived, count)
    preds = lax.all_to_all(copies, "group", 0, 0, tiled=True).reshape(GROUPS * 8, 128)
    even = jnp.concatenate([pair, across], axis=0)
    odd = from_chip(even, 2)
    sums = moments(preds, own, given)
    sums = lax.all_to_all(sums, "slab", 0, 0, tiled=True)
    here = jnp.concatenate([even, odd], axis=0)
    there = lax.ppermute(here, "group", [(i, i ^ 1) for i in range(GROUPS)])
    updated = update(group, sums, here, there)
    return final, updated.reshape(theta.shape)


def solution(mesh):
    return jax.shard_map(
        local,
        mesh=mesh,
        in_specs=(
            P("group", "slab", None, None),
            P("group", "slab", None, None),
            P("slab", None, None),
            P(),
            P("slab"),
            P("slab"),
            P("group", "slab"),
        ),
        out_specs=(P("group", "slab", None, None), P("group", "slab", None, None)),
        check_vma=False,
    )
```
